32 devices in a mesh: dp: 8 (over y, x, core), tensor: 4 (over z).
Axes of the slice: x: 2, y: 2, z: 4, core: 2. Of those that a mesh axis runs over, the one named last changes fastest.
Arguments:
- layer_in: bfloat16 [8, 1024, 1024], P(None, ('dp', 'tensor')), may hold values from -6 to 6
- text_mask: int32 [1024], P(('dp', 'tensor')), may hold values 0 or 1
- w_qkv: float32 [8, 3, 1024, 1024], P(None, None, 'dp', 'tensor'), may hold values from -0.1875 to 0.1875
- w_out: float32 [8, 1024, 1024], P(None, 'tensor', 'dp'), may hold values from -0.375 to 0.375
- w_gate_up: float32 [8, 2, 1024, 4096], P(None, None, 'dp', 'tensor'), may hold values from -0.1875 to 0.1875
- w_down: float32 [8, 4096, 1024], P(None, 'tensor', 'dp'), may hold values from -0.1875 to 0.1875
- norm_gains: float32 [2, 1024], P(None, 'dp'), may hold values from 0.1 to 1.9
- pad_row: float32 [1024], P('dp'), may hold values from -6 to 6
- out_grad: bfloat16 [8, 1024, 1024], P(None, ('dp', 'tensor')), may hold values from -6 to 6
Outputs:
- layer_out: bfloat16 [8, 1024, 1024], P(None, ('dp', 'tensor'))
- input_grad: bfloat16 [8, 1024, 1024], P(None, ('dp', 'tensor'))
- grad_qkv: float32 [8, 3, 1024, 1024], P(None, None, 'dp', 'tensor')
- grad_out: float32 [8, 1024, 1024], P(None, 'tensor', 'dp')
- grad_gate_up: float32 [8, 2, 1024, 4096], P(None, None, 'dp', 'tensor')
- grad_down: float32 [8, 4096, 1024], P(None, 'tensor', 'dp')
- grad_gains: float32 [2, 1024], P(None, 'dp')
- grad_pad: float32 [1024], P('dp')
The draws below stay inside these ranges and needn't reach their ends.
All inputs are finite; a program needn't handle non-finite values. No bound on the sum of `text_mask` on one device may be relied on, other than what follows from the above.
Results may differ from the reference program's by a relative error of at most 0.014.
The reference program's roundings to bfloat16 on the way count: a program that leaves them out, or rounds other values in their place, can miss the bound.
Values may be sent and summed in bfloat16 or wider, within the bound.
No kernel may reach another device: no remote copies, remote signals or barrier semaphores. Data moves between devices by JAX's collectives and lax.ppermute only.
A program may use at most 320 MiB of HBM per device.

```python
import math
import jax
import jax.numpy as jnp
from jax import lax

D = 1024
FF = 4096
STEPS = 8
HEAD = 64
FRAMES = 1024


def with_ends(result, stream_key, smallest, top_value):
    spot = [jax.random.randint(jax.random.fold_in(stream_key, axis), (), 0, length) for axis, length in enumerate(result.shape)]
    widest = result.shape.index(max(result.shape))
    neighbour = spot[:widest] + [(spot[widest] + 1) % result.shape[widest]] + spot[widest + 1:]
    return result.at[tuple(spot)].set(smallest).at[tuple(neighbour)].set(top_value)


def shard_levels(key, dims, shards, low, largest):
    loudness = 1.0
    for dim, blocks in shards:
        heights = jax.random.uniform(jax.random.fold_in(jax.random.fold_in(key, 6), dim), (blocks,), jnp.float32, low / len(shards), largest / len(shards))
        loudness = loudness * jnp.repeat(jnp.exp(heights), dims[dim] // blocks).reshape((-1,) + (1,) * (len(dims) - 1 - dim))
    return loudness


def centred(own_key, dims, scale, reach, split=(), held_as=jnp.bfloat16):
    level = shard_levels(own_key, dims, split, -0.22, 0.18) if split else 1.0
    array = jax.random.normal(own_key, dims, jnp.float32) * scale * level
    return jnp.minimum(jnp.maximum(array, -reach), reach).astype(held_as)


def setup_inputs(seed: int = 0) -> dict:
    key_of = jax.random.split(jax.random.key(seed), 10)
    layer_in = centred(key_of[0], (STEPS, FRAMES, D), 1.0, 6.0, ((1, 32),))
    text_mask = with_ends((jax.random.randint(key_of[1], (FRAMES,), 0, 2) < 1).astype(jnp.int32), jax.random.fold_in(key_of[1], 1), 0, 1)
    w_qkv = centred(key_of[2], (STEPS, 3, D, D), D ** -0.5, 0.1875, ((2, 8), (3, 4)), jnp.float32)
    w_out = centred(key_of[3], (STEPS, D, D), (D // 4) ** -0.5, 0.375, ((1, 4), (2, 8)), jnp.float32)
    w_gate_up = centred(key_of[4], (STEPS, 2, D, FF), D ** -0.5, 0.1875, ((2, 8), (3, 4)), jnp.float32)
    w_down = centred(key_of[5], (STEPS, FF, D), (FF // 4) ** -0.5, 0.1875, ((1, 4), (2, 8)), jnp.float32)
    norm_gains = jnp.clip(1.0 + 0.18 * jax.random.normal(key_of[6], (2, D), jnp.float32), 0.1, 1.9)
    pad_row = centred(key_of[7], (D,), 1.0, 6.0, ((0, 8),), jnp.float32)
    out_grad = centred(key_of[8], (STEPS, FRAMES, D), 1.0, 6.0, ((1, 32),))
    return dict(layer_in=layer_in, text_mask=text_mask, w_qkv=w_qkv, w_out=w_out, w_gate_up=w_gate_up, w_down=w_down, norm_gains=norm_gains, pad_row=pad_row, out_grad=out_grad)


@jax.custom_vjp
def low(v):
    return lax.optimization_barrier(v.astype(jnp.bfloat16)).astype(jnp.float32)

@jax.custom_vjp
def low_back(v):
    return v

def low_keep(v):
    return (low(v), None)

def low_pass(kept, grad):
    return (grad,)

def back_keep(v):
    return (v, None)

def back_low(kept, grad):
    return (low(grad),)
low.defvjp(low_keep, low_pass)
low_back.defvjp(back_keep, back_low)
EPS = 1e-05
HIGH = lax.Precision.HIGHEST

def layer(xval, maskf, w_qkv, w_out, w_gate_up, w_down, norm_gains, pad_row):
    steps, frames, width = xval.shape
    w_qkv = low(w_qkv)
    w_out = low(w_out)
    w_gate_up = low(w_gate_up)
    w_down = low(w_down)
    gains = low(norm_gains)
    padv = low(pad_row)
    first = (jnp.arange(steps) == 0).astype(jnp.float32)
    h0 = xval + first[:, None, None] * (1.0 - maskf)[None, :, None] * padv[None, None, :]
    r1 = lax.rsqrt(lax.optimization_barrier(jnp.mean(h0 * h0, axis=-1, keepdims=True)) + EPS)
    n1 = low(h0 * r1 * gains[0])
    qkv = jnp.einsum('sfd,sjde->sjfe', n1, w_qkv, precision=HIGH)
    qkv = low(low_back(qkv))
    heads = width // HEAD
    query = qkv[:, 0].reshape(steps, frames, heads, HEAD)
    keyv = qkv[:, 1].reshape(steps, frames, heads, HEAD)
    value = qkv[:, 2].reshape(steps, frames, heads, HEAD)
    scores = jnp.einsum('sfhe,tfhe->fhst', query, keyv, precision=HIGH) / math.sqrt(HEAD)
    causal = jnp.arange(steps)[:, None] >= jnp.arange(steps)[None, :]
    scores = jnp.where(causal, scores, -1e+30)
    top = lax.optimization_barrier(jnp.max(scores, axis=-1, keepdims=True))
    expo = jnp.exp(scores - top)
    probs = low(expo / lax.optimization_barrier(jnp.sum(expo, axis=-1, keepdims=True)))
    mixed = jnp.einsum('fhst,tfhe->sfhe', probs, value, precision=HIGH).reshape(steps, frames, width)
    mixed = low(low_back(mixed))
    attn = low_back(jnp.einsum('sfd,sde->sfe', mixed, w_out, precision=HIGH))
    h1 = h0 + attn
    r2 = lax.rsqrt(lax.optimization_barrier(jnp.mean(h1 * h1, axis=-1, keepdims=True)) + EPS)
    n2 = low(h1 * r2 * gains[1])
    gate_up = low_back(jnp.einsum('sfd,sjde->sjfe', n2, w_gate_up, precision=HIGH))
    gate = gate_up[:, 0]
    hidden = low(gate * jax.nn.sigmoid(gate) * gate_up[:, 1])
    ffout = low_back(jnp.einsum('sfk,skd->sfd', hidden, w_down, precision=HIGH))
    return h1 + ffout

def reference(layer_in, text_mask, w_qkv, w_out, w_gate_up, w_down, norm_gains, pad_row, out_grad):
    steps, frames, width = layer_in.shape
    block = math.gcd(frames, max(1, 4096 // steps))
    count = frames // block
    xs = layer_in.astype(jnp.float32).reshape(steps, count, block, width).transpose(1, 0, 2, 3)
    gs = out_grad.astype(jnp.float32).reshape(steps, count, block, width).transpose(1, 0, 2, 3)
    ms = text_mask.astype(jnp.float32).reshape(count, block)
    weights = (w_qkv, w_out, w_gate_up, w_down, norm_gains, pad_row)

    def one(carry, pieces):
        xb, mb, gb = pieces

        def local_fn(xv, a, b, c, d, e, f):
            return layer(xv, mb, a, b, c, d, e, f)
        outv, pull = jax.vjp(local_fn, xb, *weights)
        grads = pull(gb)
        carry = tuple((c + g for c, g in zip(carry, grads[1:])))
        return (carry, (outv.astype(jnp.bfloat16), grads[0].astype(jnp.bfloat16)))
    init = tuple((jnp.zeros(w.shape, jnp.float32) for w in weights))
    sums, (outs, dxs) = lax.scan(one, init, (xs, ms, gs))
    layer_out = outs.transpose(1, 0, 2, 3).reshape(steps, frames, width)
    input_grad = dxs.transpose(1, 0, 2, 3).reshape(steps, frames, width)
    return (layer_out, input_grad, sums[0], sums[1], sums[2], sums[3], sums[4], sums[5])
```

```python
import math

import jax
import jax.numpy as jnp
import numpy as np
from jax import lax
from jax.sharding import Mesh
from jax.sharding import PartitionSpec as P

HEAD = 64
EPS = 1e-05
HIGH = lax.Precision.HIGHEST
BF = jnp.bfloat16
F32 = jnp.float32
SWAP = ((0, 1), (1, 0))


def norm_back(upstream, hval, rstat, gain):
    scaled = upstream * gain
    dgain = jnp.sum(upstream * hval * rstat, axis=(0, 1))
    dhval = rstat * scaled - hval * rstat**3 * jnp.mean(scaled * hval, axis=-1, keepdims=True)
    return (dhval, dgain)


def half(array, axis, which):
    size = array.shape[axis] // 2
    return lax.dynamic_slice_in_dim(array, which * size, size, axis)


def ordered(core, own, other, axis):
    is_first = core == 0
    return jnp.concatenate(
        [jnp.where(is_first, own, other), jnp.where(is_first, other, own)], axis=axis
    )


def make_shards(tensor_size):
    def around(shift):
        return [(i, (i + shift) % tensor_size) for i in range(tensor_size)]

    def trade(core, weight, split_axis, join_axis):
        mine = half(weight, split_axis, core)
        theirs = half(weight, split_axis, 1 - core)
        got = lax.ppermute(theirs, "core", SWAP)
        return ordered(core, mine, got, join_axis)

    def collect(rows):
        parts = [rows] + [
            lax.ppermute(rows, "tensor", around(k)) for k in range(1, tensor_size)
        ]
        near = jnp.stack(parts, axis=1)
        far = lax.ppermute(near, "core", SWAP)
        whole = jnp.concatenate([near, far], axis=1)
        return whole.reshape(rows.shape[0], -1, rows.shape[2])

    def deal(partial):
        steps, frames, width = partial.shape
        split = partial.reshape(steps, 2, tensor_size, frames // (2 * tensor_size), width)
        got = lax.ppermute(split[:, 1].astype(BF), "core", SWAP)
        chip = split[:, 0].astype(F32) + got.astype(F32)
        total = chip[:, 0]
        for k in range(1, tensor_size):
            total = total + lax.ppermute(chip[:, k].astype(BF), "tensor", around(-k)).astype(F32)
        return total

    def shards(
        layer_in, text_mask, w_qkv, w_out, w_gate_up, w_down, norm_gains, pad_row, out_grad
    ):
        core = lax.axis_index("core")
        steps, local_frames, width = layer_in.shape

        w_attn = jnp.concatenate(
            [w_qkv.astype(BF), jnp.swapaxes(w_out, 1, 2)[:, None].astype(BF)], axis=1
        )
        w_attn = lax.all_gather(trade(core, w_attn, 3, 2), "xy", axis=2, tiled=True)
        small = jnp.concatenate([norm_gains, pad_row[None]], axis=0).astype(BF)
        small = lax.all_gather(small, ("xy", "core"), axis=1, tiled=True).astype(F32)
        wgu = lax.all_gather(trade(core, w_gate_up.astype(BF), 3, 2), "xy", axis=2, tiled=True)
        wdown = lax.all_gather(trade(core, w_down.astype(BF), 1, 2), "xy", axis=2, tiled=True)

        gain_one, gain_two, pad_vec = small[0], small[1], small[2]
        maskf = text_mask.astype(F32)
        first = (jnp.arange(steps) == 0).astype(F32)
        h0 = (
            layer_in.astype(F32)
            + first[:, None, None] * (1.0 - maskf)[None, :, None] * pad_vec[None, None, :]
        )
        r1 = lax.rsqrt(jnp.mean(h0 * h0, axis=-1, keepdims=True) + EPS)
        n1 = (h0 * r1 * gain_one).astype(BF)
        n1_all = collect(n1)
        grad_all = collect(out_grad)
        frames = n1_all.shape[1]
        wqkv, wout_t = w_attn[:, :3], w_attn[:, 3]
        qkv = jnp.einsum("sfd,sjde->sjfe", n1_all, wqkv, preferred_element_type=F32).astype(BF)
        col_width = qkv.shape[-1]
        heads = col_width // HEAD
        scale = 1.0 / math.sqrt(HEAD)
        query = qkv[:, 0].reshape(steps, frames, heads, HEAD)
        keyv = qkv[:, 1].reshape(steps, frames, heads, HEAD)
        value = qkv[:, 2].reshape(steps, frames, heads, HEAD)
        causal = jnp.arange(steps)[:, None] >= jnp.arange(steps)[None, :]

        def score_of(qv, kv):
            raw = jnp.einsum("sfhe,tfhe->fhst", qv, kv, preferred_element_type=F32) * scale
            return jnp.where(causal, raw, -1e30)

        scores = score_of(query, keyv)
        top = jnp.max(scores, axis=-1, keepdims=True)
        expo = jnp.exp(scores - top)
        total = jnp.sum(expo, axis=-1, keepdims=True)
        lse = top + jnp.log(total)
        probs_low = (expo / total).astype(BF)
        mixed = jnp.einsum("fhst,tfhe->sfhe", probs_low, value, preferred_element_type=F32)
        mixed = mixed.reshape(steps, frames, col_width).astype(BF)
        attn = deal(jnp.einsum("sfd,sed->sfe", mixed, wout_t, preferred_element_type=F32))
        h1 = h0 + attn
        r2 = lax.rsqrt(jnp.mean(h1 * h1, axis=-1, keepdims=True) + EPS)
        n2 = (h1 * r2 * gain_two).astype(BF)
        n2_all = collect(n2)
        gate_up = jnp.einsum("sfd,sjde->sjfe", n2_all, wgu, preferred_element_type=F32)
        gate = gate_up[:, 0]
        upval = gate_up[:, 1]
        sigma = jax.nn.sigmoid(gate)
        silu_val = gate * sigma
        hidden = (silu_val * upval).astype(BF)
        d_down = jnp.einsum("sfk,sfd->skd", hidden, grad_all, preferred_element_type=F32)
        r_down = lax.psum_scatter(d_down.astype(BF), "xy", scatter_dimension=2, tiled=True)
        d_hidden = jnp.einsum("sfd,skd->sfk", grad_all, wdown, preferred_element_type=F32)
        d_gate = d_hidden * upval * (sigma * (1.0 + gate * (1.0 - sigma)))
        d_up = d_hidden * silu_val
        d_gu = jnp.stack([d_gate, d_up], axis=1).astype(BF)
        d_gate_up = jnp.einsum("sfd,sjfe->sjde", n2_all, d_gu, preferred_element_type=F32)
        r_gate_up = lax.psum_scatter(d_gate_up.astype(BF), "xy", scatter_dimension=2, tiled=True)
        dn2 = deal(jnp.einsum("sjfe,sjde->sfd", d_gu, wgu, preferred_element_type=F32))
        dh_norm2, dgain_two = norm_back(dn2, h1, r2, gain_two)
        dh1 = out_grad.astype(F32) + dh_norm2
        dh1_all = collect(dh1.astype(BF))
        ffout = deal(jnp.einsum("sfk,skd->sfd", hidden, wdown, preferred_element_type=F32))
        layer_out = (h1 + ffout).astype(BF)
        d_out_t = jnp.einsum("sfe,sfd->sed", dh1_all, mixed, preferred_element_type=F32)
        d_mixed = jnp.einsum("sfe,sed->sfd", dh1_all, wout_t, preferred_element_type=F32)
        d_mixed = d_mixed.astype(BF).reshape(steps, frames, heads, HEAD)
        probs = jnp.exp(score_of(query, keyv) - lse)
        d_probs = jnp.einsum("sfhe,tfhe->fhst", d_mixed, value, preferred_element_type=F32)
        d_value = jnp.einsum("fhst,sfhe->tfhe", probs_low, d_mixed, preferred_element_type=F32)
        d_scores = probs * (d_probs - jnp.sum(probs * d_probs, axis=-1, keepdims=True))
        d_query = (
            jnp.einsum("fhst,tfhe->sfhe", d_scores, keyv.astype(F32), precision=HIGH) * scale
        )
        d_key = (
            jnp.einsum("fhst,sfhe->tfhe", d_scores, query.astype(F32), precision=HIGH) * scale
        )
        d_qkv = jnp.stack(
            [
                d_query.reshape(steps, frames, col_width),
                d_key.reshape(steps, frames, col_width),
                d_value.reshape(steps, frames, col_width),
            ],
            axis=1,
        ).astype(BF)
        d_wqkv = jnp.einsum("sfd,sjfe->sjde", n1_all, d_qkv, preferred_element_type=F32)
        d_attn = jnp.concatenate([d_wqkv.astype(BF), d_out_t[:, None].astype(BF)], axis=1)
        r_attn = lax.psum_scatter(d_attn, "xy", scatter_dimension=2, tiled=True)
        dn1 = deal(jnp.einsum("sjfe,sjde->sfd", d_qkv, wqkv, preferred_element_type=F32))
        dh_norm1, dgain_one = norm_back(dn1, h0, r1, gain_one)
        dh0 = dh1 + dh_norm1
        input_grad = dh0.astype(BF)
        d_pad = jnp.sum(dh0[0] * (1.0 - maskf)[:, None], axis=0)
        small_grad = jnp.stack([dgain_one, dgain_two, d_pad], axis=0)
        small_grad = lax.psum(small_grad, ("xy", "core", "tensor"))
        place = lax.axis_index("xy") * 2 + core
        g_small = lax.dynamic_slice_in_dim(
            small_grad, place * pad_row.shape[0], pad_row.shape[0], 1
        )

        def settle(reduced, split_axis, join_axis):
            return trade(core, reduced, split_axis, join_axis).astype(F32)

        g_down = settle(r_down, 2, 1)
        g_gate_up = settle(r_gate_up, 2, 3)
        g_attn = settle(r_attn, 2, 3)
        g_qkv = g_attn[:, :3]
        g_out = jnp.swapaxes(g_attn[:, 3], 1, 2)
        return (layer_out, input_grad, g_qkv, g_out, g_gate_up, g_down, g_small[0:2], g_small[2])

    return shards


def solution(mesh):
    dp_size, tensor_size = mesh.shape["dp"], mesh.shape["tensor"]
    inner = Mesh(
        np.asarray(mesh.devices).reshape(dp_size // 2, 2, tensor_size), ("xy", "core", "tensor")
    )
    dp = ("xy", "core")
    rows = ("xy", "core", "tensor")
    return jax.shard_map(
        make_shards(tensor_size),
        mesh=inner,
        in_specs=(
            P(None, rows, None),
            P(rows),
            P(None, None, dp, "tensor"),
            P(None, "tensor", dp),
            P(None, None, dp, "tensor"),
            P(None, "tensor", dp),
            P(None, dp),
            P(dp),
            P(None, rows, None),
        ),
        out_specs=(
            P(None, rows, None),
            P(None, rows, None),
            P(None, None, dp, "tensor"),
            P(None, "tensor", dp),
            P(None, None, dp, "tensor"),
            P(None, "tensor", dp),
            P(None, dp),
            P(dp),
        ),
        check_vma=False,
    )
```

```python
import math

import jax
import jax.numpy as jnp
import numpy as np
from jax import lax
from jax.sharding import Mesh
from jax.sharding import PartitionSpec as P

HEAD = 64
EPS = 1e-05
HIGH = lax.Precision.HIGHEST
BF = jnp.bfloat16
F32 = jnp.float32
SWAP = ((0, 1), (1, 0))


def norm_back(upstream, hval, rstat, gain):
    scaled = upstream * gain
    dgain = jnp.sum(upstream * hval * rstat, axis=(0, 1))
    dhval = rstat * scaled - hval * rstat**3 * jnp.mean(scaled * hval, axis=-1, keepdims=True)
    return (dhval, dgain)


def half(array, axis, which):
    size = array.shape[axis] // 2
    return lax.dynamic_slice_in_dim(array, which * size, size, axis)


def ordered(core, own, other, axis):
    is_first = core == 0
    return jnp.concatenate(
        [jnp.where(is_first, own, other), jnp.where(is_first, other, own)], axis=axis
    )


def make_shards(plane_size, tensor_size):
    paired = plane_size == 4

    def around(shift):
        return [(i, (i + shift) % tensor_size) for i in range(tensor_size)]

    def across(array, bits):
        return lax.ppermute(array, "xy", [(i, i ^ bits) for i in range(plane_size)])

    def relative(array):
        if not paired:
            return array
        size = array.shape[-1] // plane_size
        chip = lax.axis_index("xy")
        blocks = [
            lax.dynamic_slice_in_dim(array, (chip ^ r) * size, size, array.ndim - 1)
            for r in range(plane_size)
        ]
        return jnp.concatenate(blocks, axis=-1)

    def plane_gather(weight):
        if not paired:
            return lax.all_gather(weight, "xy", axis=2, tiled=True), weight
        from_x, from_y = across(weight, 1), across(weight, 2)
        far_a = across(from_y[:, :2], 1)
        far_b = across(from_x[:, 2:], 2)
        far = jnp.concatenate([far_a, far_b], axis=1)
        return jnp.concatenate([weight, from_x, from_y, far], axis=2), (from_x, from_y)

    def plane_reduce(first, second):
        if not paired:
            both = jnp.concatenate([first, second], axis=1)
            return lax.psum_scatter(both, "xy", scatter_dimension=2, tiled=True).astype(F32)
        size = first.shape[2] // plane_size
        results = []
        for part, near, other in ((first, 1, 2), (second, 2, 1)):
            block = [part[:, :, r * size : (r + 1) * size] for r in range(plane_size)]
            got = across(jnp.concatenate([block[near], block[3]], axis=2), near)
            own = block[0].astype(F32) + got[:, :, :size].astype(F32)
            passed = block[other].astype(F32) + got[:, :, size:].astype(F32)
            results.append(own + across(passed.astype(BF), other).astype(F32))
        return jnp.concatenate(results, axis=1)

    def small_sum(vectors, core, local):
        if not paired:
            vectors = lax.psum(vectors, ("xy", "core", "tensor"))
            place = lax.axis_index("xy") * 2 + core
            return lax.dynamic_slice_in_dim(vectors, place * local, local, 1)
        total = vectors
        for k in range(1, tensor_size):
            total = total + lax.ppermute(vectors, "tensor", around(k))
        total = relative(total + lax.ppermute(total, "core", SWAP))
        size = total.shape[1] // plane_size
        mine = total[:, :size]
        for r in range(1, plane_size):
            mine = mine + across(total[:, r * size : (r + 1) * size], r)
        return half(mine, 1, core)

    def trade(core, weight, split_axis, join_axis):
        mine = half(weight, split_axis, core)
        theirs = half(weight, split_axis, 1 - core)
        got = lax.ppermute(theirs, "core", SWAP)
        return ordered(core, mine, got, join_axis)

    def collect(rows):
        parts = [rows] + [
            lax.ppermute(rows, "tensor", around(k)) for k in range(1, tensor_size)
        ]
        near = jnp.stack(parts, axis=1)
        far = lax.ppermute(near, "core", SWAP)
        whole = jnp.concatenate([near, far], axis=1)
        return whole.reshape(rows.shape[0], -1, rows.shape[2])

    def deal(partial):
        steps, frames, width = partial.shape
        split = partial.reshape(steps, 2, tensor_size, frames // (2 * tensor_size), width)
        got = lax.ppermute(split[:, 1].astype(BF), "core", SWAP)
        chip = split[:, 0].astype(F32) + got.astype(F32)
        total = chip[:, 0]
        for k in range(1, tensor_size):
            total = total + lax.ppermute(chip[:, k].astype(BF), "tensor", around(-k)).astype(F32)
        return total

    def shards(
        layer_in, text_mask, w_qkv, w_out, w_gate_up, w_down, norm_gains, pad_row, out_grad
    ):
        core = lax.axis_index("core")
        steps, local_frames, width = layer_in.shape

        w_attn = jnp.concatenate(
            [w_qkv.astype(BF), jnp.swapaxes(w_out, 1, 2)[:, None].astype(BF)], axis=1
        )
        w_attn, arrived = plane_gather(trade(core, w_attn, 3, 2))
        small = jnp.concatenate([norm_gains, pad_row[None]], axis=0).astype(BF)
        small = lax.all_gather(small, ("xy", "core"), axis=1, tiled=True).astype(F32)
        wgu, arrived = lax.optimization_barrier((trade(core, w_gate_up.astype(BF), 3, 2), arrived))
        wgu = lax.all_gather(wgu, "xy", axis=2, tiled=True)
        wdown = lax.all_gather(trade(core, w_down.astype(BF), 1, 2), "xy", axis=2, tiled=True)

        gain_one, gain_two, pad_vec = small[0], small[1], small[2]
        maskf = text_mask.astype(F32)
        first = (jnp.arange(steps) == 0).astype(F32)
        h0 = (
            layer_in.astype(F32)
            + first[:, None, None] * (1.0 - maskf)[None, :, None] * pad_vec[None, None, :]
        )
        r1 = lax.rsqrt(jnp.mean(h0 * h0, axis=-1, keepdims=True) + EPS)
        n1 = (h0 * r1 * gain_one).astype(BF)
        n1_all = collect(relative(n1))
        grad_all = collect(out_grad)
        frames = n1_all.shape[1]
        wqkv, wout_t = w_attn[:, :3], w_attn[:, 3]
        qkv = jnp.einsum("sfd,sjde->sjfe", n1_all, wqkv, preferred_element_type=F32).astype(BF)
        col_width = qkv.shape[-1]
        heads = col_width // HEAD
        scale = 1.0 / math.sqrt(HEAD)
        query = qkv[:, 0].reshape(steps, frames, heads, HEAD)
        keyv = qkv[:, 1].reshape(steps, frames, heads, HEAD)
        value = qkv[:, 2].reshape(steps, frames, heads, HEAD)
        causal = jnp.arange(steps)[:, None] >= jnp.arange(steps)[None, :]

        def score_of(qv, kv):
            raw = jnp.einsum("sfhe,tfhe->fhst", qv, kv, preferred_element_type=F32) * scale
            return jnp.where(causal, raw, -1e30)

        scores = score_of(query, keyv)
        top = jnp.max(scores, axis=-1, keepdims=True)
        expo = jnp.exp(scores - top)
        total = jnp.sum(expo, axis=-1, keepdims=True)
        lse = top + jnp.log(total)
        probs_low = (expo / total).astype(BF)
        mixed = jnp.einsum("fhst,tfhe->sfhe", probs_low, value, preferred_element_type=F32)
        mixed = mixed.reshape(steps, frames, col_width).astype(BF)
        attn = relative(deal(jnp.einsum("sfd,sed->sfe", mixed, wout_t, preferred_element_type=F32)))
        h1 = h0 + attn
        r2 = lax.rsqrt(jnp.mean(h1 * h1, axis=-1, keepdims=True) + EPS)
        n2 = (h1 * r2 * gain_two).astype(BF)
        n2_all = collect(n2)
        gate_up = jnp.einsum("sfd,sjde->sjfe", n2_all, wgu, preferred_element_type=F32)
        gate = gate_up[:, 0]
        upval = gate_up[:, 1]
        sigma = jax.nn.sigmoid(gate)
        silu_val = gate * sigma
        hidden = (silu_val * upval).astype(BF)
        d_down = jnp.einsum("sfk,sfd->skd", hidden, grad_all, preferred_element_type=F32)
        d_down, wdown = lax.optimization_barrier((d_down.astype(BF), wdown))
        r_down = lax.psum_scatter(d_down, "xy", scatter_dimension=2, tiled=True)
        d_hidden = jnp.einsum("sfd,skd->sfk", grad_all, wdown, preferred_element_type=F32)
        d_gate = d_hidden * upval * (sigma * (1.0 + gate * (1.0 - sigma)))
        d_up = d_hidden * silu_val
        d_gu = jnp.stack([d_gate, d_up], axis=1).astype(BF)
        d_gate_up = jnp.einsum("sfd,sjfe->sjde", n2_all, d_gu, preferred_element_type=F32)
        r_gate_up = lax.psum_scatter(d_gate_up.astype(BF), "xy", scatter_dimension=2, tiled=True)
        dn2 = deal(jnp.einsum("sjfe,sjde->sfd", d_gu, wgu, preferred_element_type=F32))
        dh_norm2, dgain_two = norm_back(dn2, h1, r2, gain_two)
        dh1 = out_grad.astype(F32) + dh_norm2
        dh1_all = collect(relative(dh1.astype(BF)))
        ffout = deal(jnp.einsum("sfk,skd->sfd", hidden, wdown, preferred_element_type=F32))
        layer_out = (h1 + ffout).astype(BF)
        d_out_t = jnp.einsum("sfe,sfd->sed", dh1_all, mixed, preferred_element_type=F32)
        d_mixed = jnp.einsum("sfe,sed->sfd", dh1_all, wout_t, preferred_element_type=F32)
        d_mixed = d_mixed.astype(BF).reshape(steps, frames, heads, HEAD)
        probs = jnp.exp(score_of(query, keyv) - lse)
        d_probs = jnp.einsum("sfhe,tfhe->fhst", d_mixed, value, preferred_element_type=F32)
        d_value = jnp.einsum("fhst,sfhe->tfhe", probs_low, d_mixed, preferred_element_type=F32)
        d_scores = probs * (d_probs - jnp.sum(probs * d_probs, axis=-1, keepdims=True))
        d_query = (
            jnp.einsum("fhst,tfhe->sfhe", d_scores, keyv.astype(F32), precision=HIGH) * scale
        )
        d_key = (
            jnp.einsum("fhst,sfhe->tfhe", d_scores, query.astype(F32), precision=HIGH) * scale
        )
        d_qk = jnp.stack(
            [
                d_query.reshape(steps, frames, col_width),
                d_key.reshape(steps, frames, col_width),
            ],
            axis=1,
        ).astype(BF)
        d_v = d_value.reshape(steps, frames, col_width).astype(BF)
        d_wqk = jnp.einsum("sfd,sjfe->sjde", n1_all, d_qk, preferred_element_type=F32)
        d_wv = jnp.einsum("sfd,sfe->sde", n1_all, d_v, preferred_element_type=F32)
        d_vo = jnp.stack([d_wv, d_out_t], axis=1).astype(BF)
        r_attn = plane_reduce(d_wqk.astype(BF), d_vo)
        d_qkv = jnp.concatenate([d_qk, d_v[:, None]], axis=1)
        dn1 = relative(
            deal(jnp.einsum("sjfe,sjde->sfd", d_qkv, wqkv, preferred_element_type=F32))
        )
        dh_norm1, dgain_one = norm_back(dn1, h0, r1, gain_one)
        dh0 = dh1 + dh_norm1
        input_grad = dh0.astype(BF)
        d_pad = jnp.sum(dh0[0] * (1.0 - maskf)[:, None], axis=0)
        small_grad = jnp.stack([dgain_one, dgain_two, d_pad], axis=0)
        g_small = small_sum(small_grad, core, pad_row.shape[0])

        def settle(reduced, split_axis, join_axis):
            return trade(core, reduced.astype(BF), split_axis, join_axis).astype(F32)

        g_down = settle(r_down, 2, 1)
        g_gate_up = settle(r_gate_up, 2, 3)
        g_attn = settle(r_attn, 2, 3)
        g_qkv = g_attn[:, :3]
        g_out = jnp.swapaxes(g_attn[:, 3], 1, 2)
        return (layer_out, input_grad, g_qkv, g_out, g_gate_up, g_down, g_small[0:2], g_small[2])

    return shards


def solution(mesh):
    dp_size, tensor_size = mesh.shape["dp"], mesh.shape["tensor"]
    inner = Mesh(
        np.asarray(mesh.devices).reshape(dp_size // 2, 2, tensor_size), ("xy", "core", "tensor")
    )
    dp = ("xy", "core")
    rows = ("xy", "core", "tensor")
    return jax.shard_map(
        make_shards(dp_size // 2, tensor_size),
        mesh=inner,
        in_specs=(
            P(None, rows, None),
            P(rows),
            P(None, None, dp, "tensor"),
            P(None, "tensor", dp),
            P(None, None, dp, "tensor"),
            P(None, "tensor", dp),
            P(None, dp),
            P(dp),
            P(None, rows, None),
        ),
        out_specs=(
            P(None, rows, None),
            P(None, rows, None),
            P(None, None, dp, "tensor"),
            P(None, "tensor", dp),
            P(None, None, dp, "tensor"),
            P(None, "tensor", dp),
            P(None, dp),
            P(dp),
        ),
        check_vma=False,
    )
```

```python
import math

import jax
import jax.numpy as jnp
import numpy as np
from jax import lax
from jax.sharding import Mesh
from jax.sharding import PartitionSpec as P

HEAD = 64
EPS = 1e-05
HIGH = lax.Precision.HIGHEST
BF = jnp.bfloat16
F32 = jnp.float32
SWAP = ((0, 1), (1, 0))
TILE = 16


def norm_back(upstream, hval, rstat, gain):
    scaled = upstream * gain
    dgain = jnp.sum(upstream * hval * rstat, axis=(0, 1))
    dhval = rstat * scaled - hval * rstat**3 * jnp.mean(scaled * hval, axis=-1, keepdims=True)
    return (dhval, dgain)


def half(array, axis, which):
    size = array.shape[axis] // 2
    return lax.dynamic_slice_in_dim(array, which * size, size, axis)


def ordered(core, own, other, axis):
    is_first = core == 0
    return jnp.concatenate(
        [jnp.where(is_first, own, other), jnp.where(is_first, other, own)], axis=axis
    )


def make_shards(tensor_size):
    def around(shift):
        return [(i, (i + shift) % tensor_size) for i in range(tensor_size)]

    def trade(core, weight, split_axis, join_axis):
        mine = half(weight, split_axis, core)
        theirs = half(weight, split_axis, 1 - core)
        got = lax.ppermute(theirs, "core", SWAP)
        return ordered(core, mine, got, join_axis)

    def collect(rows):
        parts = [rows] + [
            lax.ppermute(rows, "tensor", around(k)) for k in range(1, tensor_size)
        ]
        near = jnp.stack(parts, axis=1)
        far = lax.ppermute(near, "core", SWAP)
        whole = jnp.concatenate([near, far], axis=1)
        return whole.reshape(rows.shape[0], -1, rows.shape[2])

    def deal(partial):
        steps, frames, width = partial.shape
        split = partial.reshape(steps, 2, tensor_size, frames // (2 * tensor_size), width)
        got = lax.ppermute(split[:, 1].astype(BF), "core", SWAP)
        chip = split[:, 0].astype(F32) + got.astype(F32)
        total = chip[:, 0]
        for k in range(1, tensor_size):
            total = total + lax.ppermute(chip[:, k].astype(BF), "tensor", around(-k)).astype(F32)
        return total

    def shards(
        layer_in, text_mask, w_qkv, w_out, w_gate_up, w_down, norm_gains, pad_row, out_grad
    ):
        core = lax.axis_index("core")
        steps, local_frames, width = layer_in.shape

        w_attn = jnp.concatenate(
            [w_qkv.astype(BF), jnp.swapaxes(w_out, 1, 2)[:, None].astype(BF)], axis=1
        )
        w_attn = lax.all_gather(trade(core, w_attn, 3, 2), "xy", axis=2, tiled=True)
        small = jnp.concatenate([norm_gains, pad_row[None]], axis=0).astype(BF)
        small = lax.all_gather(small, ("xy", "core"), axis=1, tiled=True).astype(F32)
        wgu = lax.all_gather(trade(core, w_gate_up.astype(BF), 3, 2), "xy", axis=2, tiled=True)
        wdown = lax.all_gather(trade(core, w_down.astype(BF), 1, 2), "xy", axis=2, tiled=True)

        gain_one, gain_two, pad_vec = small[0], small[1], small[2]
        maskf = text_mask.astype(F32)
        first = (jnp.arange(steps) == 0).astype(F32)
        h0 = (
            layer_in.astype(F32)
            + first[:, None, None] * (1.0 - maskf)[None, :, None] * pad_vec[None, None, :]
        )
        r1 = lax.rsqrt(jnp.mean(h0 * h0, axis=-1, keepdims=True) + EPS)
        n1 = (h0 * r1 * gain_one).astype(BF)
        n1_all = collect(n1)
        grad_all = collect(out_grad)
        frames = n1_all.shape[1]
        wqkv, wout_t = w_attn[:, :3], w_attn[:, 3]
        qkv = jnp.einsum("sfd,sjde->sjfe", n1_all, wqkv, preferred_element_type=F32).astype(BF)
        col_width = qkv.shape[-1]
        heads = col_width // HEAD
        scale = 1.0 / math.sqrt(HEAD)
        query = qkv[:, 0].reshape(steps, frames, heads, HEAD)
        keyv = qkv[:, 1].reshape(steps, frames, heads, HEAD)
        value = qkv[:, 2].reshape(steps, frames, heads, HEAD)
        causal = jnp.arange(steps)[:, None] >= jnp.arange(steps)[None, :]

        def score_of(qv, kv):
            raw = jnp.einsum("sfhe,tfhe->fhst", qv, kv, preferred_element_type=F32) * scale
            return jnp.where(causal, raw, -1e30)

        scores = score_of(query, keyv)
        top = jnp.max(scores, axis=-1, keepdims=True)
        expo = jnp.exp(scores - top)
        total = jnp.sum(expo, axis=-1, keepdims=True)
        lse = top + jnp.log(total)
        probs_low = (expo / total).astype(BF)
        mixed = jnp.einsum("fhst,tfhe->sfhe", probs_low, value, preferred_element_type=F32)
        mixed = mixed.reshape(steps, frames, col_width).astype(BF)
        attn = deal(jnp.einsum("sfd,sed->sfe", mixed, wout_t, preferred_element_type=F32))
        h1 = h0 + attn
        r2 = lax.rsqrt(jnp.mean(h1 * h1, axis=-1, keepdims=True) + EPS)
        n2 = (h1 * r2 * gain_two).astype(BF)
        n2_all = collect(n2)
        gate_up = jnp.einsum("sfd,sjde->sjfe", n2_all, wgu, preferred_element_type=F32)
        gate = gate_up[:, 0]
        upval = gate_up[:, 1]
        sigma = jax.nn.sigmoid(gate)
        silu_val = gate * sigma
        hidden = (silu_val * upval).astype(BF)
        d_down = jnp.einsum("sfk,sfd->skd", hidden, grad_all, preferred_element_type=F32)
        r_down = lax.psum_scatter(d_down.astype(BF), "xy", scatter_dimension=2, tiled=True)
        d_hidden = jnp.einsum("sfd,skd->sfk", grad_all, wdown, preferred_element_type=F32)
        d_gate = d_hidden * upval * (sigma * (1.0 + gate * (1.0 - sigma)))
        d_up = d_hidden * silu_val
        d_gu = jnp.stack([d_gate, d_up], axis=1).astype(BF)
        d_gate_up = jnp.einsum("sfd,sjfe->sjde", n2_all, d_gu, preferred_element_type=F32)
        r_gate_up = lax.psum_scatter(d_gate_up.astype(BF), "xy", scatter_dimension=2, tiled=True)
        dn2 = deal(jnp.einsum("sjfe,sjde->sfd", d_gu, wgu, preferred_element_type=F32))
        dh_norm2, dgain_two = norm_back(dn2, h1, r2, gain_two)
        dh1 = out_grad.astype(F32) + dh_norm2
        dh1_all = collect(dh1.astype(BF))
        ffout = deal(jnp.einsum("sfk,skd->sfd", hidden, wdown, preferred_element_type=F32))
        layer_out = (h1 + ffout).astype(BF)
        d_out_t = jnp.einsum("sfe,sfd->sed", dh1_all, mixed, preferred_element_type=F32)
        d_mixed = jnp.einsum("sfe,sed->sfd", dh1_all, wout_t, preferred_element_type=F32)
        d_mixed = d_mixed.astype(BF).reshape(steps, frames, heads, HEAD)
        probs = jnp.exp(score_of(query, keyv) - lse)
        d_probs = jnp.einsum("sfhe,tfhe->fhst", d_mixed, value, preferred_element_type=F32)
        d_value = jnp.einsum("fhst,sfhe->tfhe", probs_low, d_mixed, preferred_element_type=F32)
        d_scores = probs * (d_probs - jnp.sum(probs * d_probs, axis=-1, keepdims=True))
        d_query = (
            jnp.einsum("fhst,tfhe->sfhe", d_scores, keyv.astype(F32), precision=HIGH) * scale
        )
        d_key = (
            jnp.einsum("fhst,sfhe->tfhe", d_scores, query.astype(F32), precision=HIGH) * scale
        )
        d_qkv = jnp.stack(
            [
                d_query.reshape(steps, frames, col_width),
                d_key.reshape(steps, frames, col_width),
                d_value.reshape(steps, frames, col_width),
            ],
            axis=1,
        ).astype(BF)
        d_wqkv = jnp.einsum("sfd,sjfe->sjde", n1_all, d_qkv, preferred_element_type=F32)
        d_attn = jnp.concatenate([d_wqkv.astype(BF), d_out_t[:, None].astype(BF)], axis=1)
        r_attn = lax.psum_scatter(d_attn, "xy", scatter_dimension=2, tiled=True)
        dn1 = deal(jnp.einsum("sjfe,sjde->sfd", d_qkv, wqkv, preferred_element_type=F32))
        dh_norm1, dgain_one = norm_back(dn1, h0, r1, gain_one)
        dh0 = dh1 + dh_norm1
        input_grad = dh0.astype(BF)
        d_pad = jnp.sum(dh0[0] * (1.0 - maskf)[:, None], axis=0)
        small_grad = jnp.stack([dgain_one, dgain_two, d_pad], axis=0)
        small_grad = lax.psum(small_grad, ("xy", "core", "tensor"))
        place = lax.axis_index("xy") * 2 + core
        g_small = lax.dynamic_slice_in_dim(
            small_grad, place * pad_row.shape[0], pad_row.shape[0], 1
        )

        def settle(reduced, split_axis, join_axis):
            return trade(core, reduced, split_axis, join_axis).astype(F32)

        g_down = settle(r_down, 2, 1)
        g_gate_up = settle(r_gate_up, 2, 3)
        g_attn = settle(r_attn, 2, 3)
        g_qkv = g_attn[:, :3]
        g_out = jnp.swapaxes(g_attn[:, 3], 1, 2)
        return (layer_out, input_grad, g_qkv, g_out, g_gate_up, g_down, g_small[0:2], g_small[2])

    return shards


def make_step_shards(count, lanes):

    def swap(block, k):
        return lax.ppermute(block, "dp", [(i, i ^ k) for i in range(count)])

    def exchange(blocks):
        return [blocks[0]] + [swap(blocks[k], k) for k in range(1, count)]

    def up(block, senders):
        return lax.ppermute(block, "tensor", [(i, i + 1) for i in range(senders)])

    def down(block, senders):
        return lax.ppermute(block, "tensor", [(i, i - 1) for i in range(lanes - senders, lanes)])

    def collect(rows):
        below, above = [rows], [rows]
        for k in range(1, lanes):
            below.append(lax.ppermute(
                below[-1], "tensor", [(i, i + 1) for i in range(k - 1, lanes - 1)]))
            above.append(lax.ppermute(
                above[-1], "tensor", [(i, i - 1) for i in range(1, lanes - k + 1)]))
        parts = [rows] + [above[k] + below[lanes - k] for k in range(1, lanes)]
        return jnp.stack(parts, axis=1).reshape(-1, rows.shape[-1])

    def deal(partial):
        slots = partial.reshape(count, lanes, -1, partial.shape[-1])
        rising, falling = 0.0, 0.0
        for r in range(1, lanes):
            rising = up((slots[:, lanes - r] + rising).astype(BF), r).astype(F32)
            falling = down((slots[:, r] + falling).astype(BF), r).astype(F32)
        return slots[:, 0] + rising + falling

    def shards(
        layer_in, text_mask, w_qkv, w_out, w_gate_up, w_down, norm_gains, pad_row, out_grad
    ):
        me = lax.axis_index("dp")
        steps, local, width = layer_in.shape
        block = width // count

        def pick(array, k):
            return lax.dynamic_index_in_dim(array, me ^ k, 0, keepdims=False)

        def relative(array):
            return jnp.concatenate(
                [
                    lax.dynamic_slice_in_dim(array, (me ^ r) * block, block, array.ndim - 1)
                    for r in range(count)
                ],
                axis=-1,
            )

        def place(blocks):
            whole = jnp.zeros((count,) + blocks[0].shape, blocks[0].dtype)
            for k in range(count):
                whole = lax.dynamic_update_index_in_dim(whole, blocks[k], me ^ k, 0)
            return whole

        def tag(rows, *vectors):
            line = jnp.concatenate([v.astype(rows.dtype) for v in vectors])
            return jnp.concatenate(
                [rows, jnp.pad(line[None], ((0, TILE - 1), (0, width - line.shape[0])))]
            )

        small = jnp.concatenate([norm_gains, pad_row[None]], axis=0).astype(BF).reshape(-1)
        hello = exchange([tag(pick(layer_in, k), small, text_mask) for k in range(count)])
        rows_in = relative(jnp.stack([h[:local] for h in hello])).astype(F32)
        notes = jnp.stack([h[local] for h in hello]).astype(F32)
        small = jnp.swapaxes(notes[:, : 3 * block].reshape(count, 3, block), 0, 1)
        gain_one, gain_two, pad_vec = small.reshape(3, width)
        padded = jnp.where(me == 0, 1.0 - notes[:, 3 * block : 3 * block + local], 0.0)[..., None]
        h0 = rows_in + padded * pad_vec
        r1 = lax.rsqrt(jnp.mean(h0 * h0, axis=-1, keepdims=True) + EPS)
        n1 = (h0 * r1 * gain_one).astype(BF)
        n1_all = collect(n1)

        def attn_block(k):
            parts = [pick(w_qkv, k)[j] for j in range(3)] + [pick(w_out, k).T]
            return jnp.concatenate(parts, axis=1).astype(BF)

        w_attn = jnp.concatenate(exchange([attn_block(k) for k in range(count)]), axis=0)
        cols = w_attn.shape[1] // 4
        w_in, wout_t = w_attn[:, : 3 * cols], w_attn[:, 3 * cols :]
        qkv = jnp.dot(n1_all, w_in, preferred_element_type=F32).astype(BF)

        def frame_split(array):
            return jnp.stack(exchange(list(array.reshape(count, -1, array.shape[-1]))))

        def frame_join(array):
            return jnp.concatenate(exchange(list(array)), axis=0)

        qkv = frame_split(qkv)
        frames = qkv.shape[1]
        heads = cols // HEAD
        scale = 1.0 / math.sqrt(HEAD)
        query = qkv[..., :cols].reshape(steps, frames, heads, HEAD)
        keyv = qkv[..., cols : 2 * cols].reshape(steps, frames, heads, HEAD)
        value = qkv[..., 2 * cols :].reshape(steps, frames, heads, HEAD)
        order = jnp.arange(steps) ^ me
        causal = order[:, None] >= order[None, :]

        def score_of(qv, kv):
            raw = jnp.einsum("sfhe,tfhe->fhst", qv, kv, preferred_element_type=F32) * scale
            return jnp.where(causal, raw, -1e30)

        scores = score_of(query, keyv)
        top = jnp.max(scores, axis=-1, keepdims=True)
        expo = jnp.exp(scores - top)
        total = jnp.sum(expo, axis=-1, keepdims=True)
        lse = top + jnp.log(total)
        probs_low = (expo / total).astype(BF)
        mixed = jnp.einsum("fhst,tfhe->sfhe", probs_low, value, preferred_element_type=F32)
        mixed_all = frame_join(mixed.reshape(steps, frames, cols).astype(BF))

        w_gate_up, w_down, mixed_all = lax.optimization_barrier((w_gate_up, w_down, mixed_all))

        def gu_block(k):
            pair = pick(w_gate_up, k)
            return jnp.concatenate([pair[0], pair[1]], axis=1).astype(BF)

        wgu = jnp.concatenate(exchange([gu_block(k) for k in range(count)]), axis=0)
        wdown = jnp.concatenate(
            exchange([pick(w_down, k).astype(BF) for k in range(count)]), axis=1
        )
        out_grad, _ = lax.optimization_barrier((out_grad, n1_all))
        grad = relative(jnp.stack(exchange([pick(out_grad, k) for k in range(count)])))
        grad_all = collect(grad)

        attn = deal(jnp.einsum("fe,de->fd", mixed_all, wout_t, preferred_element_type=F32))
        h1 = h0 + attn
        r2 = lax.rsqrt(jnp.mean(h1 * h1, axis=-1, keepdims=True) + EPS)
        n2 = (h1 * r2 * gain_two).astype(BF)
        n2_all = collect(n2)
        gate_up = jnp.dot(n2_all, wgu, preferred_element_type=F32)
        hid_width = gate_up.shape[1] // 2
        gate, upval = gate_up[:, :hid_width], gate_up[:, hid_width:]
        sigma = jax.nn.sigmoid(gate)
        silu_val = gate * sigma
        hidden = (silu_val * upval).astype(BF)
        d_hidden = jnp.einsum("fd,kd->fk", grad_all, wdown, preferred_element_type=F32)
        d_gate = d_hidden * upval * (sigma * (1.0 + gate * (1.0 - sigma)))
        d_up = d_hidden * silu_val
        d_gu = jnp.concatenate([d_gate, d_up], axis=1).astype(BF)
        dn2 = deal(jnp.einsum("fk,dk->fd", d_gu, wgu, preferred_element_type=F32))

        d_down = jnp.einsum("fk,fd->kd", hidden, grad_all, preferred_element_type=F32).astype(BF)
        g_down = exchange([d_down[:, r * block : (r + 1) * block] for r in range(count)])
        d_gate_up = jnp.einsum("fd,fk->dk", n2_all, d_gu, preferred_element_type=F32).astype(BF)
        g_gate_up = exchange(list(d_gate_up.reshape(count, block, -1)))

        dh_norm2, dgain_two = norm_back(dn2, h1, r2, gain_two)
        dh1 = grad.astype(F32) + dh_norm2
        dh1_all = collect(dh1.astype(BF))
        d_mixed = jnp.dot(dh1_all, wout_t, preferred_element_type=F32).astype(BF)
        d_mixed = frame_split(d_mixed).reshape(steps, frames, heads, HEAD)

        hidden, _ = lax.optimization_barrier((hidden, dh1_all))
        ffout = deal(jnp.dot(hidden, wdown, preferred_element_type=F32))
        layer_out = relative((h1 + ffout).astype(BF))
        layer_out = place(exchange(list(layer_out)))

        probs = jnp.exp(score_of(query, keyv) - lse)
        d_probs = jnp.einsum("sfhe,tfhe->fhst", d_mixed, value, preferred_element_type=F32)
        d_value = jnp.einsum("fhst,sfhe->tfhe", probs_low, d_mixed, preferred_element_type=F32)
        d_scores = probs * (d_probs - jnp.sum(probs * d_probs, axis=-1, keepdims=True))
        d_query = (
            jnp.einsum("fhst,tfhe->sfhe", d_scores, keyv.astype(F32), precision=HIGH) * scale
        )
        d_key = (
            jnp.einsum("fhst,sfhe->tfhe", d_scores, query.astype(F32), precision=HIGH) * scale
        )
        d_qkv = jnp.concatenate(
            [a.reshape(steps, frames, cols).astype(BF) for a in (d_query, d_key, d_value)],
            axis=-1,
        )
        d_qkv = frame_join(d_qkv)
        dn1 = deal(jnp.einsum("fe,de->fd", d_qkv, w_in, preferred_element_type=F32))
        d_attn = jnp.concatenate(
            [
                jnp.einsum("fd,fe->de", n1_all, d_qkv, preferred_element_type=F32).astype(BF),
                jnp.einsum("fd,fe->de", dh1_all, mixed_all, preferred_element_type=F32).astype(BF),
            ],
            axis=1,
        )
        g_attn = exchange(list(d_attn.reshape(count, block, -1)))

        dh_norm1, dgain_one = norm_back(dn1, h0, r1, gain_one)
        dh0 = dh1 + dh_norm1
        d_pad = jnp.sum(dh0 * padded, axis=(0, 1))
        sums = jnp.stack([dgain_one, dgain_two, d_pad]).reshape(3, count, block)
        high = sums.astype(BF)
        rest = (sums - high.astype(F32)).astype(BF)
        input_grad = relative(dh0.astype(BF))
        last = exchange(
            [
                tag(input_grad[k], high[:, k].reshape(-1), rest[:, k].reshape(-1))
                for k in range(count)
            ]
        )
        input_grad = place([h[:local] for h in last])
        sums = jnp.stack([h[local] for h in last]).astype(F32)
        sums = jnp.sum(sums, axis=0)[: 6 * block].reshape(2, 3, block)
        sums = sums[0] + sums[1]
        g_small = sums
        for k in range(1, lanes):
            around = [(i, (i + k) % lanes) for i in range(lanes)]
            g_small = g_small + lax.ppermute(sums, "tensor", around)

        g_down = place([g.astype(F32) for g in g_down])
        g_gate_up = place(
            [
                jnp.stack([g[:, :hid_width], g[:, hid_width:]]).astype(F32)
                for g in g_gate_up
            ]
        )
        g_qkv = place(
            [
                jnp.stack([g[:, j * cols : (j + 1) * cols] for j in range(3)]).astype(F32)
                for g in g_attn
            ]
        )
        g_out = place([g[:, 3 * cols :].T.astype(F32) for g in g_attn])
        return (layer_out, input_grad, g_qkv, g_out, g_gate_up, g_down, g_small[0:2], g_small[2])

    return shards


def spread(body, mesh, dp):
    rows = dp + ("tensor",)
    weights = (
        P(None, None, dp, "tensor"),
        P(None, "tensor", dp),
        P(None, None, dp, "tensor"),
        P(None, "tensor", dp),
        P(None, dp),
        P(dp),
    )
    return jax.shard_map(
        body,
        mesh=mesh,
        in_specs=(P(None, rows, None), P(rows)) + weights + (P(None, rows, None),),
        out_specs=(P(None, rows, None), P(None, rows, None)) + weights,
        check_vma=False,
    )


def solution(mesh):
    dp_size, tensor_size = mesh.shape["dp"], mesh.shape["tensor"]

    def layer(layer_in, *others):
        steps, frames, width = layer_in.shape
        local = frames // (dp_size * tensor_size)
        block = width // dp_size
        fits = 6 * block <= width and 3 * block + local <= width
        if steps == dp_size and dp_size & (dp_size - 1) == 0 and fits:
            body, over, dp = make_step_shards(dp_size, tensor_size), mesh, ("dp",)
        else:
            over = Mesh(
                np.asarray(mesh.devices).reshape(dp_size // 2, 2, tensor_size),
                ("xy", "core", "tensor"),
            )
            body, dp = make_shards(tensor_size), ("xy", "core")
        return spread(body, over, dp)(layer_in, *others)

    return layer
```

```python
import math

import jax
import jax.numpy as jnp
import numpy as np
from jax import lax
from jax.sharding import Mesh
from jax.sharding import PartitionSpec as P

HEAD = 64
EPS = 1e-05
HIGH = lax.Precision.HIGHEST
BF = jnp.bfloat16
F32 = jnp.float32
SWAP = ((0, 1), (1, 0))
TILE = 16


def norm_back(upstream, hval, rstat, gain):
    scaled = upstream * gain
    dgain = jnp.sum(upstream * hval * rstat, axis=(0, 1))
    dhval = rstat * scaled - hval * rstat**3 * jnp.mean(scaled * hval, axis=-1, keepdims=True)
    return (dhval, dgain)


def half(array, axis, which):
    size = array.shape[axis] // 2
    return lax.dynamic_slice_in_dim(array, which * size, size, axis)


def ordered(core, own, other, axis):
    is_first = core == 0
    return jnp.concatenate(
        [jnp.where(is_first, own, other), jnp.where(is_first, other, own)], axis=axis
    )


def make_shards(tensor_size):
    def around(shift):
        return [(i, (i + shift) % tensor_size) for i in range(tensor_size)]

    def trade(core, weight, split_axis, join_axis):
        mine = half(weight, split_axis, core)
        theirs = half(weight, split_axis, 1 - core)
        got = lax.ppermute(theirs, "core", SWAP)
        return ordered(core, mine, got, join_axis)

    def collect(rows):
        parts = [rows] + [
            lax.ppermute(rows, "tensor", around(k)) for k in range(1, tensor_size)
        ]
        near = jnp.stack(parts, axis=1)
        far = lax.ppermute(near, "core", SWAP)
        whole = jnp.concatenate([near, far], axis=1)
        return whole.reshape(rows.shape[0], -1, rows.shape[2])

    def deal(partial):
        steps, frames, width = partial.shape
        split = partial.reshape(steps, 2, tensor_size, frames // (2 * tensor_size), width)
        got = lax.ppermute(split[:, 1].astype(BF), "core", SWAP)
        chip = split[:, 0].astype(F32) + got.astype(F32)
        total = chip[:, 0]
        for k in range(1, tensor_size):
            total = total + lax.ppermute(chip[:, k].astype(BF), "tensor", around(-k)).astype(F32)
        return total

    def shards(
        layer_in, text_mask, w_qkv, w_out, w_gate_up, w_down, norm_gains, pad_row, out_grad
    ):
        core = lax.axis_index("core")
        steps, local_frames, width = layer_in.shape

        w_attn = jnp.concatenate(
            [w_qkv.astype(BF), jnp.swapaxes(w_out, 1, 2)[:, None].astype(BF)], axis=1
        )
        w_attn = lax.all_gather(trade(core, w_attn, 3, 2), "xy", axis=2, tiled=True)
        small = jnp.concatenate([norm_gains, pad_row[None]], axis=0).astype(BF)
        small = lax.all_gather(small, ("xy", "core"), axis=1, tiled=True).astype(F32)
        wgu = lax.all_gather(trade(core, w_gate_up.astype(BF), 3, 2), "xy", axis=2, tiled=True)
        wdown = lax.all_gather(trade(core, w_down.astype(BF), 1, 2), "xy", axis=2, tiled=True)

        gain_one, gain_two, pad_vec = small[0], small[1], small[2]
        maskf = text_mask.astype(F32)
        first = (jnp.arange(steps) == 0).astype(F32)
        h0 = (
            layer_in.astype(F32)
            + first[:, None, None] * (1.0 - maskf)[None, :, None] * pad_vec[None, None, :]
        )
        r1 = lax.rsqrt(jnp.mean(h0 * h0, axis=-1, keepdims=True) + EPS)
        n1 = (h0 * r1 * gain_one).astype(BF)
        n1_all = collect(n1)
        grad_all = collect(out_grad)
        frames = n1_all.shape[1]
        wqkv, wout_t = w_attn[:, :3], w_attn[:, 3]
        qkv = jnp.einsum("sfd,sjde->sjfe", n1_all, wqkv, preferred_element_type=F32).astype(BF)
        col_width = qkv.shape[-1]
        heads = col_width // HEAD
        scale = 1.0 / math.sqrt(HEAD)
        query = qkv[:, 0].reshape(steps, frames, heads, HEAD)
        keyv = qkv[:, 1].reshape(steps, frames, heads, HEAD)
        value = qkv[:, 2].reshape(steps, frames, heads, HEAD)
        causal = jnp.arange(steps)[:, None] >= jnp.arange(steps)[None, :]

        def score_of(qv, kv):
            raw = jnp.einsum("sfhe,tfhe->fhst", qv, kv, preferred_element_type=F32) * scale
            return jnp.where(causal, raw, -1e30)

        scores = score_of(query, keyv)
        top = jnp.max(scores, axis=-1, keepdims=True)
        expo = jnp.exp(scores - top)
        total = jnp.sum(expo, axis=-1, keepdims=True)
        lse = top + jnp.log(total)
        probs_low = (expo / total).astype(BF)
        mixed = jnp.einsum("fhst,tfhe->sfhe", probs_low, value, preferred_element_type=F32)
        mixed = mixed.reshape(steps, frames, col_width).astype(BF)
        attn = deal(jnp.einsum("sfd,sed->sfe", mixed, wout_t, preferred_element_type=F32))
        h1 = h0 + attn
        r2 = lax.rsqrt(jnp.mean(h1 * h1, axis=-1, keepdims=True) + EPS)
        n2 = (h1 * r2 * gain_two).astype(BF)
        n2_all = collect(n2)
        gate_up = jnp.einsum("sfd,sjde->sjfe", n2_all, wgu, preferred_element_type=F32)
        gate = gate_up[:, 0]
        upval = gate_up[:, 1]
        sigma = jax.nn.sigmoid(gate)
        silu_val = gate * sigma
        hidden = (silu_val * upval).astype(BF)
        d_down = jnp.einsum("sfk,sfd->skd", hidden, grad_all, preferred_element_type=F32)
        r_down = lax.psum_scatter(d_down.astype(BF), "xy", scatter_dimension=2, tiled=True)
        d_hidden = jnp.einsum("sfd,skd->sfk", grad_all, wdown, preferred_element_type=F32)
        d_gate = d_hidden * upval * (sigma * (1.0 + gate * (1.0 - sigma)))
        d_up = d_hidden * silu_val
        d_gu = jnp.stack([d_gate, d_up], axis=1).astype(BF)
        d_gate_up = jnp.einsum("sfd,sjfe->sjde", n2_all, d_gu, preferred_element_type=F32)
        r_gate_up = lax.psum_scatter(d_gate_up.astype(BF), "xy", scatter_dimension=2, tiled=True)
        dn2 = deal(jnp.einsum("sjfe,sjde->sfd", d_gu, wgu, preferred_element_type=F32))
        dh_norm2, dgain_two = norm_back(dn2, h1, r2, gain_two)
        dh1 = out_grad.astype(F32) + dh_norm2
        dh1_all = collect(dh1.astype(BF))
        ffout = deal(jnp.einsum("sfk,skd->sfd", hidden, wdown, preferred_element_type=F32))
        layer_out = (h1 + ffout).astype(BF)
        d_out_t = jnp.einsum("sfe,sfd->sed", dh1_all, mixed, preferred_element_type=F32)
        d_mixed = jnp.einsum("sfe,sed->sfd", dh1_all, wout_t, preferred_element_type=F32)
        d_mixed = d_mixed.astype(BF).reshape(steps, frames, heads, HEAD)
        probs = jnp.exp(score_of(query, keyv) - lse)
        d_probs = jnp.einsum("sfhe,tfhe->fhst", d_mixed, value, preferred_element_type=F32)
        d_value = jnp.einsum("fhst,sfhe->tfhe", probs_low, d_mixed, preferred_element_type=F32)
        d_scores = probs * (d_probs - jnp.sum(probs * d_probs, axis=-1, keepdims=True))
        d_query = (
            jnp.einsum("fhst,tfhe->sfhe", d_scores, keyv.astype(F32), precision=HIGH) * scale
        )
        d_key = (
            jnp.einsum("fhst,sfhe->tfhe", d_scores, query.astype(F32), precision=HIGH) * scale
        )
        d_qkv = jnp.stack(
            [
                d_query.reshape(steps, frames, col_width),
                d_key.reshape(steps, frames, col_width),
                d_value.reshape(steps, frames, col_width),
            ],
            axis=1,
        ).astype(BF)
        d_wqkv = jnp.einsum("sfd,sjfe->sjde", n1_all, d_qkv, preferred_element_type=F32)
        d_attn = jnp.concatenate([d_wqkv.astype(BF), d_out_t[:, None].astype(BF)], axis=1)
        r_attn = lax.psum_scatter(d_attn, "xy", scatter_dimension=2, tiled=True)
        dn1 = deal(jnp.einsum("sjfe,sjde->sfd", d_qkv, wqkv, preferred_element_type=F32))
        dh_norm1, dgain_one = norm_back(dn1, h0, r1, gain_one)
        dh0 = dh1 + dh_norm1
        input_grad = dh0.astype(BF)
        d_pad = jnp.sum(dh0[0] * (1.0 - maskf)[:, None], axis=0)
        small_grad = jnp.stack([dgain_one, dgain_two, d_pad], axis=0)
        small_grad = lax.psum(small_grad, ("xy", "core", "tensor"))
        place = lax.axis_index("xy") * 2 + core
        g_small = lax.dynamic_slice_in_dim(
            small_grad, place * pad_row.shape[0], pad_row.shape[0], 1
        )

        def settle(reduced, split_axis, join_axis):
            return trade(core, reduced, split_axis, join_axis).astype(F32)

        g_down = settle(r_down, 2, 1)
        g_gate_up = settle(r_gate_up, 2, 3)
        g_attn = settle(r_attn, 2, 3)
        g_qkv = g_attn[:, :3]
        g_out = jnp.swapaxes(g_attn[:, 3], 1, 2)
        return (layer_out, input_grad, g_qkv, g_out, g_gate_up, g_down, g_small[0:2], g_small[2])

    return shards


def make_step_shards(count, lanes):

    def exchange(blocks):
        return lax.all_to_all(blocks, "dp", 0, 0, tiled=True)

    def collect(rows):
        return lax.all_gather(rows, "tensor", axis=0).reshape(-1, rows.shape[-1])

    def deal(partial):
        slots = partial.astype(BF).reshape(lanes, count, -1, partial.shape[-1])
        return lax.psum_scatter(slots, "tensor", scatter_dimension=0).astype(F32)

    def frame_split(array):
        slots = array.reshape(lanes, count, -1, array.shape[-1])
        slots = jnp.swapaxes(slots, 0, 1)
        return exchange(slots.reshape(count, -1, array.shape[-1]))

    def frame_join(array):
        slots = exchange(array).reshape(count, lanes, -1, array.shape[-1])
        return jnp.swapaxes(slots, 0, 1).reshape(-1, array.shape[-1])

    def after(value, *waiting):
        return lax.optimization_barrier((value,) + waiting)

    def shards(
        layer_in, text_mask, w_qkv, w_out, w_gate_up, w_down, norm_gains, pad_row, out_grad
    ):
        me = lax.axis_index("dp")
        steps, local, width = layer_in.shape
        block = width // count

        def tile(line):
            pads = [(0, 0)] * (line.ndim - 1) + [(0, TILE - 1), (0, width - line.shape[-1])]
            return jnp.pad(line[..., None, :], pads)

        small = jnp.concatenate([norm_gains, pad_row[None]], axis=0).astype(BF).reshape(-1)
        line = jnp.concatenate([small, text_mask.astype(BF)])
        notes = jnp.broadcast_to(tile(line)[None], (count, TILE, width))
        hello = exchange(jnp.concatenate([layer_in, notes], axis=1))
        rows_in = hello[:, :local].astype(F32)
        notes = hello[:, local].astype(F32)
        small = jnp.swapaxes(notes[:, : 3 * block].reshape(count, 3, block), 0, 1)
        gain_one, gain_two, pad_vec = small.reshape(3, width)
        padded = jnp.where(me == 0, 1.0 - notes[:, 3 * block : 3 * block + local], 0.0)[..., None]
        h0 = rows_in + padded * pad_vec
        r1 = lax.rsqrt(jnp.mean(h0 * h0, axis=-1, keepdims=True) + EPS)
        n1 = (h0 * r1 * gain_one).astype(BF)
        n1, w_qkv, w_out = after(n1, w_qkv, w_out)
        n1_all = collect(n1)

        w_attn = jnp.concatenate(
            [w_qkv[:, 0], w_qkv[:, 1], w_qkv[:, 2], jnp.swapaxes(w_out, 1, 2)], axis=2
        )
        w_attn = exchange(w_attn.astype(BF)).reshape(width, -1)
        cols = w_attn.shape[1] // 4
        w_in, wout_t = w_attn[:, : 3 * cols], w_attn[:, 3 * cols :]
        w_attn, out_grad = after(w_attn, out_grad)
        grad = exchange(out_grad)
        grad_all = collect(grad)
        qkv = jnp.dot(n1_all, w_in, preferred_element_type=F32).astype(BF)

        qkv = frame_split(qkv)
        frames = qkv.shape[1]
        heads = cols // HEAD
        scale = 1.0 / math.sqrt(HEAD)
        query = qkv[..., :cols].reshape(steps, frames, heads, HEAD)
        keyv = qkv[..., cols : 2 * cols].reshape(steps, frames, heads, HEAD)
        value = qkv[..., 2 * cols :].reshape(steps, frames, heads, HEAD)
        causal = jnp.arange(steps)[:, None] >= jnp.arange(steps)[None, :]

        def score_of(qv, kv):
            raw = jnp.einsum("sfhe,tfhe->fhst", qv, kv, preferred_element_type=F32) * scale
            return jnp.where(causal, raw, -1e30)

        scores = score_of(query, keyv)
        top = jnp.max(scores, axis=-1, keepdims=True)
        expo = jnp.exp(scores - top)
        total = jnp.sum(expo, axis=-1, keepdims=True)
        lse = top + jnp.log(total)
        probs_low = (expo / total).astype(BF)
        mixed = jnp.einsum("fhst,tfhe->sfhe", probs_low, value, preferred_element_type=F32)
        mixed_all = frame_join(mixed.reshape(steps, frames, cols).astype(BF))
        attn = jnp.einsum("fe,de->fd", mixed_all, wout_t, preferred_element_type=F32)

        attn, w_down = after(attn.astype(BF), w_down)
        attn = deal(attn)
        wdown = exchange(w_down.astype(BF))
        wdown = jnp.swapaxes(wdown, 0, 1).reshape(-1, width)
        h1 = h0 + attn
        r2 = lax.rsqrt(jnp.mean(h1 * h1, axis=-1, keepdims=True) + EPS)
        n2 = (h1 * r2 * gain_two).astype(BF)
        n2, w_gate_up = after(n2, w_gate_up)
        n2_all = collect(n2)
        wgu = jnp.concatenate([w_gate_up[:, 0], w_gate_up[:, 1]], axis=2).astype(BF)
        wgu = exchange(wgu).reshape(width, -1)

        gate_up = jnp.dot(n2_all, wgu, preferred_element_type=F32)
        hid_width = gate_up.shape[1] // 2
        gate, upval = gate_up[:, :hid_width], gate_up[:, hid_width:]
        sigma = jax.nn.sigmoid(gate)
        silu_val = gate * sigma
        hidden = (silu_val * upval).astype(BF)
        d_hidden = jnp.einsum("fd,kd->fk", grad_all, wdown, preferred_element_type=F32)
        d_gate = d_hidden * upval * (sigma * (1.0 + gate * (1.0 - sigma)))
        d_up = d_hidden * silu_val
        d_gu = jnp.concatenate([d_gate, d_up], axis=1).astype(BF)
        dn2 = jnp.einsum("fk,dk->fd", d_gu, wgu, preferred_element_type=F32).astype(BF)

        dn2, hidden = after(dn2, hidden)
        dn2 = deal(dn2)
        d_down = jnp.einsum(
            "fk,frd->rkd",
            hidden,
            grad_all.reshape(-1, count, block),
            preferred_element_type=F32,
        )
        g_down = exchange(d_down.astype(BF)).astype(F32)
        dh_norm2, dgain_two = norm_back(dn2, h1, r2, gain_two)
        dh1 = grad.astype(F32) + dh_norm2
        dh1_low, d_gu, hidden = after(dh1.astype(BF), d_gu, hidden)
        dh1_all = collect(dh1_low)
        d_gate_up = jnp.einsum("fd,fk->dk", n2_all, d_gu, preferred_element_type=F32)
        g_gate_up = exchange(d_gate_up.astype(BF).reshape(count, block, -1))
        g_gate_up = jnp.stack([g_gate_up[..., :hid_width], g_gate_up[..., hid_width:]], axis=1)
        g_gate_up = g_gate_up.astype(F32)

        ffout = deal(jnp.dot(hidden, wdown, preferred_element_type=F32))
        d_mixed = jnp.dot(dh1_all, wout_t, preferred_element_type=F32).astype(BF)
        d_mixed = frame_split(d_mixed).reshape(steps, frames, heads, HEAD)
        probs = jnp.exp(score_of(query, keyv) - lse)
        d_probs = jnp.einsum("sfhe,tfhe->fhst", d_mixed, value, preferred_element_type=F32)
        d_value = jnp.einsum("fhst,sfhe->tfhe", probs_low, d_mixed, preferred_element_type=F32)
        d_scores = probs * (d_probs - jnp.sum(probs * d_probs, axis=-1, keepdims=True))
        d_query = (
            jnp.einsum("fhst,tfhe->sfhe", d_scores, keyv.astype(F32), precision=HIGH) * scale
        )
        d_key = (
            jnp.einsum("fhst,sfhe->tfhe", d_scores, query.astype(F32), precision=HIGH) * scale
        )
        d_qkv = jnp.concatenate(
            [a.reshape(steps, frames, cols).astype(BF) for a in (d_query, d_key, d_value)],
            axis=-1,
        )
        d_qkv = frame_join(d_qkv)
        dn1 = jnp.einsum("fe,de->fd", d_qkv, w_in, preferred_element_type=F32).astype(BF)

        dn1, d_qkv, ffout = after(dn1, d_qkv, ffout)
        dn1 = deal(dn1)
        d_attn = jnp.concatenate(
            [
                jnp.einsum("fd,fe->de", n1_all, d_qkv, preferred_element_type=F32).astype(BF),
                jnp.einsum("fd,fe->de", dh1_all, mixed_all, preferred_element_type=F32).astype(BF),
            ],
            axis=1,
        )
        g_attn = exchange(d_attn.reshape(count, block, -1)).astype(F32)
        g_qkv = jnp.stack([g_attn[..., j * cols : (j + 1) * cols] for j in range(3)], axis=1)
        g_out = jnp.swapaxes(g_attn[..., 3 * cols :], 1, 2)
        layer_out = exchange((h1 + ffout).astype(BF))

        dh_norm1, dgain_one = norm_back(dn1, h0, r1, gain_one)
        dh0 = dh1 + dh_norm1
        d_pad = jnp.sum(dh0 * padded, axis=(0, 1))
        sums = jnp.stack([dgain_one, dgain_two, d_pad]).reshape(3, count, block)
        sums = jnp.swapaxes(sums, 0, 1).reshape(count, -1)
        high = sums.astype(BF)
        rest = (sums - high.astype(F32)).astype(BF)
        notes = tile(jnp.concatenate([high, rest], axis=1))
        last = exchange(jnp.concatenate([dh0.astype(BF), notes], axis=1))
        input_grad = last[:, :local]
        sums = jnp.sum(last[:, local].astype(F32), axis=0)[: 6 * block].reshape(2, 3, block)
        sums = sums[0] + sums[1]
        g_small = sums
        for k in range(1, lanes):
            around = [(i, (i + k) % lanes) for i in range(lanes)]
            g_small = g_small + lax.ppermute(sums, "tensor", around)
        return (layer_out, input_grad, g_qkv, g_out, g_gate_up, g_down, g_small[0:2], g_small[2])

    return shards


def spread(body, mesh, dp):
    rows = dp + ("tensor",)
    weights = (
        P(None, None, dp, "tensor"),
        P(None, "tensor", dp),
        P(None, None, dp, "tensor"),
        P(None, "tensor", dp),
        P(None, dp),
        P(dp),
    )
    return jax.shard_map(
        body,
        mesh=mesh,
        in_specs=(P(None, rows, None), P(rows)) + weights + (P(None, rows, None),),
        out_specs=(P(None, rows, None), P(None, rows, None)) + weights,
        check_vma=False,
    )


def solution(mesh):
    dp_size, tensor_size = mesh.shape["dp"], mesh.shape["tensor"]

    def layer(layer_in, *others):
        steps, frames, width = layer_in.shape
        local = frames // (dp_size * tensor_size)
        block = width // dp_size
        fits = 6 * block <= width and 3 * block + local <= width
        if steps == dp_size and dp_size & (dp_size - 1) == 0 and fits:
            body, over, dp = make_step_shards(dp_size, tensor_size), mesh, ("dp",)
        else:
            over = Mesh(
                np.asarray(mesh.devices).reshape(dp_size // 2, 2, tensor_size),
                ("xy", "core", "tensor"),
            )
            body, dp = make_shards(tensor_size), ("xy", "core")
        return spread(body, over, dp)(layer_in, *others)

    return layer
```

```python
import math

import jax
import jax.numpy as jnp
import numpy as np
from jax import lax
from jax.sharding import Mesh
from jax.sharding import PartitionSpec as P

HEAD = 64
EPS = 1e-05
HIGH = lax.Precision.HIGHEST
BF = jnp.bfloat16
F32 = jnp.float32
SWAP = ((0, 1), (1, 0))
TILE = 16


def norm_back(upstream, hval, rstat, gain):
    scaled = upstream * gain
    dgain = jnp.sum(upstream * hval * rstat, axis=(0, 1))
    dhval = rstat * scaled - hval * rstat**3 * jnp.mean(scaled * hval, axis=-1, keepdims=True)
    return (dhval, dgain)


def half(array, axis, which):
    size = array.shape[axis] // 2
    return lax.dynamic_slice_in_dim(array, which * size, size, axis)


def ordered(core, own, other, axis):
    is_first = core == 0
    return jnp.concatenate(
        [jnp.where(is_first, own, other), jnp.where(is_first, other, own)], axis=axis
    )


def make_shards(tensor_size):
    def around(shift):
        return [(i, (i + shift) % tensor_size) for i in range(tensor_size)]

    def trade(core, weight, split_axis, join_axis):
        mine = half(weight, split_axis, core)
        theirs = half(weight, split_axis, 1 - core)
        got = lax.ppermute(theirs, "core", SWAP)
        return ordered(core, mine, got, join_axis)

    def collect(rows):
        parts = [rows] + [
            lax.ppermute(rows, "tensor", around(k)) for k in range(1, tensor_size)
        ]
        near = jnp.stack(parts, axis=1)
        far = lax.ppermute(near, "core", SWAP)
        whole = jnp.concatenate([near, far], axis=1)
        return whole.reshape(rows.shape[0], -1, rows.shape[2])

    def deal(partial):
        steps, frames, width = partial.shape
        split = partial.reshape(steps, 2, tensor_size, frames // (2 * tensor_size), width)
        got = lax.ppermute(split[:, 1].astype(BF), "core", SWAP)
        chip = split[:, 0].astype(F32) + got.astype(F32)
        total = chip[:, 0]
        for k in range(1, tensor_size):
            total = total + lax.ppermute(chip[:, k].astype(BF), "tensor", around(-k)).astype(F32)
        return total

    def shards(
        layer_in, text_mask, w_qkv, w_out, w_gate_up, w_down, norm_gains, pad_row, out_grad
    ):
        core = lax.axis_index("core")
        steps, local_frames, width = layer_in.shape

        w_attn = jnp.concatenate(
            [w_qkv.astype(BF), jnp.swapaxes(w_out, 1, 2)[:, None].astype(BF)], axis=1
        )
        w_attn = lax.all_gather(trade(core, w_attn, 3, 2), "xy", axis=2, tiled=True)
        small = jnp.concatenate([norm_gains, pad_row[None]], axis=0).astype(BF)
        small = lax.all_gather(small, ("xy", "core"), axis=1, tiled=True).astype(F32)
        wgu = lax.all_gather(trade(core, w_gate_up.astype(BF), 3, 2), "xy", axis=2, tiled=True)
        wdown = lax.all_gather(trade(core, w_down.astype(BF), 1, 2), "xy", axis=2, tiled=True)

        gain_one, gain_two, pad_vec = small[0], small[1], small[2]
        maskf = text_mask.astype(F32)
        first = (jnp.arange(steps) == 0).astype(F32)
        h0 = (
            layer_in.astype(F32)
            + first[:, None, None] * (1.0 - maskf)[None, :, None] * pad_vec[None, None, :]
        )
        r1 = lax.rsqrt(jnp.mean(h0 * h0, axis=-1, keepdims=True) + EPS)
        n1 = (h0 * r1 * gain_one).astype(BF)
        n1_all = collect(n1)
        grad_all = collect(out_grad)
        frames = n1_all.shape[1]
        wqkv, wout_t = w_attn[:, :3], w_attn[:, 3]
        qkv = jnp.einsum("sfd,sjde->sjfe", n1_all, wqkv, preferred_element_type=F32).astype(BF)
        col_width = qkv.shape[-1]
        heads = col_width // HEAD
        scale = 1.0 / math.sqrt(HEAD)
        query = qkv[:, 0].reshape(steps, frames, heads, HEAD)
        keyv = qkv[:, 1].reshape(steps, frames, heads, HEAD)
        value = qkv[:, 2].reshape(steps, frames, heads, HEAD)
        causal = jnp.arange(steps)[:, None] >= jnp.arange(steps)[None, :]

        def score_of(qv, kv):
            raw = jnp.einsum("sfhe,tfhe->fhst", qv, kv, preferred_element_type=F32) * scale
            return jnp.where(causal, raw, -1e30)

        scores = score_of(query, keyv)
        top = jnp.max(scores, axis=-1, keepdims=True)
        expo = jnp.exp(scores - top)
        total = jnp.sum(expo, axis=-1, keepdims=True)
        lse = top + jnp.log(total)
        probs_low = (expo / total).astype(BF)
        mixed = jnp.einsum("fhst,tfhe->sfhe", probs_low, value, preferred_element_type=F32)
        mixed = mixed.reshape(steps, frames, col_width).astype(BF)
        attn = deal(jnp.einsum("sfd,sed->sfe", mixed, wout_t, preferred_element_type=F32))
        h1 = h0 + attn
        r2 = lax.rsqrt(jnp.mean(h1 * h1, axis=-1, keepdims=True) + EPS)
        n2 = (h1 * r2 * gain_two).astype(BF)
        n2_all = collect(n2)
        gate_up = jnp.einsum("sfd,sjde->sjfe", n2_all, wgu, preferred_element_type=F32)
        gate = gate_up[:, 0]
        upval = gate_up[:, 1]
        sigma = jax.nn.sigmoid(gate)
        silu_val = gate * sigma
        hidden = (silu_val * upval).astype(BF)
        d_down = jnp.einsum("sfk,sfd->skd", hidden, grad_all, preferred_element_type=F32)
        r_down = lax.psum_scatter(d_down.astype(BF), "xy", scatter_dimension=2, tiled=True)
        d_hidden = jnp.einsum("sfd,skd->sfk", grad_all, wdown, preferred_element_type=F32)
        d_gate = d_hidden * upval * (sigma * (1.0 + gate * (1.0 - sigma)))
        d_up = d_hidden * silu_val
        d_gu = jnp.stack([d_gate, d_up], axis=1).astype(BF)
        d_gate_up = jnp.einsum("sfd,sjfe->sjde", n2_all, d_gu, preferred_element_type=F32)
        r_gate_up = lax.psum_scatter(d_gate_up.astype(BF), "xy", scatter_dimension=2, tiled=True)
        dn2 = deal(jnp.einsum("sjfe,sjde->sfd", d_gu, wgu, preferred_element_type=F32))
        dh_norm2, dgain_two = norm_back(dn2, h1, r2, gain_two)
        dh1 = out_grad.astype(F32) + dh_norm2
        dh1_all = collect(dh1.astype(BF))
        ffout = deal(jnp.einsum("sfk,skd->sfd", hidden, wdown, preferred_element_type=F32))
        layer_out = (h1 + ffout).astype(BF)
        d_out_t = jnp.einsum("sfe,sfd->sed", dh1_all, mixed, preferred_element_type=F32)
        d_mixed = jnp.einsum("sfe,sed->sfd", dh1_all, wout_t, preferred_element_type=F32)
        d_mixed = d_mixed.astype(BF).reshape(steps, frames, heads, HEAD)
        probs = jnp.exp(score_of(query, keyv) - lse)
        d_probs = jnp.einsum("sfhe,tfhe->fhst", d_mixed, value, preferred_element_type=F32)
        d_value = jnp.einsum("fhst,sfhe->tfhe", probs_low, d_mixed, preferred_element_type=F32)
        d_scores = probs * (d_probs - jnp.sum(probs * d_probs, axis=-1, keepdims=True))
        d_query = (
            jnp.einsum("fhst,tfhe->sfhe", d_scores, keyv.astype(F32), precision=HIGH) * scale
        )
        d_key = (
            jnp.einsum("fhst,sfhe->tfhe", d_scores, query.astype(F32), precision=HIGH) * scale
        )
        d_qkv = jnp.stack(
            [
                d_query.reshape(steps, frames, col_width),
                d_key.reshape(steps, frames, col_width),
                d_value.reshape(steps, frames, col_width),
            ],
            axis=1,
        ).astype(BF)
        d_wqkv = jnp.einsum("sfd,sjfe->sjde", n1_all, d_qkv, preferred_element_type=F32)
        d_attn = jnp.concatenate([d_wqkv.astype(BF), d_out_t[:, None].astype(BF)], axis=1)
        r_attn = lax.psum_scatter(d_attn, "xy", scatter_dimension=2, tiled=True)
        dn1 = deal(jnp.einsum("sjfe,sjde->sfd", d_qkv, wqkv, preferred_element_type=F32))
        dh_norm1, dgain_one = norm_back(dn1, h0, r1, gain_one)
        dh0 = dh1 + dh_norm1
        input_grad = dh0.astype(BF)
        d_pad = jnp.sum(dh0[0] * (1.0 - maskf)[:, None], axis=0)
        small_grad = jnp.stack([dgain_one, dgain_two, d_pad], axis=0)
        small_grad = lax.psum(small_grad, ("xy", "core", "tensor"))
        place = lax.axis_index("xy") * 2 + core
        g_small = lax.dynamic_slice_in_dim(
            small_grad, place * pad_row.shape[0], pad_row.shape[0], 1
        )

        def settle(reduced, split_axis, join_axis):
            return trade(core, reduced, split_axis, join_axis).astype(F32)

        g_down = settle(r_down, 2, 1)
        g_gate_up = settle(r_gate_up, 2, 3)
        g_attn = settle(r_attn, 2, 3)
        g_qkv = g_attn[:, :3]
        g_out = jnp.swapaxes(g_attn[:, 3], 1, 2)
        return (layer_out, input_grad, g_qkv, g_out, g_gate_up, g_down, g_small[0:2], g_small[2])

    return shards


def make_step_shards(count, lanes):

    def exchange(blocks):
        return lax.all_to_all(blocks, "dp", 0, 0, tiled=True)

    def collect(rows):
        return lax.all_gather(rows, "tensor", axis=0).reshape(-1, rows.shape[-1])

    def deal(partial):
        slots = partial.astype(BF).reshape(lanes, count, -1, partial.shape[-1])
        return lax.psum_scatter(slots, "tensor", scatter_dimension=0).astype(F32)

    def frame_split(array):
        slots = array.reshape(lanes, count, -1, array.shape[-1])
        slots = jnp.swapaxes(slots, 0, 1)
        return exchange(slots.reshape(count, -1, array.shape[-1]))

    def frame_join(array):
        slots = exchange(array).reshape(count, lanes, -1, array.shape[-1])
        return jnp.swapaxes(slots, 0, 1).reshape(-1, array.shape[-1])

    def after(value, *waiting):
        return lax.optimization_barrier((value,) + waiting)

    def shards(
        layer_in, text_mask, w_qkv, w_out, w_gate_up, w_down, norm_gains, pad_row, out_grad
    ):
        me = lax.axis_index("dp")
        steps, local, width = layer_in.shape
        block = width // count

        def tile(line):
            pads = [(0, 0)] * (line.ndim - 1) + [(0, TILE - 1), (0, width - line.shape[-1])]
            return jnp.pad(line[..., None, :], pads)

        small = jnp.concatenate([norm_gains, pad_row[None]], axis=0).astype(BF).reshape(-1)
        line = jnp.concatenate([small, text_mask.astype(BF)])
        notes = jnp.broadcast_to(tile(line)[None], (count, TILE, width))
        hello = exchange(jnp.concatenate([layer_in, notes], axis=1))
        rows_in = hello[:, :local].astype(F32)
        notes = hello[:, local].astype(F32)
        small = jnp.swapaxes(notes[:, : 3 * block].reshape(count, 3, block), 0, 1)
        gain_one, gain_two, pad_vec = small.reshape(3, width)
        padded = jnp.where(me == 0, 1.0 - notes[:, 3 * block : 3 * block + local], 0.0)[..., None]
        h0 = rows_in + padded * pad_vec
        r1 = lax.rsqrt(jnp.mean(h0 * h0, axis=-1, keepdims=True) + EPS)
        n1 = (h0 * r1 * gain_one).astype(BF)
        n1, w_qkv, w_out = after(n1, w_qkv, w_out)
        n1_all = collect(n1)

        w_attn = jnp.concatenate(
            [w_qkv[:, 0], w_qkv[:, 1], w_qkv[:, 2], jnp.swapaxes(w_out, 1, 2)], axis=2
        )
        w_attn = exchange(w_attn.astype(BF)).reshape(width, -1)
        cols = w_attn.shape[1] // 4
        w_in, wout_t = w_attn[:, : 3 * cols], w_attn[:, 3 * cols :]
        w_attn, out_grad = after(w_attn, out_grad)
        grad = exchange(out_grad)
        n1_all, grad = after(n1_all, grad)
        grad_all = collect(grad)
        qkv = jnp.dot(n1_all, w_in, preferred_element_type=F32).astype(BF)

        qkv = frame_split(qkv)
        frames = qkv.shape[1]
        heads = cols // HEAD
        scale = 1.0 / math.sqrt(HEAD)
        query = qkv[..., :cols].reshape(steps, frames, heads, HEAD)
        keyv = qkv[..., cols : 2 * cols].reshape(steps, frames, heads, HEAD)
        value = qkv[..., 2 * cols :].reshape(steps, frames, heads, HEAD)
        causal = jnp.arange(steps)[:, None] >= jnp.arange(steps)[None, :]

        def score_of(qv, kv):
            raw = jnp.einsum("sfhe,tfhe->fhst", qv, kv, preferred_element_type=F32) * scale
            return jnp.where(causal, raw, -1e30)

        scores = score_of(query, keyv)
        top = jnp.max(scores, axis=-1, keepdims=True)
        expo = jnp.exp(scores - top)
        total = jnp.sum(expo, axis=-1, keepdims=True)
        lse = top + jnp.log(total)
        probs_low = (expo / total).astype(BF)
        mixed = jnp.einsum("fhst,tfhe->sfhe", probs_low, value, preferred_element_type=F32)
        mixed_all = frame_join(mixed.reshape(steps, frames, cols).astype(BF))
        attn = jnp.einsum("fe,de->fd", mixed_all, wout_t, preferred_element_type=F32)

        attn, w_down, w_gate_up, grad_all = after(attn.astype(BF), w_down, w_gate_up, grad_all)
        attn = deal(attn)
        wdown = exchange(w_down.astype(BF))
        wgu = jnp.concatenate([w_gate_up[:, 0], w_gate_up[:, 1]], axis=2).astype(BF)
        attn, wdown, wgu = after(attn, wdown, wgu)
        wdown = jnp.swapaxes(wdown, 0, 1).reshape(-1, width)
        h1 = h0 + attn
        r2 = lax.rsqrt(jnp.mean(h1 * h1, axis=-1, keepdims=True) + EPS)
        n2 = (h1 * r2 * gain_two).astype(BF)
        n2, wgu = after(n2, wgu)
        n2_all = collect(n2)
        wgu = exchange(wgu).reshape(width, -1)

        gate_up = jnp.dot(n2_all, wgu, preferred_element_type=F32)
        hid_width = gate_up.shape[1] // 2
        gate, upval = gate_up[:, :hid_width], gate_up[:, hid_width:]
        sigma = jax.nn.sigmoid(gate)
        silu_val = gate * sigma
        hidden = (silu_val * upval).astype(BF)
        d_hidden = jnp.einsum("fd,kd->fk", grad_all, wdown, preferred_element_type=F32)
        d_gate = (d_hidden * upval * (sigma * (1.0 + gate * (1.0 - sigma)))).astype(BF)
        d_up = (d_hidden * silu_val).astype(BF)
        wgate, wup = wgu[:, :hid_width], wgu[:, hid_width:]
        dn2 = jnp.einsum("fk,dk->fd", d_gate, wgate, preferred_element_type=F32)
        dn2 = dn2 + jnp.einsum("fk,dk->fd", d_up, wup, preferred_element_type=F32)

        dn2, hidden, d_gate, d_up = after(dn2.astype(BF), hidden, d_gate, d_up)
        dn2 = deal(dn2)
        d_down = jnp.einsum(
            "fk,frd->rkd",
            hidden,
            grad_all.reshape(-1, count, block),
            preferred_element_type=F32,
        )
        g_down = exchange(d_down.astype(BF))
        g_gate = jnp.einsum("fd,fk->dk", n2_all, d_gate, preferred_element_type=F32).astype(BF)
        g_up = jnp.einsum("fd,fk->dk", n2_all, d_up, preferred_element_type=F32).astype(BF)
        dn2, g_down, g_gate, g_up = after(dn2, g_down, g_gate, g_up)
        dh_norm2, dgain_two = norm_back(dn2, h1, r2, gain_two)
        dh1 = grad.astype(F32) + dh_norm2
        dh1_low, g_gate, hidden = after(dh1.astype(BF), g_gate, hidden)
        dh1_all = collect(dh1_low)
        g_gate = exchange(g_gate.reshape(count, block, -1))
        dh1_all, g_gate = after(dh1_all, g_gate)

        ffout = deal(jnp.dot(hidden, wdown, preferred_element_type=F32))
        d_mixed = jnp.dot(dh1_all, wout_t, preferred_element_type=F32).astype(BF)
        d_mixed, g_up = after(frame_split(d_mixed), g_up)
        d_mixed = d_mixed.reshape(steps, frames, heads, HEAD)
        g_up = exchange(g_up.reshape(count, block, -1))
        probs = jnp.exp(score_of(query, keyv) - lse)
        d_probs = jnp.einsum("sfhe,tfhe->fhst", d_mixed, value, preferred_element_type=F32)
        d_value = jnp.einsum("fhst,sfhe->tfhe", probs_low, d_mixed, preferred_element_type=F32)
        d_scores = probs * (d_probs - jnp.sum(probs * d_probs, axis=-1, keepdims=True))
        d_query = (
            jnp.einsum("fhst,tfhe->sfhe", d_scores, keyv.astype(F32), precision=HIGH) * scale
        )
        d_key = (
            jnp.einsum("fhst,sfhe->tfhe", d_scores, query.astype(F32), precision=HIGH) * scale
        )
        d_qkv = jnp.concatenate(
            [a.reshape(steps, frames, cols).astype(BF) for a in (d_query, d_key, d_value)],
            axis=-1,
        )
        d_qkv, g_up = after(d_qkv, g_up)
        g_gate_up = jnp.stack([g_gate, g_up], axis=1).astype(F32)
        d_qkv = frame_join(d_qkv)
        dn1 = jnp.einsum("fe,de->fd", d_qkv, w_in, preferred_element_type=F32).astype(BF)

        dn1, d_qkv, ffout = after(dn1, d_qkv, ffout)
        dn1 = deal(dn1)
        d_attn = jnp.concatenate(
            [
                jnp.einsum("fd,fe->de", n1_all, d_qkv, preferred_element_type=F32).astype(BF),
                jnp.einsum("fd,fe->de", dh1_all, mixed_all, preferred_element_type=F32).astype(BF),
            ],
            axis=1,
        )
        g_attn = exchange(d_attn.reshape(count, block, -1))
        layer_out = exchange((h1 + ffout).astype(BF))
        dn1, g_attn, layer_out = after(dn1, g_attn, layer_out)
        g_down, g_attn = g_down.astype(F32), g_attn.astype(F32)
        g_qkv = jnp.stack([g_attn[..., j * cols : (j + 1) * cols] for j in range(3)], axis=1)
        g_out = jnp.swapaxes(g_attn[..., 3 * cols :], 1, 2)

        dh_norm1, dgain_one = norm_back(dn1, h0, r1, gain_one)
        dh0 = dh1 + dh_norm1
        d_pad = jnp.sum(dh0 * padded, axis=(0, 1))
        sums = jnp.stack([dgain_one, dgain_two, d_pad]).reshape(3, count, block)
        sums = jnp.swapaxes(sums, 0, 1).reshape(count, -1)
        high = sums.astype(BF)
        rest = (sums - high.astype(F32)).astype(BF)
        notes = tile(jnp.concatenate([high, rest], axis=1))
        last = exchange(jnp.concatenate([dh0.astype(BF), notes], axis=1))
        input_grad = last[:, :local]
        sums = jnp.sum(last[:, local].astype(F32), axis=0)[: 6 * block].reshape(2, 3, block)
        sums = sums[0] + sums[1]
        g_small = sums
        for k in range(1, lanes):
            around = [(i, (i + k) % lanes) for i in range(lanes)]
            g_small = g_small + lax.ppermute(sums, "tensor", around)
        return (layer_out, input_grad, g_qkv, g_out, g_gate_up, g_down, g_small[0:2], g_small[2])

    return shards


def spread(body, mesh, dp):
    rows = dp + ("tensor",)
    weights = (
        P(None, None, dp, "tensor"),
        P(None, "tensor", dp),
        P(None, None, dp, "tensor"),
        P(None, "tensor", dp),
        P(None, dp),
        P(dp),
    )
    return jax.shard_map(
        body,
        mesh=mesh,
        in_specs=(P(None, rows, None), P(rows)) + weights + (P(None, rows, None),),
        out_specs=(P(None, rows, None), P(None, rows, None)) + weights,
        check_vma=False,
    )


def solution(mesh):
    dp_size, tensor_size = mesh.shape["dp"], mesh.shape["tensor"]

    def layer(layer_in, *others):
        steps, frames, width = layer_in.shape
        local = frames // (dp_size * tensor_size)
        block = width // dp_size
        fits = 6 * block <= width and 3 * block + local <= width
        if steps == dp_size and dp_size & (dp_size - 1) == 0 and fits:
            body, over, dp = make_step_shards(dp_size, tensor_size), mesh, ("dp",)
        else:
            over = Mesh(
                np.asarray(mesh.devices).reshape(dp_size // 2, 2, tensor_size),
                ("xy", "core", "tensor"),
            )
            body, dp = make_shards(tensor_size), ("xy", "core")
        return spread(body, over, dp)(layer_in, *others)

    return layer
```

```python
import math

import jax
import jax.numpy as jnp
import numpy as np
from jax import lax
from jax.sharding import Mesh
from jax.sharding import PartitionSpec as P

HEAD = 64
EPS = 1e-05
HIGH = lax.Precision.HIGHEST
BF = jnp.bfloat16
F32 = jnp.float32
SWAP = ((0, 1), (1, 0))
TILE = 16


def norm_back(upstream, hval, rstat, gain):
    scaled = upstream * gain
    dgain = jnp.sum(upstream * hval * rstat, axis=(0, 1))
    dhval = rstat * scaled - hval * rstat**3 * jnp.mean(scaled * hval, axis=-1, keepdims=True)
    return (dhval, dgain)


def half(array, axis, which):
    size = array.shape[axis] // 2
    return lax.dynamic_slice_in_dim(array, which * size, size, axis)


def ordered(core, own, other, axis):
    is_first = core == 0
    return jnp.concatenate(
        [jnp.where(is_first, own, other), jnp.where(is_first, other, own)], axis=axis
    )


def make_shards(tensor_size):
    def around(shift):
        return [(i, (i + shift) % tensor_size) for i in range(tensor_size)]

    def trade(core, weight, split_axis, join_axis):
        mine = half(weight, split_axis, core)
        theirs = half(weight, split_axis, 1 - core)
        got = lax.ppermute(theirs, "core", SWAP)
        return ordered(core, mine, got, join_axis)

    def collect(rows):
        parts = [rows] + [
            lax.ppermute(rows, "tensor", around(k)) for k in range(1, tensor_size)
        ]
        near = jnp.stack(parts, axis=1)
        far = lax.ppermute(near, "core", SWAP)
        whole = jnp.concatenate([near, far], axis=1)
        return whole.reshape(rows.shape[0], -1, rows.shape[2])

    def deal(partial):
        steps, frames, width = partial.shape
        split = partial.reshape(steps, 2, tensor_size, frames // (2 * tensor_size), width)
        got = lax.ppermute(split[:, 1].astype(BF), "core", SWAP)
        chip = split[:, 0].astype(F32) + got.astype(F32)
        total = chip[:, 0]
        for k in range(1, tensor_size):
            total = total + lax.ppermute(chip[:, k].astype(BF), "tensor", around(-k)).astype(F32)
        return total

    def shards(
        layer_in, text_mask, w_qkv, w_out, w_gate_up, w_down, norm_gains, pad_row, out_grad
    ):
        core = lax.axis_index("core")
        steps, local_frames, width = layer_in.shape

        w_attn = jnp.concatenate(
            [w_qkv.astype(BF), jnp.swapaxes(w_out, 1, 2)[:, None].astype(BF)], axis=1
        )
        w_attn = lax.all_gather(trade(core, w_attn, 3, 2), "xy", axis=2, tiled=True)
        small = jnp.concatenate([norm_gains, pad_row[None]], axis=0).astype(BF)
        small = lax.all_gather(small, ("xy", "core"), axis=1, tiled=True).astype(F32)
        wgu = lax.all_gather(trade(core, w_gate_up.astype(BF), 3, 2), "xy", axis=2, tiled=True)
        wdown = lax.all_gather(trade(core, w_down.astype(BF), 1, 2), "xy", axis=2, tiled=True)

        gain_one, gain_two, pad_vec = small[0], small[1], small[2]
        maskf = text_mask.astype(F32)
        first = (jnp.arange(steps) == 0).astype(F32)
        h0 = (
            layer_in.astype(F32)
            + first[:, None, None] * (1.0 - maskf)[None, :, None] * pad_vec[None, None, :]
        )
        r1 = lax.rsqrt(jnp.mean(h0 * h0, axis=-1, keepdims=True) + EPS)
        n1 = (h0 * r1 * gain_one).astype(BF)
        n1_all = collect(n1)
        grad_all = collect(out_grad)
        frames = n1_all.shape[1]
        wqkv, wout_t = w_attn[:, :3], w_attn[:, 3]
        qkv = jnp.einsum("sfd,sjde->sjfe", n1_all, wqkv, preferred_element_type=F32).astype(BF)
        col_width = qkv.shape[-1]
        heads = col_width // HEAD
        scale = 1.0 / math.sqrt(HEAD)
        query = qkv[:, 0].reshape(steps, frames, heads, HEAD)
        keyv = qkv[:, 1].reshape(steps, frames, heads, HEAD)
        value = qkv[:, 2].reshape(steps, frames, heads, HEAD)
        causal = jnp.arange(steps)[:, None] >= jnp.arange(steps)[None, :]

        def score_of(qv, kv):
            raw = jnp.einsum("sfhe,tfhe->fhst", qv, kv, preferred_element_type=F32) * scale
            return jnp.where(causal, raw, -1e30)

        scores = score_of(query, keyv)
        top = jnp.max(scores, axis=-1, keepdims=True)
        expo = jnp.exp(scores - top)
        total = jnp.sum(expo, axis=-1, keepdims=True)
        lse = top + jnp.log(total)
        probs_low = (expo / total).astype(BF)
        mixed = jnp.einsum("fhst,tfhe->sfhe", probs_low, value, preferred_element_type=F32)
        mixed = mixed.reshape(steps, frames, col_width).astype(BF)
        attn = deal(jnp.einsum("sfd,sed->sfe", mixed, wout_t, preferred_element_type=F32))
        h1 = h0 + attn
        r2 = lax.rsqrt(jnp.mean(h1 * h1, axis=-1, keepdims=True) + EPS)
        n2 = (h1 * r2 * gain_two).astype(BF)
        n2_all = collect(n2)
        gate_up = jnp.einsum("sfd,sjde->sjfe", n2_all, wgu, preferred_element_type=F32)
        gate = gate_up[:, 0]
        upval = gate_up[:, 1]
        sigma = jax.nn.sigmoid(gate)
        silu_val = gate * sigma
        hidden = (silu_val * upval).astype(BF)
        d_down = jnp.einsum("sfk,sfd->skd", hidden, grad_all, preferred_element_type=F32)
        r_down = lax.psum_scatter(d_down.astype(BF), "xy", scatter_dimension=2, tiled=True)
        d_hidden = jnp.einsum("sfd,skd->sfk", grad_all, wdown, preferred_element_type=F32)
        d_gate = d_hidden * upval * (sigma * (1.0 + gate * (1.0 - sigma)))
        d_up = d_hidden * silu_val
        d_gu = jnp.stack([d_gate, d_up], axis=1).astype(BF)
        d_gate_up = jnp.einsum("sfd,sjfe->sjde", n2_all, d_gu, preferred_element_type=F32)
        r_gate_up = lax.psum_scatter(d_gate_up.astype(BF), "xy", scatter_dimension=2, tiled=True)
        dn2 = deal(jnp.einsum("sjfe,sjde->sfd", d_gu, wgu, preferred_element_type=F32))
        dh_norm2, dgain_two = norm_back(dn2, h1, r2, gain_two)
        dh1 = out_grad.astype(F32) + dh_norm2
        dh1_all = collect(dh1.astype(BF))
        ffout = deal(jnp.einsum("sfk,skd->sfd", hidden, wdown, preferred_element_type=F32))
        layer_out = (h1 + ffout).astype(BF)
        d_out_t = jnp.einsum("sfe,sfd->sed", dh1_all, mixed, preferred_element_type=F32)
        d_mixed = jnp.einsum("sfe,sed->sfd", dh1_all, wout_t, preferred_element_type=F32)
        d_mixed = d_mixed.astype(BF).reshape(steps, frames, heads, HEAD)
        probs = jnp.exp(score_of(query, keyv) - lse)
        d_probs = jnp.einsum("sfhe,tfhe->fhst", d_mixed, value, preferred_element_type=F32)
        d_value = jnp.einsum("fhst,sfhe->tfhe", probs_low, d_mixed, preferred_element_type=F32)
        d_scores = probs * (d_probs - jnp.sum(probs * d_probs, axis=-1, keepdims=True))
        d_query = (
            jnp.einsum("fhst,tfhe->sfhe", d_scores, keyv.astype(F32), precision=HIGH) * scale
        )
        d_key = (
            jnp.einsum("fhst,sfhe->tfhe", d_scores, query.astype(F32), precision=HIGH) * scale
        )
        d_qkv = jnp.stack(
            [
                d_query.reshape(steps, frames, col_width),
                d_key.reshape(steps, frames, col_width),
                d_value.reshape(steps, frames, col_width),
            ],
            axis=1,
        ).astype(BF)
        d_wqkv = jnp.einsum("sfd,sjfe->sjde", n1_all, d_qkv, preferred_element_type=F32)
        d_attn = jnp.concatenate([d_wqkv.astype(BF), d_out_t[:, None].astype(BF)], axis=1)
        r_attn = lax.psum_scatter(d_attn, "xy", scatter_dimension=2, tiled=True)
        dn1 = deal(jnp.einsum("sjfe,sjde->sfd", d_qkv, wqkv, preferred_element_type=F32))
        dh_norm1, dgain_one = norm_back(dn1, h0, r1, gain_one)
        dh0 = dh1 + dh_norm1
        input_grad = dh0.astype(BF)
        d_pad = jnp.sum(dh0[0] * (1.0 - maskf)[:, None], axis=0)
        small_grad = jnp.stack([dgain_one, dgain_two, d_pad], axis=0)
        small_grad = lax.psum(small_grad, ("xy", "core", "tensor"))
        place = lax.axis_index("xy") * 2 + core
        g_small = lax.dynamic_slice_in_dim(
            small_grad, place * pad_row.shape[0], pad_row.shape[0], 1
        )

        def settle(reduced, split_axis, join_axis):
            return trade(core, reduced, split_axis, join_axis).astype(F32)

        g_down = settle(r_down, 2, 1)
        g_gate_up = settle(r_gate_up, 2, 3)
        g_attn = settle(r_attn, 2, 3)
        g_qkv = g_attn[:, :3]
        g_out = jnp.swapaxes(g_attn[:, 3], 1, 2)
        return (layer_out, input_grad, g_qkv, g_out, g_gate_up, g_down, g_small[0:2], g_small[2])

    return shards


def make_step_shards(count, lanes):

    def exchange(blocks):
        return lax.all_to_all(blocks, "dp", 0, 0, tiled=True)

    def collect(rows):
        return lax.all_gather(rows, "tensor", axis=0).reshape(-1, rows.shape[-1])

    def deal(partial):
        slots = partial.astype(BF).reshape(lanes, count, -1, partial.shape[-1])
        return lax.psum_scatter(slots, "tensor", scatter_dimension=0).astype(F32)

    def frame_split(array):
        slots = array.reshape(lanes, count, -1, array.shape[-1])
        slots = jnp.swapaxes(slots, 0, 1)
        return exchange(slots.reshape(count, -1, array.shape[-1]))

    def frame_join(array):
        slots = exchange(array).reshape(count, lanes, -1, array.shape[-1])
        return jnp.swapaxes(slots, 0, 1).reshape(-1, array.shape[-1])

    def after(value, *waiting):
        return lax.optimization_barrier((value,) + waiting)

    def shards(
        layer_in, text_mask, w_qkv, w_out, w_gate_up, w_down, norm_gains, pad_row, out_grad
    ):
        me = lax.axis_index("dp")
        steps, local, width = layer_in.shape
        block = width // count

        def tile(line):
            pads = [(0, 0)] * (line.ndim - 1) + [(0, TILE - 1), (0, width - line.shape[-1])]
            return jnp.pad(line[..., None, :], pads)

        here = lax.axis_index("tensor")

        def own(array):
            return lax.dynamic_index_in_dim(array, here, 0, keepdims=False)

        small = jnp.concatenate([norm_gains, pad_row[None]], axis=0).astype(BF).reshape(-1)
        line = jnp.concatenate([small, text_mask.astype(BF)])
        hello = jnp.concatenate([layer_in.reshape(-1, width), tile(line)])
        hello = lax.all_gather(hello, "tensor", axis=0)

        w_attn = jnp.concatenate(
            [w_qkv[:, 0], w_qkv[:, 1], w_qkv[:, 2], jnp.swapaxes(w_out, 1, 2)], axis=2
        )
        w_attn = exchange(w_attn.astype(BF)).reshape(width, -1)
        cols = w_attn.shape[1] // 4
        hello, w_attn = after(hello, w_attn)
        w_in, wout_t = w_attn[:, : 3 * cols], w_attn[:, 3 * cols :]
        wout_all = lax.all_gather(wout_t, "tensor", axis=0)

        rows_in = hello[:, : steps * local].reshape(lanes, steps, local, width)
        rows_in = jnp.swapaxes(rows_in, 0, 1).reshape(steps, -1, width)
        notes = jnp.pad(hello[:, steps * local], ((0, TILE - lanes), (0, 0)))
        notes = jnp.broadcast_to(notes[None], (count, TILE, width))
        hello = exchange(jnp.concatenate([rows_in, notes], axis=1))
        rows_in = jnp.swapaxes(hello[:, : lanes * local].reshape(count, lanes, local, width), 0, 1)
        notes = hello[:, lanes * local : lanes * local + lanes].astype(F32)
        small = jnp.swapaxes(notes[:, 0, : 3 * block].reshape(count, 3, block), 0, 1)
        gain_one, gain_two, pad_vec = small.reshape(3, width)
        mask = jnp.swapaxes(notes[..., 3 * block : 3 * block + local], 0, 1)
        padded = jnp.where(me == 0, 1.0 - mask, 0.0)[..., None]
        h0 = rows_in.astype(F32) + padded * pad_vec
        r1 = lax.rsqrt(jnp.mean(h0 * h0, axis=-1, keepdims=True) + EPS)
        n1_all = (h0 * r1 * gain_one).astype(BF).reshape(-1, width)
        rows_in, out_grad = after(rows_in, out_grad)
        grad = exchange(out_grad)
        qkv = jnp.dot(n1_all, w_in, preferred_element_type=F32).astype(BF)
        qkv, grad, w_gate_up, w_down = after(qkv, grad, w_gate_up, w_down)
        grad_all = collect(grad)
        wgu = jnp.concatenate([w_gate_up[:, 0], w_gate_up[:, 1]], axis=2).astype(BF)
        wdown = w_down.astype(BF)

        qkv, wgu, wdown = after(frame_split(qkv), wgu, wdown)
        frames = qkv.shape[1]
        heads = cols // HEAD
        scale = 1.0 / math.sqrt(HEAD)
        query = qkv[..., :cols].reshape(steps, frames, heads, HEAD)
        keyv = qkv[..., cols : 2 * cols].reshape(steps, frames, heads, HEAD)
        value = qkv[..., 2 * cols :].reshape(steps, frames, heads, HEAD)
        causal = jnp.arange(steps)[:, None] >= jnp.arange(steps)[None, :]

        def score_of(qv, kv):
            raw = jnp.einsum("sfhe,tfhe->fhst", qv, kv, preferred_element_type=F32) * scale
            return jnp.where(causal, raw, -1e30)

        scores = score_of(query, keyv)
        top = jnp.max(scores, axis=-1, keepdims=True)
        expo = jnp.exp(scores - top)
        total = jnp.sum(expo, axis=-1, keepdims=True)
        lse = top + jnp.log(total)
        probs_low = (expo / total).astype(BF)
        mixed = jnp.einsum("fhst,tfhe->sfhe", probs_low, value, preferred_element_type=F32)
        mixed_all = frame_join(mixed.reshape(steps, frames, cols).astype(BF))

        mixed_all, wout_all, grad_all, wgu, wdown = after(
            mixed_all, wout_all, grad_all, wgu, wdown
        )
        mixed_full = lax.all_gather(mixed_all, "tensor", axis=0)
        mixed_full = jnp.concatenate([mixed_full[k] for k in range(lanes)], axis=1)
        wout_full = jnp.concatenate([wout_all[k] for k in range(lanes)], axis=1)
        wgu, wdown = after(exchange(wgu).reshape(width, -1), wdown)
        wdown = jnp.swapaxes(exchange(wdown), 0, 1).reshape(-1, width)
        attn = jnp.einsum("fe,de->fd", mixed_full, wout_full, preferred_element_type=F32)
        h1 = h0 + attn.reshape(h0.shape)
        r2 = lax.rsqrt(jnp.mean(h1 * h1, axis=-1, keepdims=True) + EPS)
        n2_all = (h1 * r2 * gain_two).astype(BF).reshape(-1, width)
        h0, r1, h1, r2, padded = own(h0), own(r1), own(h1), own(r2), own(padded)

        gate_up = jnp.dot(n2_all, wgu, preferred_element_type=F32)
        hid_width = gate_up.shape[1] // 2
        gate, upval = gate_up[:, :hid_width], gate_up[:, hid_width:]
        sigma = jax.nn.sigmoid(gate)
        silu_val = gate * sigma
        hidden = (silu_val * upval).astype(BF)
        d_hidden = jnp.einsum("fd,kd->fk", grad_all, wdown, preferred_element_type=F32)
        d_gate = (d_hidden * upval * (sigma * (1.0 + gate * (1.0 - sigma)))).astype(BF)
        d_up = (d_hidden * silu_val).astype(BF)
        wgate, wup = wgu[:, :hid_width], wgu[:, hid_width:]
        dn2 = jnp.einsum("fk,dk->fd", d_gate, wgate, preferred_element_type=F32)
        dn2 = dn2 + jnp.einsum("fk,dk->fd", d_up, wup, preferred_element_type=F32)

        dn2, hidden, d_gate, d_up = after(dn2.astype(BF), hidden, d_gate, d_up)
        dn2 = deal(dn2)
        d_down = jnp.einsum(
            "fk,frd->rkd",
            hidden,
            grad_all.reshape(-1, count, block),
            preferred_element_type=F32,
        )
        g_down = exchange(d_down.astype(BF))
        g_gate = jnp.einsum("fd,fk->dk", n2_all, d_gate, preferred_element_type=F32).astype(BF)
        g_up = jnp.einsum("fd,fk->dk", n2_all, d_up, preferred_element_type=F32).astype(BF)
        dn2, g_down, g_gate, g_up = after(dn2, g_down, g_gate, g_up)
        dh_norm2, dgain_two = norm_back(dn2, h1, r2, gain_two)
        dh1 = grad.astype(F32) + dh_norm2
        dh1_low, g_gate, hidden = after(dh1.astype(BF), g_gate, hidden)
        dh1_all = collect(dh1_low)
        g_gate = exchange(g_gate.reshape(count, block, -1))
        dh1_all, g_gate = after(dh1_all, g_gate)

        ffout = deal(jnp.dot(hidden, wdown, preferred_element_type=F32))
        d_mixed = jnp.dot(dh1_all, wout_t, preferred_element_type=F32).astype(BF)
        d_mixed, g_up = after(frame_split(d_mixed), g_up)
        d_mixed = d_mixed.reshape(steps, frames, heads, HEAD)
        g_up = exchange(g_up.reshape(count, block, -1))
        probs = jnp.exp(score_of(query, keyv) - lse)
        d_probs = jnp.einsum("sfhe,tfhe->fhst", d_mixed, value, preferred_element_type=F32)
        d_value = jnp.einsum("fhst,sfhe->tfhe", probs_low, d_mixed, preferred_element_type=F32)
        d_scores = probs * (d_probs - jnp.sum(probs * d_probs, axis=-1, keepdims=True))
        d_query = (
            jnp.einsum("fhst,tfhe->sfhe", d_scores, keyv.astype(F32), precision=HIGH) * scale
        )
        d_key = (
            jnp.einsum("fhst,sfhe->tfhe", d_scores, query.astype(F32), precision=HIGH) * scale
        )
        d_qkv = jnp.concatenate(
            [a.reshape(steps, frames, cols).astype(BF) for a in (d_query, d_key, d_value)],
            axis=-1,
        )
        d_qkv, g_up = after(d_qkv, g_up)
        g_gate_up = jnp.stack([g_gate, g_up], axis=1).astype(F32)
        d_qkv = frame_join(d_qkv)
        dn1 = jnp.einsum("fe,de->fd", d_qkv, w_in, preferred_element_type=F32).astype(BF)

        dn1, d_qkv, ffout = after(dn1, d_qkv, ffout)
        dn1 = deal(dn1)
        d_attn = jnp.concatenate(
            [
                jnp.einsum("fd,fe->de", n1_all, d_qkv, preferred_element_type=F32).astype(BF),
                jnp.einsum("fd,fe->de", dh1_all, mixed_all, preferred_element_type=F32).astype(BF),
            ],
            axis=1,
        )
        g_attn = exchange(d_attn.reshape(count, block, -1))
        layer_out = exchange((h1 + ffout).astype(BF))
        dn1, g_attn, layer_out = after(dn1, g_attn, layer_out)
        g_down, g_attn = g_down.astype(F32), g_attn.astype(F32)
        g_qkv = jnp.stack([g_attn[..., j * cols : (j + 1) * cols] for j in range(3)], axis=1)
        g_out = jnp.swapaxes(g_attn[..., 3 * cols :], 1, 2)

        dh_norm1, dgain_one = norm_back(dn1, h0, r1, gain_one)
        dh0 = dh1 + dh_norm1
        d_pad = jnp.sum(dh0 * padded, axis=(0, 1))
        sums = jnp.stack([dgain_one, dgain_two, d_pad]).reshape(3, count, block)
        sums = jnp.swapaxes(sums, 0, 1).reshape(count, -1)
        high = sums.astype(BF)
        rest = (sums - high.astype(F32)).astype(BF)
        notes = tile(jnp.concatenate([high, rest], axis=1))
        last = exchange(jnp.concatenate([dh0.astype(BF), notes], axis=1))
        input_grad = last[:, :local]
        sums = jnp.sum(last[:, local].astype(F32), axis=0)[: 6 * block].reshape(2, 3, block)
        sums = sums[0] + sums[1]
        g_small = sums
        for k in range(1, lanes):
            around = [(i, (i + k) % lanes) for i in range(lanes)]
            g_small = g_small + lax.ppermute(sums, "tensor", around)
        return (layer_out, input_grad, g_qkv, g_out, g_gate_up, g_down, g_small[0:2], g_small[2])

    return shards


def spread(body, mesh, dp):
    rows = dp + ("tensor",)
    weights = (
        P(None, None, dp, "tensor"),
        P(None, "tensor", dp),
        P(None, None, dp, "tensor"),
        P(None, "tensor", dp),
        P(None, dp),
        P(dp),
    )
    return jax.shard_map(
        body,
        mesh=mesh,
        in_specs=(P(None, rows, None), P(rows)) + weights + (P(None, rows, None),),
        out_specs=(P(None, rows, None), P(None, rows, None)) + weights,
        check_vma=False,
    )


def solution(mesh):
    dp_size, tensor_size = mesh.shape["dp"], mesh.shape["tensor"]

    def layer(layer_in, *others):
        steps, frames, width = layer_in.shape
        local = frames // (dp_size * tensor_size)
        block = width // dp_size
        fits = 6 * block <= width and 3 * block + local <= width
        if steps == dp_size and dp_size & (dp_size - 1) == 0 and fits:
            body, over, dp = make_step_shards(dp_size, tensor_size), mesh, ("dp",)
        else:
            over = Mesh(
                np.asarray(mesh.devices).reshape(dp_size // 2, 2, tensor_size),
                ("xy", "core", "tensor"),
            )
            body, dp = make_shards(tensor_size), ("xy", "core")
        return spread(body, over, dp)(layer_in, *others)

    return layer
```

```python
import math

import jax
import jax.numpy as jnp
import numpy as np
from jax import lax
from jax.experimental import pallas as pl
from jax.sharding import Mesh
from jax.sharding import PartitionSpec as P

HEAD = 64
EPS = 1e-05
HIGH = lax.Precision.HIGHEST
BF = jnp.bfloat16
F32 = jnp.float32
SWAP = ((0, 1), (1, 0))
TILE = 16


def norm_back(upstream, hval, rstat, gain):
    scaled = upstream * gain
    dgain = jnp.sum(upstream * hval * rstat, axis=(0, 1))
    dhval = rstat * scaled - hval * rstat**3 * jnp.mean(scaled * hval, axis=-1, keepdims=True)
    return (dhval, dgain)


def half(array, axis, which):
    size = array.shape[axis] // 2
    return lax.dynamic_slice_in_dim(array, which * size, size, axis)


def ordered(core, own, other, axis):
    is_first = core == 0
    return jnp.concatenate(
        [jnp.where(is_first, own, other), jnp.where(is_first, other, own)], axis=axis
    )


def make_shards(tensor_size):
    def around(shift):
        return [(i, (i + shift) % tensor_size) for i in range(tensor_size)]

    def trade(core, weight, split_axis, join_axis):
        mine = half(weight, split_axis, core)
        theirs = half(weight, split_axis, 1 - core)
        got = lax.ppermute(theirs, "core", SWAP)
        return ordered(core, mine, got, join_axis)

    def collect(rows):
        parts = [rows] + [
            lax.ppermute(rows, "tensor", around(k)) for k in range(1, tensor_size)
        ]
        near = jnp.stack(parts, axis=1)
        far = lax.ppermute(near, "core", SWAP)
        whole = jnp.concatenate([near, far], axis=1)
        return whole.reshape(rows.shape[0], -1, rows.shape[2])

    def deal(partial):
        steps, frames, width = partial.shape
        split = partial.reshape(steps, 2, tensor_size, frames // (2 * tensor_size), width)
        got = lax.ppermute(split[:, 1].astype(BF), "core", SWAP)
        chip = split[:, 0].astype(F32) + got.astype(F32)
        total = chip[:, 0]
        for k in range(1, tensor_size):
            total = total + lax.ppermute(chip[:, k].astype(BF), "tensor", around(-k)).astype(F32)
        return total

    def shards(
        layer_in, text_mask, w_qkv, w_out, w_gate_up, w_down, norm_gains, pad_row, out_grad
    ):
        core = lax.axis_index("core")
        steps, local_frames, width = layer_in.shape

        w_attn = jnp.concatenate(
            [w_qkv.astype(BF), jnp.swapaxes(w_out, 1, 2)[:, None].astype(BF)], axis=1
        )
        w_attn = lax.all_gather(trade(core, w_attn, 3, 2), "xy", axis=2, tiled=True)
        small = jnp.concatenate([norm_gains, pad_row[None]], axis=0).astype(BF)
        small = lax.all_gather(small, ("xy", "core"), axis=1, tiled=True).astype(F32)
        wgu = lax.all_gather(trade(core, w_gate_up.astype(BF), 3, 2), "xy", axis=2, tiled=True)
        wdown = lax.all_gather(trade(core, w_down.astype(BF), 1, 2), "xy", axis=2, tiled=True)

        gain_one, gain_two, pad_vec = small[0], small[1], small[2]
        maskf = text_mask.astype(F32)
        first = (jnp.arange(steps) == 0).astype(F32)
        h0 = (
            layer_in.astype(F32)
            + first[:, None, None] * (1.0 - maskf)[None, :, None] * pad_vec[None, None, :]
        )
        r1 = lax.rsqrt(jnp.mean(h0 * h0, axis=-1, keepdims=True) + EPS)
        n1 = (h0 * r1 * gain_one).astype(BF)
        n1_all = collect(n1)
        grad_all = collect(out_grad)
        frames = n1_all.shape[1]
        wqkv, wout_t = w_attn[:, :3], w_attn[:, 3]
        qkv = jnp.einsum("sfd,sjde->sjfe", n1_all, wqkv, preferred_element_type=F32).astype(BF)
        col_width = qkv.shape[-1]
        heads = col_width // HEAD
        scale = 1.0 / math.sqrt(HEAD)
        query = qkv[:, 0].reshape(steps, frames, heads, HEAD)
        keyv = qkv[:, 1].reshape(steps, frames, heads, HEAD)
        value = qkv[:, 2].reshape(steps, frames, heads, HEAD)
        causal = jnp.arange(steps)[:, None] >= jnp.arange(steps)[None, :]

        def score_of(qv, kv):
            raw = jnp.einsum("sfhe,tfhe->fhst", qv, kv, preferred_element_type=F32) * scale
            return jnp.where(causal, raw, -1e30)

        scores = score_of(query, keyv)
        top = jnp.max(scores, axis=-1, keepdims=True)
        expo = jnp.exp(scores - top)
        total = jnp.sum(expo, axis=-1, keepdims=True)
        lse = top + jnp.log(total)
        probs_low = (expo / total).astype(BF)
        mixed = jnp.einsum("fhst,tfhe->sfhe", probs_low, value, preferred_element_type=F32)
        mixed = mixed.reshape(steps, frames, col_width).astype(BF)
        attn = deal(jnp.einsum("sfd,sed->sfe", mixed, wout_t, preferred_element_type=F32))
        h1 = h0 + attn
        r2 = lax.rsqrt(jnp.mean(h1 * h1, axis=-1, keepdims=True) + EPS)
        n2 = (h1 * r2 * gain_two).astype(BF)
        n2_all = collect(n2)
        gate_up = jnp.einsum("sfd,sjde->sjfe", n2_all, wgu, preferred_element_type=F32)
        gate = gate_up[:, 0]
        upval = gate_up[:, 1]
        sigma = jax.nn.sigmoid(gate)
        silu_val = gate * sigma
        hidden = (silu_val * upval).astype(BF)
        d_down = jnp.einsum("sfk,sfd->skd", hidden, grad_all, preferred_element_type=F32)
        r_down = lax.psum_scatter(d_down.astype(BF), "xy", scatter_dimension=2, tiled=True)
        d_hidden = jnp.einsum("sfd,skd->sfk", grad_all, wdown, preferred_element_type=F32)
        d_gate = d_hidden * upval * (sigma * (1.0 + gate * (1.0 - sigma)))
        d_up = d_hidden * silu_val
        d_gu = jnp.stack([d_gate, d_up], axis=1).astype(BF)
        d_gate_up = jnp.einsum("sfd,sjfe->sjde", n2_all, d_gu, preferred_element_type=F32)
        r_gate_up = lax.psum_scatter(d_gate_up.astype(BF), "xy", scatter_dimension=2, tiled=True)
        dn2 = deal(jnp.einsum("sjfe,sjde->sfd", d_gu, wgu, preferred_element_type=F32))
        dh_norm2, dgain_two = norm_back(dn2, h1, r2, gain_two)
        dh1 = out_grad.astype(F32) + dh_norm2
        dh1_all = collect(dh1.astype(BF))
        ffout = deal(jnp.einsum("sfk,skd->sfd", hidden, wdown, preferred_element_type=F32))
        layer_out = (h1 + ffout).astype(BF)
        d_out_t = jnp.einsum("sfe,sfd->sed", dh1_all, mixed, preferred_element_type=F32)
        d_mixed = jnp.einsum("sfe,sed->sfd", dh1_all, wout_t, preferred_element_type=F32)
        d_mixed = d_mixed.astype(BF).reshape(steps, frames, heads, HEAD)
        probs = jnp.exp(score_of(query, keyv) - lse)
        d_probs = jnp.einsum("sfhe,tfhe->fhst", d_mixed, value, preferred_element_type=F32)
        d_value = jnp.einsum("fhst,sfhe->tfhe", probs_low, d_mixed, preferred_element_type=F32)
        d_scores = probs * (d_probs - jnp.sum(probs * d_probs, axis=-1, keepdims=True))
        d_query = (
            jnp.einsum("fhst,tfhe->sfhe", d_scores, keyv.astype(F32), precision=HIGH) * scale
        )
        d_key = (
            jnp.einsum("fhst,sfhe->tfhe", d_scores, query.astype(F32), precision=HIGH) * scale
        )
        d_qkv = jnp.stack(
            [
                d_query.reshape(steps, frames, col_width),
                d_key.reshape(steps, frames, col_width),
                d_value.reshape(steps, frames, col_width),
            ],
            axis=1,
        ).astype(BF)
        d_wqkv = jnp.einsum("sfd,sjfe->sjde", n1_all, d_qkv, preferred_element_type=F32)
        d_attn = jnp.concatenate([d_wqkv.astype(BF), d_out_t[:, None].astype(BF)], axis=1)
        r_attn = lax.psum_scatter(d_attn, "xy", scatter_dimension=2, tiled=True)
        dn1 = deal(jnp.einsum("sjfe,sjde->sfd", d_qkv, wqkv, preferred_element_type=F32))
        dh_norm1, dgain_one = norm_back(dn1, h0, r1, gain_one)
        dh0 = dh1 + dh_norm1
        input_grad = dh0.astype(BF)
        d_pad = jnp.sum(dh0[0] * (1.0 - maskf)[:, None], axis=0)
        small_grad = jnp.stack([dgain_one, dgain_two, d_pad], axis=0)
        small_grad = lax.psum(small_grad, ("xy", "core", "tensor"))
        place = lax.axis_index("xy") * 2 + core
        g_small = lax.dynamic_slice_in_dim(
            small_grad, place * pad_row.shape[0], pad_row.shape[0], 1
        )

        def settle(reduced, split_axis, join_axis):
            return trade(core, reduced, split_axis, join_axis).astype(F32)

        g_down = settle(r_down, 2, 1)
        g_gate_up = settle(r_gate_up, 2, 3)
        g_attn = settle(r_attn, 2, 3)
        g_qkv = g_attn[:, :3]
        g_out = jnp.swapaxes(g_attn[:, 3], 1, 2)
        return (layer_out, input_grad, g_qkv, g_out, g_gate_up, g_down, g_small[0:2], g_small[2])

    return shards


def attention_masks(steps):
    size = steps * TILE
    row = lax.broadcasted_iota(jnp.int32, (size, size), 0)
    col = lax.broadcasted_iota(jnp.int32, (size, size), 1)
    keep = (row % TILE == col % TILE) & (row >= col)
    lane = lax.broadcasted_iota(jnp.int32, (size, 2 * HEAD), 1)
    return keep, lane < HEAD


def times(left, right, left_axis, right_axis):
    return lax.dot_general(
        left, right, (((left_axis,), (right_axis,)), ((), ())), preferred_element_type=F32
    )


def attention_probs(query, keyv, keep):
    scores = jnp.where(keep, times(query, keyv, 1, 1) * (1.0 / math.sqrt(HEAD)), -1e30)
    expo = jnp.exp(scores - jnp.max(scores, axis=-1, keepdims=True))
    return expo / jnp.sum(expo, axis=-1, keepdims=True)


def attention_tile(ref, tile, start):
    part = ref[:, tile * TILE : (tile + 1) * TILE, start : start + 2 * HEAD]
    return part.reshape(-1, 2 * HEAD)


def attention_forward_body(qkv_ref, out_ref):
    steps, frames, cols = out_ref.shape
    keep, is_first = attention_masks(steps)
    for tile in range(frames // TILE):
        for pair in range(0, cols, 2 * HEAD):
            query, keyv, value = [
                attention_tile(qkv_ref, tile, j * cols + pair) for j in range(3)
            ]
            mixed = []
            for mine in (is_first, ~is_first):
                probs = attention_probs(jnp.where(mine, query, 0), keyv, keep)
                mixed.append(times(probs.astype(BF), value, 1, 0))
            mixed = jnp.where(is_first, mixed[0], mixed[1]).astype(BF)
            out_ref[:, tile * TILE : (tile + 1) * TILE, pair : pair + 2 * HEAD] = mixed.reshape(
                steps, TILE, 2 * HEAD
            )


def attention_backward_body(qkv_ref, grad_ref, out_ref):
    steps, frames, cols = grad_ref.shape
    keep, is_first = attention_masks(steps)
    scale = 1.0 / math.sqrt(HEAD)
    for tile in range(frames // TILE):
        for pair in range(0, cols, 2 * HEAD):
            query, keyv, value = [
                attention_tile(qkv_ref, tile, j * cols + pair) for j in range(3)
            ]
            grad = attention_tile(grad_ref, tile, pair)
            found = []
            for mine in (is_first, ~is_first):
                probs = attention_probs(jnp.where(mine, query, 0), keyv, keep)
                d_probs = times(jnp.where(mine, grad, 0), value, 1, 1)
                d_value = times(probs.astype(BF), grad, 0, 0)
                d_scores = probs * (d_probs - jnp.sum(probs * d_probs, axis=-1, keepdims=True))
                high = d_scores.astype(BF)
                rest = (d_scores - high.astype(F32)).astype(BF)
                d_query = (times(high, keyv, 1, 0) + times(rest, keyv, 1, 0)) * scale
                d_key = (times(high, query, 0, 0) + times(rest, query, 0, 0)) * scale
                found.append((d_query, d_key, d_value))
            for j in range(3):
                part = jnp.where(is_first, found[0][j], found[1][j]).astype(BF)
                start = j * cols + pair
                out_ref[:, tile * TILE : (tile + 1) * TILE, start : start + 2 * HEAD] = (
                    part.reshape(steps, TILE, 2 * HEAD)
                )


def attention_call(body, arrays, cols, span):
    steps, frames = arrays[0].shape[:2]

    def spec(width):
        return pl.BlockSpec((steps, span, width), lambda i: (0, i, 0))

    return pl.pallas_call(
        body,
        grid=(frames // span,),
        in_specs=[spec(a.shape[2]) for a in arrays],
        out_specs=spec(cols),
        out_shape=jax.ShapeDtypeStruct((steps, frames, cols), BF),
    )(*arrays)


def make_step_shards(count, lanes):

    def exchange(blocks):
        return lax.all_to_all(blocks, "dp", 0, 0, tiled=True)

    def collect(rows):
        return lax.all_gather(rows, "tensor", axis=0).reshape(-1, rows.shape[-1])

    def deal(partial):
        slots = partial.astype(BF).reshape(lanes, count, -1, partial.shape[-1])
        return lax.psum_scatter(slots, "tensor", scatter_dimension=0).astype(F32)

    def frame_split(array):
        slots = array.reshape(lanes, count, -1, array.shape[-1])
        slots = jnp.swapaxes(slots, 0, 1)
        return exchange(slots.reshape(count, -1, array.shape[-1]))

    def frame_join(array):
        slots = exchange(array).reshape(count, lanes, -1, array.shape[-1])
        return jnp.swapaxes(slots, 0, 1).reshape(-1, array.shape[-1])

    def after(value, *waiting):
        return lax.optimization_barrier((value,) + waiting)

    def shards(
        layer_in, text_mask, w_qkv, w_out, w_gate_up, w_down, norm_gains, pad_row, out_grad
    ):
        me = lax.axis_index("dp")
        steps, local, width = layer_in.shape
        block = width // count

        def tile(line):
            pads = [(0, 0)] * (line.ndim - 1) + [(0, TILE - 1), (0, width - line.shape[-1])]
            return jnp.pad(line[..., None, :], pads)

        small = jnp.concatenate([norm_gains, pad_row[None]], axis=0).astype(BF).reshape(-1)
        line = jnp.concatenate([small, text_mask.astype(BF)])
        notes = jnp.broadcast_to(tile(line)[None], (count, TILE, width))
        hello = exchange(jnp.concatenate([layer_in, notes], axis=1))
        rows_in = hello[:, :local].astype(F32)
        notes = hello[:, local].astype(F32)
        small = jnp.swapaxes(notes[:, : 3 * block].reshape(count, 3, block), 0, 1)
        gain_one, gain_two, pad_vec = small.reshape(3, width)
        padded = jnp.where(me == 0, 1.0 - notes[:, 3 * block : 3 * block + local], 0.0)[..., None]
        h0 = rows_in + padded * pad_vec
        r1 = lax.rsqrt(jnp.mean(h0 * h0, axis=-1, keepdims=True) + EPS)
        n1 = (h0 * r1 * gain_one).astype(BF)
        n1, w_qkv, w_out = after(n1, w_qkv, w_out)
        n1_all = collect(n1)

        w_attn = jnp.concatenate(
            [w_qkv[:, 0], w_qkv[:, 1], w_qkv[:, 2], jnp.swapaxes(w_out, 1, 2)], axis=2
        )
        w_attn = exchange(w_attn.astype(BF)).reshape(width, -1)
        cols = w_attn.shape[1] // 4
        w_in, wout_t = w_attn[:, : 3 * cols], w_attn[:, 3 * cols :]
        w_attn, out_grad = after(w_attn, out_grad)
        grad = exchange(out_grad)
        n1_all, grad = after(n1_all, grad)
        grad_all = collect(grad)
        qkv = jnp.dot(n1_all, w_in, preferred_element_type=F32).astype(BF)

        qkv = frame_split(qkv)
        mixed_all = frame_join(attention_call(attention_forward_body, (qkv,), cols, 2 * TILE))
        attn = jnp.einsum("fe,de->fd", mixed_all, wout_t, preferred_element_type=F32)

        attn, w_down, w_gate_up, grad_all = after(attn.astype(BF), w_down, w_gate_up, grad_all)
        attn = deal(attn)
        wdown = exchange(w_down.astype(BF))
        wgu = jnp.concatenate([w_gate_up[:, 0], w_gate_up[:, 1]], axis=2).astype(BF)
        attn, wdown, wgu = after(attn, wdown, wgu)
        wdown = jnp.swapaxes(wdown, 0, 1).reshape(-1, width)
        h1 = h0 + attn
        r2 = lax.rsqrt(jnp.mean(h1 * h1, axis=-1, keepdims=True) + EPS)
        n2 = (h1 * r2 * gain_two).astype(BF)
        n2, wgu = after(n2, wgu)
        n2_all = collect(n2)
        wgu = exchange(wgu).reshape(width, -1)

        gate_up = jnp.dot(n2_all, wgu, preferred_element_type=F32)
        hid_width = gate_up.shape[1] // 2
        gate, upval = gate_up[:, :hid_width], gate_up[:, hid_width:]
        sigma = jax.nn.sigmoid(gate)
        silu_val = gate * sigma
        hidden = (silu_val * upval).astype(BF)
        d_hidden = jnp.einsum("fd,kd->fk", grad_all, wdown, preferred_element_type=F32)
        d_gate = (d_hidden * upval * (sigma * (1.0 + gate * (1.0 - sigma)))).astype(BF)
        d_up = (d_hidden * silu_val).astype(BF)
        wgate, wup = wgu[:, :hid_width], wgu[:, hid_width:]
        dn2 = jnp.einsum("fk,dk->fd", d_gate, wgate, preferred_element_type=F32)
        dn2 = dn2 + jnp.einsum("fk,dk->fd", d_up, wup, preferred_element_type=F32)

        dn2, hidden, d_gate, d_up = after(dn2.astype(BF), hidden, d_gate, d_up)
        dn2 = deal(dn2)
        d_down = jnp.einsum(
            "fk,frd->rkd",
            hidden,
            grad_all.reshape(-1, count, block),
            preferred_element_type=F32,
        )
        g_down = exchange(d_down.astype(BF))
        g_gate = jnp.einsum("fd,fk->dk", n2_all, d_gate, preferred_element_type=F32).astype(BF)
        g_up = jnp.einsum("fd,fk->dk", n2_all, d_up, preferred_element_type=F32).astype(BF)
        part = hid_width // 2
        g_gate = jnp.concatenate([g_gate, g_up[:, :part]], axis=1).reshape(count, block, -1)
        g_up = g_up[:, part:].reshape(count, block, -1)
        dn2, g_down, g_gate, g_up = after(dn2, g_down, g_gate, g_up)
        dh_norm2, dgain_two = norm_back(dn2, h1, r2, gain_two)
        dh1 = grad.astype(F32) + dh_norm2
        dh1_low, g_gate, hidden = after(dh1.astype(BF), g_gate, hidden)
        dh1_all = collect(dh1_low)
        g_gate = exchange(g_gate)
        dh1_all, g_gate = after(dh1_all, g_gate)

        ffout = deal(jnp.dot(hidden, wdown, preferred_element_type=F32))
        d_mixed = jnp.dot(dh1_all, wout_t, preferred_element_type=F32).astype(BF)
        d_mixed, g_up = after(frame_split(d_mixed), g_up)
        g_up = exchange(g_up)
        d_qkv = attention_call(attention_backward_body, (qkv, d_mixed), 3 * cols, 2 * TILE)
        d_qkv, g_up = after(d_qkv, g_up)
        g_up = jnp.concatenate([g_gate[..., hid_width:], g_up], axis=2)
        g_gate_up = jnp.stack([g_gate[..., :hid_width], g_up], axis=1).astype(F32)
        d_qkv = frame_join(d_qkv)
        dn1 = jnp.einsum("fe,de->fd", d_qkv, w_in, preferred_element_type=F32).astype(BF)

        dn1, d_qkv, ffout = after(dn1, d_qkv, ffout)
        dn1 = deal(dn1)
        d_attn = jnp.concatenate(
            [
                jnp.einsum("fd,fe->de", n1_all, d_qkv, preferred_element_type=F32).astype(BF),
                jnp.einsum("fd,fe->de", dh1_all, mixed_all, preferred_element_type=F32).astype(BF),
            ],
            axis=1,
        )
        g_attn = exchange(d_attn.reshape(count, block, -1))
        layer_out = exchange((h1 + ffout).astype(BF))
        dn1, g_attn, layer_out = after(dn1, g_attn, layer_out)
        g_down, g_attn = g_down.astype(F32), g_attn.astype(F32)
        g_qkv = jnp.stack([g_attn[..., j * cols : (j + 1) * cols] for j in range(3)], axis=1)
        g_out = jnp.swapaxes(g_attn[..., 3 * cols :], 1, 2)

        dh_norm1, dgain_one = norm_back(dn1, h0, r1, gain_one)
        dh0 = dh1 + dh_norm1
        d_pad = jnp.sum(dh0 * padded, axis=(0, 1))
        sums = jnp.stack([dgain_one, dgain_two, d_pad]).reshape(3, count, block)
        sums = jnp.swapaxes(sums, 0, 1).reshape(count, -1)
        high = sums.astype(BF)
        rest = (sums - high.astype(F32)).astype(BF)
        notes = tile(jnp.concatenate([high, rest], axis=1))
        last = exchange(jnp.concatenate([dh0.astype(BF), notes], axis=1))
        input_grad = last[:, :local]
        sums = jnp.sum(last[:, local].astype(F32), axis=0)[: 6 * block].reshape(2, 3, block)
        sums = sums[0] + sums[1]
        g_small = sums
        for k in range(1, lanes):
            around = [(i, (i + k) % lanes) for i in range(lanes)]
            g_small = g_small + lax.ppermute(sums, "tensor", around)
        return (layer_out, input_grad, g_qkv, g_out, g_gate_up, g_down, g_small[0:2], g_small[2])

    return shards


def spread(body, mesh, dp):
    rows = dp + ("tensor",)
    weights = (
        P(None, None, dp, "tensor"),
        P(None, "tensor", dp),
        P(None, None, dp, "tensor"),
        P(None, "tensor", dp),
        P(None, dp),
        P(dp),
    )
    return jax.shard_map(
        body,
        mesh=mesh,
        in_specs=(P(None, rows, None), P(rows)) + weights + (P(None, rows, None),),
        out_specs=(P(None, rows, None), P(None, rows, None)) + weights,
        check_vma=False,
    )


def solution(mesh):
    dp_size, tensor_size = mesh.shape["dp"], mesh.shape["tensor"]

    def layer(layer_in, *others):
        steps, frames, width = layer_in.shape
        local = frames // (dp_size * tensor_size)
        block = width // dp_size
        fits = 6 * block <= width and 3 * block + local <= width
        if steps == dp_size and dp_size & (dp_size - 1) == 0 and fits:
            body, over, dp = make_step_shards(dp_size, tensor_size), mesh, ("dp",)
        else:
            over = Mesh(
                np.asarray(mesh.devices).reshape(dp_size // 2, 2, tensor_size),
                ("xy", "core", "tensor"),
            )
            body, dp = make_shards(tensor_size), ("xy", "core")
        return spread(body, over, dp)(layer_in, *others)

    return layer
```

```python
import math

import jax
import jax.numpy as jnp
import numpy as np
from jax import lax
from jax.experimental import pallas as pl
from jax.experimental.layout import Layout, with_layout_constraint
from jax.experimental.pallas import tpu as pltpu
from jax.sharding import Mesh
from jax.sharding import PartitionSpec as P

HEAD = 64
EPS = 1e-05
HIGH = lax.Precision.HIGHEST
BF = jnp.bfloat16
F32 = jnp.float32
SWAP = ((0, 1), (1, 0))
TILE = 16


def norm_back(upstream, hval, rstat, gain):
    scaled = upstream * gain
    dgain = jnp.sum(upstream * hval * rstat, axis=(0, 1))
    dhval = rstat * scaled - hval * rstat**3 * jnp.mean(scaled * hval, axis=-1, keepdims=True)
    return (dhval, dgain)


def half(array, axis, which):
    size = array.shape[axis] // 2
    return lax.dynamic_slice_in_dim(array, which * size, size, axis)


def ordered(core, own, other, axis):
    is_first = core == 0
    return jnp.concatenate(
        [jnp.where(is_first, own, other), jnp.where(is_first, other, own)], axis=axis
    )


def make_shards(tensor_size):
    def around(shift):
        return [(i, (i + shift) % tensor_size) for i in range(tensor_size)]

    def trade(core, weight, split_axis, join_axis):
        mine = half(weight, split_axis, core)
        theirs = half(weight, split_axis, 1 - core)
        got = lax.ppermute(theirs, "core", SWAP)
        return ordered(core, mine, got, join_axis)

    def collect(rows):
        parts = [rows] + [
            lax.ppermute(rows, "tensor", around(k)) for k in range(1, tensor_size)
        ]
        near = jnp.stack(parts, axis=1)
        far = lax.ppermute(near, "core", SWAP)
        whole = jnp.concatenate([near, far], axis=1)
        return whole.reshape(rows.shape[0], -1, rows.shape[2])

    def deal(partial):
        steps, frames, width = partial.shape
        split = partial.reshape(steps, 2, tensor_size, frames // (2 * tensor_size), width)
        got = lax.ppermute(split[:, 1].astype(BF), "core", SWAP)
        chip = split[:, 0].astype(F32) + got.astype(F32)
        total = chip[:, 0]
        for k in range(1, tensor_size):
            total = total + lax.ppermute(chip[:, k].astype(BF), "tensor", around(-k)).astype(F32)
        return total

    def shards(
        layer_in, text_mask, w_qkv, w_out, w_gate_up, w_down, norm_gains, pad_row, out_grad
    ):
        core = lax.axis_index("core")
        steps, local_frames, width = layer_in.shape

        w_attn = jnp.concatenate(
            [w_qkv.astype(BF), jnp.swapaxes(w_out, 1, 2)[:, None].astype(BF)], axis=1
        )
        w_attn = lax.all_gather(trade(core, w_attn, 3, 2), "xy", axis=2, tiled=True)
        small = jnp.concatenate([norm_gains, pad_row[None]], axis=0).astype(BF)
        small = lax.all_gather(small, ("xy", "core"), axis=1, tiled=True).astype(F32)
        wgu = lax.all_gather(trade(core, w_gate_up.astype(BF), 3, 2), "xy", axis=2, tiled=True)
        wdown = lax.all_gather(trade(core, w_down.astype(BF), 1, 2), "xy", axis=2, tiled=True)

        gain_one, gain_two, pad_vec = small[0], small[1], small[2]
        maskf = text_mask.astype(F32)
        first = (jnp.arange(steps) == 0).astype(F32)
        h0 = (
            layer_in.astype(F32)
            + first[:, None, None] * (1.0 - maskf)[None, :, None] * pad_vec[None, None, :]
        )
        r1 = lax.rsqrt(jnp.mean(h0 * h0, axis=-1, keepdims=True) + EPS)
        n1 = (h0 * r1 * gain_one).astype(BF)
        n1_all = collect(n1)
        grad_all = collect(out_grad)
        frames = n1_all.shape[1]
        wqkv, wout_t = w_attn[:, :3], w_attn[:, 3]
        qkv = jnp.einsum("sfd,sjde->sjfe", n1_all, wqkv, preferred_element_type=F32).astype(BF)
        col_width = qkv.shape[-1]
        heads = col_width // HEAD
        scale = 1.0 / math.sqrt(HEAD)
        query = qkv[:, 0].reshape(steps, frames, heads, HEAD)
        keyv = qkv[:, 1].reshape(steps, frames, heads, HEAD)
        value = qkv[:, 2].reshape(steps, frames, heads, HEAD)
        causal = jnp.arange(steps)[:, None] >= jnp.arange(steps)[None, :]

        def score_of(qv, kv):
            raw = jnp.einsum("sfhe,tfhe->fhst", qv, kv, preferred_element_type=F32) * scale
            return jnp.where(causal, raw, -1e30)

        scores = score_of(query, keyv)
        top = jnp.max(scores, axis=-1, keepdims=True)
        expo = jnp.exp(scores - top)
        total = jnp.sum(expo, axis=-1, keepdims=True)
        lse = top + jnp.log(total)
        probs_low = (expo / total).astype(BF)
        mixed = jnp.einsum("fhst,tfhe->sfhe", probs_low, value, preferred_element_type=F32)
        mixed = mixed.reshape(steps, frames, col_width).astype(BF)
        attn = deal(jnp.einsum("sfd,sed->sfe", mixed, wout_t, preferred_element_type=F32))
        h1 = h0 + attn
        r2 = lax.rsqrt(jnp.mean(h1 * h1, axis=-1, keepdims=True) + EPS)
        n2 = (h1 * r2 * gain_two).astype(BF)
        n2_all = collect(n2)
        gate_up = jnp.einsum("sfd,sjde->sjfe", n2_all, wgu, preferred_element_type=F32)
        gate = gate_up[:, 0]
        upval = gate_up[:, 1]
        sigma = jax.nn.sigmoid(gate)
        silu_val = gate * sigma
        hidden = (silu_val * upval).astype(BF)
        d_down = jnp.einsum("sfk,sfd->skd", hidden, grad_all, preferred_element_type=F32)
        r_down = lax.psum_scatter(d_down.astype(BF), "xy", scatter_dimension=2, tiled=True)
        d_hidden = jnp.einsum("sfd,skd->sfk", grad_all, wdown, preferred_element_type=F32)
        d_gate = d_hidden * upval * (sigma * (1.0 + gate * (1.0 - sigma)))
        d_up = d_hidden * silu_val
        d_gu = jnp.stack([d_gate, d_up], axis=1).astype(BF)
        d_gate_up = jnp.einsum("sfd,sjfe->sjde", n2_all, d_gu, preferred_element_type=F32)
        r_gate_up = lax.psum_scatter(d_gate_up.astype(BF), "xy", scatter_dimension=2, tiled=True)
        dn2 = deal(jnp.einsum("sjfe,sjde->sfd", d_gu, wgu, preferred_element_type=F32))
        dh_norm2, dgain_two = norm_back(dn2, h1, r2, gain_two)
        dh1 = out_grad.astype(F32) + dh_norm2
        dh1_all = collect(dh1.astype(BF))
        ffout = deal(jnp.einsum("sfk,skd->sfd", hidden, wdown, preferred_element_type=F32))
        layer_out = (h1 + ffout).astype(BF)
        d_out_t = jnp.einsum("sfe,sfd->sed", dh1_all, mixed, preferred_element_type=F32)
        d_mixed = jnp.einsum("sfe,sed->sfd", dh1_all, wout_t, preferred_element_type=F32)
        d_mixed = d_mixed.astype(BF).reshape(steps, frames, heads, HEAD)
        probs = jnp.exp(score_of(query, keyv) - lse)
        d_probs = jnp.einsum("sfhe,tfhe->fhst", d_mixed, value, preferred_element_type=F32)
        d_value = jnp.einsum("fhst,sfhe->tfhe", probs_low, d_mixed, preferred_element_type=F32)
        d_scores = probs * (d_probs - jnp.sum(probs * d_probs, axis=-1, keepdims=True))
        d_query = (
            jnp.einsum("fhst,tfhe->sfhe", d_scores, keyv.astype(F32), precision=HIGH) * scale
        )
        d_key = (
            jnp.einsum("fhst,sfhe->tfhe", d_scores, query.astype(F32), precision=HIGH) * scale
        )
        d_qkv = jnp.stack(
            [
                d_query.reshape(steps, frames, col_width),
                d_key.reshape(steps, frames, col_width),
                d_value.reshape(steps, frames, col_width),
            ],
            axis=1,
        ).astype(BF)
        d_wqkv = jnp.einsum("sfd,sjfe->sjde", n1_all, d_qkv, preferred_element_type=F32)
        d_attn = jnp.concatenate([d_wqkv.astype(BF), d_out_t[:, None].astype(BF)], axis=1)
        r_attn = lax.psum_scatter(d_attn, "xy", scatter_dimension=2, tiled=True)
        dn1 = deal(jnp.einsum("sjfe,sjde->sfd", d_qkv, wqkv, preferred_element_type=F32))
        dh_norm1, dgain_one = norm_back(dn1, h0, r1, gain_one)
        dh0 = dh1 + dh_norm1
        input_grad = dh0.astype(BF)
        d_pad = jnp.sum(dh0[0] * (1.0 - maskf)[:, None], axis=0)
        small_grad = jnp.stack([dgain_one, dgain_two, d_pad], axis=0)
        small_grad = lax.psum(small_grad, ("xy", "core", "tensor"))
        place = lax.axis_index("xy") * 2 + core
        g_small = lax.dynamic_slice_in_dim(
            small_grad, place * pad_row.shape[0], pad_row.shape[0], 1
        )

        def settle(reduced, split_axis, join_axis):
            return trade(core, reduced, split_axis, join_axis).astype(F32)

        g_down = settle(r_down, 2, 1)
        g_gate_up = settle(r_gate_up, 2, 3)
        g_attn = settle(r_attn, 2, 3)
        g_qkv = g_attn[:, :3]
        g_out = jnp.swapaxes(g_attn[:, 3], 1, 2)
        return (layer_out, input_grad, g_qkv, g_out, g_gate_up, g_down, g_small[0:2], g_small[2])

    return shards


def attention_masks(steps):
    size = steps * TILE
    row = lax.broadcasted_iota(jnp.int32, (size, size), 0)
    col = lax.broadcasted_iota(jnp.int32, (size, size), 1)
    keep = (row % TILE == col % TILE) & (row <= col)
    lane = lax.broadcasted_iota(jnp.int32, (size, 2 * HEAD), 1)
    return keep, lane < HEAD


def times(left, right, left_axis, right_axis):
    return lax.dot_general(
        left, right, (((left_axis,), (right_axis,)), ((), ())), preferred_element_type=F32
    )


def attention_probs(query, keyv, keep):
    scores = jnp.where(keep, times(keyv, query, 1, 1) * (1.0 / math.sqrt(HEAD)), -1e30)
    expo = jnp.exp(scores - jnp.max(scores, axis=0, keepdims=True))
    return expo * (1.0 / jnp.sum(expo, axis=0, keepdims=True))


def attention_tile(ref, tile, start):
    part = ref[:, tile * TILE : (tile + 1) * TILE, start : start + 2 * HEAD]
    return part.reshape(-1, 2 * HEAD)


def attention_forward_body(qkv_ref, out_ref):
    steps, frames, cols = out_ref.shape
    keep, is_first = attention_masks(steps)
    for tile in range(frames // TILE):
        for pair in range(0, cols, 2 * HEAD):
            query, keyv, value = [
                attention_tile(qkv_ref, tile, j * cols + pair) for j in range(3)
            ]
            mixed = []
            for mine in (is_first, ~is_first):
                probs = attention_probs(jnp.where(mine, query, 0), keyv, keep)
                mixed.append(times(probs.astype(BF), value, 0, 0))
            mixed = jnp.where(is_first, mixed[0], mixed[1]).astype(BF)
            out_ref[:, tile * TILE : (tile + 1) * TILE, pair : pair + 2 * HEAD] = mixed.reshape(
                steps, TILE, 2 * HEAD
            )


def attention_backward_body(qkv_ref, grad_ref, out_ref):
    steps, frames, cols = grad_ref.shape
    keep, is_first = attention_masks(steps)
    scale = 1.0 / math.sqrt(HEAD)
    for tile in range(frames // TILE):
        for pair in range(0, cols, 2 * HEAD):
            query, keyv, value = [
                attention_tile(qkv_ref, tile, j * cols + pair) for j in range(3)
            ]
            grad = attention_tile(grad_ref, tile, pair)
            found = []
            for mine in (is_first, ~is_first):
                probs = attention_probs(jnp.where(mine, query, 0), keyv, keep)
                d_probs = times(value, jnp.where(mine, grad, 0), 1, 1)
                d_value = times(probs.astype(BF), grad, 1, 0)
                d_scores = probs * (d_probs - jnp.sum(probs * d_probs, axis=0, keepdims=True))
                high = d_scores.astype(BF)
                rest = (d_scores - high.astype(F32)).astype(BF)
                d_query = (times(high, keyv, 0, 0) + times(rest, keyv, 0, 0)) * scale
                d_key = (times(high, query, 1, 0) + times(rest, query, 1, 0)) * scale
                found.append((d_query, d_key, d_value))
            for j in range(3):
                part = jnp.where(is_first, found[0][j], found[1][j]).astype(BF)
                start = j * cols + pair
                out_ref[:, tile * TILE : (tile + 1) * TILE, start : start + 2 * HEAD] = (
                    part.reshape(steps, TILE, 2 * HEAD)
                )


def attention_call(body, arrays, cols, span):
    steps, frames = arrays[0].shape[:2]

    def spec(width):
        return pl.BlockSpec((steps, span, width), lambda i: (0, i, 0))

    return pl.pallas_call(
        body,
        grid=(frames // span,),
        in_specs=[spec(a.shape[2]) for a in arrays],
        out_specs=spec(cols),
        out_shape=jax.ShapeDtypeStruct((steps, frames, cols), BF),
    )(*arrays)


def feed_body(
    n2_ref, grad_ref, wgate_ref, wup_ref, wdown_ref, hid_ref, d_gate_ref, d_up_ref, dn2_ref, sum_ref
):
    step = pl.program_id(0)
    wgate, wup = wgate_ref[...], wup_ref[...]
    wdown = jnp.concatenate([wdown_ref[r] for r in range(wdown_ref.shape[0])], axis=1)
    span = min(256, n2_ref.shape[0])
    for start in range(0, n2_ref.shape[0], span):
        rows = slice(start, start + span)
        n2 = n2_ref[rows]
        gate = times(n2, wgate, 1, 0)
        upval = times(n2, wup, 1, 0)
        d_hidden = times(grad_ref[rows], wdown, 1, 1)
        sigma = 1.0 / (1.0 + jnp.exp(-gate))
        silu_val = gate * sigma
        hid_ref[rows] = (silu_val * upval).astype(BF)
        d_gate = (d_hidden * upval * (sigma * (1.0 + gate * (1.0 - sigma)))).astype(BF)
        d_up = (d_hidden * silu_val).astype(BF)
        d_gate_ref[rows] = d_gate
        d_up_ref[rows] = d_up
        part = times(d_gate, wgate, 1, 1) + times(d_up, wup, 1, 1)

        @pl.when(step == 0)
        def _():
            sum_ref[rows] = part

        @pl.when(step > 0)
        def _():
            sum_ref[rows] += part

    @pl.when(step == pl.num_programs(0) - 1)
    def _():
        dn2_ref[...] = sum_ref[...].astype(BF)


def feed_call(n2, grad, wgu, wdown):
    frames, width = n2.shape
    parts, hidden, block = wdown.shape
    span = min(256, hidden)
    count = hidden // span
    whole = pl.BlockSpec((frames, width), lambda i: (0, 0))
    piece = pl.BlockSpec((frames, span), lambda i: (0, i))
    return pl.pallas_call(
        feed_body,
        grid=(count,),
        in_specs=[
            whole,
            whole,
            pl.BlockSpec((width, span), lambda i: (0, i)),
            pl.BlockSpec((width, span), lambda i: (0, i + count)),
            pl.BlockSpec((parts, span, block), lambda i: (0, i, 0)),
        ],
        out_specs=[piece, piece, piece, whole],
        out_shape=[jax.ShapeDtypeStruct((frames, hidden), BF)] * 3
        + [jax.ShapeDtypeStruct((frames, width), BF)],
        scratch_shapes=[pltpu.VMEM((frames, width), F32)],
    )(n2, grad, wgu, wgu, wdown)


def make_step_shards(count, lanes):

    def exchange(blocks):
        return lax.all_to_all(blocks, "dp", 0, 0, tiled=True)

    def collect(rows):
        return lax.all_gather(rows, "tensor", axis=0).reshape(-1, rows.shape[-1])

    def deal(partial):
        slots = partial.astype(BF).reshape(lanes, count, -1, partial.shape[-1])
        return lax.psum_scatter(slots, "tensor", scatter_dimension=0).astype(F32)

    def frame_split(array):
        slots = array.reshape(lanes, count, -1, array.shape[-1])
        slots = jnp.swapaxes(slots, 0, 1)
        return exchange(slots.reshape(count, -1, array.shape[-1]))

    def frame_join(array):
        slots = exchange(array).reshape(count, lanes, -1, array.shape[-1])
        return jnp.swapaxes(slots, 0, 1).reshape(-1, array.shape[-1])

    def rowwise(array):
        return with_layout_constraint(array, Layout(tuple(range(array.ndim))))

    def after(value, *waiting):
        return lax.optimization_barrier((value,) + waiting)

    def shards(
        layer_in, text_mask, w_qkv, w_out, w_gate_up, w_down, norm_gains, pad_row, out_grad
    ):
        me = lax.axis_index("dp")
        steps, local, width = layer_in.shape
        block = width // count

        def tile(line):
            pads = [(0, 0)] * (line.ndim - 1) + [(0, TILE - 1), (0, width - line.shape[-1])]
            return jnp.pad(line[..., None, :], pads)

        small = jnp.concatenate([norm_gains, pad_row[None]], axis=0).astype(BF).reshape(-1)
        line = jnp.concatenate([small, text_mask.astype(BF)])
        notes = jnp.broadcast_to(tile(line)[None], (count, TILE, width))
        hello = exchange(jnp.concatenate([layer_in, notes], axis=1))
        rows_in = hello[:, :local].astype(F32)
        notes = hello[:, local].astype(F32)
        small = jnp.swapaxes(notes[:, : 3 * block].reshape(count, 3, block), 0, 1)
        gain_one, gain_two, pad_vec = small.reshape(3, width)
        padded = jnp.where(me == 0, 1.0 - notes[:, 3 * block : 3 * block + local], 0.0)[..., None]
        h0 = rows_in + padded * pad_vec
        r1 = lax.rsqrt(jnp.mean(h0 * h0, axis=-1, keepdims=True) + EPS)
        n1 = (h0 * r1 * gain_one).astype(BF)
        n1, w_qkv, w_out = after(n1, w_qkv, w_out)
        n1_all = collect(n1)

        w_attn = jnp.concatenate(
            [w_qkv[:, 0], w_qkv[:, 1], w_qkv[:, 2], jnp.swapaxes(w_out, 1, 2)], axis=2
        )
        w_attn = exchange(w_attn.astype(BF)).reshape(width, -1)
        cols = w_attn.shape[1] // 4
        w_in, wout_t = w_attn[:, : 3 * cols], w_attn[:, 3 * cols :]
        w_attn, out_grad = after(w_attn, out_grad)
        grad = exchange(out_grad)
        n1_all, grad = after(n1_all, grad)
        grad_all = collect(grad)
        qkv = jnp.dot(n1_all, w_in, preferred_element_type=F32).astype(BF)

        qkv = frame_split(qkv)
        mixed_all = frame_join(attention_call(attention_forward_body, (qkv,), cols, 2 * TILE))
        attn = jnp.einsum("fe,de->fd", mixed_all, wout_t, preferred_element_type=F32)

        attn, w_down, w_gate_up, grad_all = after(attn.astype(BF), w_down, w_gate_up, grad_all)
        attn = deal(attn)
        wdown = exchange(w_down.astype(BF))
        wgu = jnp.concatenate([w_gate_up[:, 0], w_gate_up[:, 1]], axis=2).astype(BF)
        attn, wdown, wgu = after(attn, wdown, wgu)
        h1 = h0 + attn
        r2 = lax.rsqrt(jnp.mean(h1 * h1, axis=-1, keepdims=True) + EPS)
        n2 = (h1 * r2 * gain_two).astype(BF)
        n2, wgu = after(n2, wgu)
        n2_all = collect(n2)
        wgu = exchange(wgu).reshape(width, -1)

        hidden, d_gate, d_up, dn2 = feed_call(n2_all, grad_all, wgu, wdown)
        hid_width = hidden.shape[1]
        dn2, hidden, d_gate, d_up = after(dn2, hidden, d_gate, d_up)
        dn2 = deal(dn2)
        d_down = jnp.einsum(
            "fk,frd->rkd",
            hidden,
            grad_all.reshape(-1, count, block),
            preferred_element_type=F32,
        )
        g_down = exchange(rowwise(d_down.astype(BF)))
        g_gate = jnp.einsum("fd,fk->dk", n2_all, d_gate, preferred_element_type=F32).astype(BF)
        g_up = jnp.einsum("fd,fk->dk", n2_all, d_up, preferred_element_type=F32).astype(BF)
        part = hid_width // 2
        g_gate = jnp.concatenate([g_gate, g_up[:, :part]], axis=1).reshape(count, block, -1)
        g_up = g_up[:, part:].reshape(count, block, -1)
        dn2, g_down, g_gate, g_up = after(dn2, g_down, g_gate, g_up)
        dh_norm2, dgain_two = norm_back(dn2, h1, r2, gain_two)
        dh1 = grad.astype(F32) + dh_norm2
        dh1_low, g_gate, hidden = after(dh1.astype(BF), g_gate, hidden)
        dh1_all = collect(dh1_low)
        g_gate = exchange(g_gate)
        dh1_all, g_gate = after(dh1_all, g_gate)

        wdown = jnp.swapaxes(wdown, 0, 1).reshape(-1, width)
        ffout = deal(jnp.dot(hidden, wdown, preferred_element_type=F32))
        d_mixed = jnp.dot(dh1_all, wout_t, preferred_element_type=F32).astype(BF)
        d_mixed, g_up = after(frame_split(d_mixed), g_up)
        g_up = exchange(g_up)
        d_qkv = attention_call(attention_backward_body, (qkv, d_mixed), 3 * cols, 2 * TILE)
        d_qkv, g_up = after(d_qkv, g_up)
        g_up = jnp.concatenate([g_gate[..., hid_width:], g_up], axis=2)
        g_gate_up = jnp.stack([g_gate[..., :hid_width], g_up], axis=1).astype(F32)
        d_qkv = frame_join(d_qkv)
        dn1 = jnp.einsum("fe,de->fd", d_qkv, w_in, preferred_element_type=F32).astype(BF)

        dn1, d_qkv, ffout = after(dn1, d_qkv, ffout)
        dn1 = deal(dn1)
        d_attn = jnp.concatenate(
            [
                jnp.einsum("fd,fe->de", n1_all, d_qkv, preferred_element_type=F32).astype(BF),
                jnp.einsum("fd,fe->de", dh1_all, mixed_all, preferred_element_type=F32).astype(BF),
            ],
            axis=1,
        )
        g_attn = exchange(rowwise(d_attn.reshape(count, block, -1)))
        layer_out = (h1 + ffout).astype(BF)
        dn1, g_attn, layer_out = after(dn1, g_attn, layer_out)
        g_down, g_attn = g_down.astype(F32), g_attn.astype(F32)
        g_qkv = jnp.stack([g_attn[..., j * cols : (j + 1) * cols] for j in range(3)], axis=1)
        g_out = jnp.swapaxes(g_attn[..., 3 * cols :], 1, 2)

        dh_norm1, dgain_one = norm_back(dn1, h0, r1, gain_one)
        dh0 = dh1 + dh_norm1
        d_pad = jnp.sum(dh0 * padded, axis=(0, 1))
        sums = jnp.stack([dgain_one, dgain_two, d_pad]).reshape(3, count, block)
        sums = jnp.swapaxes(sums, 0, 1).reshape(count, -1)
        high = sums.astype(BF)
        rest = (sums - high.astype(F32)).astype(BF)
        notes = tile(jnp.concatenate([high, rest], axis=1))
        last = exchange(jnp.concatenate([dh0.astype(BF), layer_out, notes], axis=1))
        g_qkv, g_out = rowwise(g_qkv), rowwise(g_out)
        last, g_gate_up, g_qkv, g_out, g_down = after(last, g_gate_up, g_qkv, g_out, g_down)
        input_grad, layer_out = last[:, :local], last[:, local : 2 * local]
        sums = jnp.sum(last[:, 2 * local].astype(F32), axis=0)[: 6 * block].reshape(2, 3, block)
        sums = sums[0] + sums[1]
        g_small = sums
        for k in range(1, lanes):
            around = [(i, (i + k) % lanes) for i in range(lanes)]
            g_small = g_small + lax.ppermute(sums, "tensor", around)
        return (layer_out, input_grad, g_qkv, g_out, g_gate_up, g_down, g_small[0:2], g_small[2])

    return shards


def spread(body, mesh, dp):
    rows = dp + ("tensor",)
    weights = (
        P(None, None, dp, "tensor"),
        P(None, "tensor", dp),
        P(None, None, dp, "tensor"),
        P(None, "tensor", dp),
        P(None, dp),
        P(dp),
    )
    return jax.shard_map(
        body,
        mesh=mesh,
        in_specs=(P(None, rows, None), P(rows)) + weights + (P(None, rows, None),),
        out_specs=(P(None, rows, None), P(None, rows, None)) + weights,
        check_vma=False,
    )


def solution(mesh):
    dp_size, tensor_size = mesh.shape["dp"], mesh.shape["tensor"]

    def layer(layer_in, *others):
        steps, frames, width = layer_in.shape
        local = frames // (dp_size * tensor_size)
        block = width // dp_size
        fits = 6 * block <= width and 3 * block + local <= width
        if steps == dp_size and dp_size & (dp_size - 1) == 0 and fits:
            body, over, dp = make_step_shards(dp_size, tensor_size), mesh, ("dp",)
        else:
            over = Mesh(
                np.asarray(mesh.devices).reshape(dp_size // 2, 2, tensor_size),
                ("xy", "core", "tensor"),
            )
            body, dp = make_shards(tensor_size), ("xy", "core")
        return spread(body, over, dp)(layer_in, *others)

    return layer
```

```python
import math

import jax
import jax.numpy as jnp
import numpy as np
from jax import lax
from jax.experimental import pallas as pl
from jax.experimental.layout import Layout, with_layout_constraint
from jax.experimental.pallas import tpu as pltpu
from jax.sharding import Mesh
from jax.sharding import PartitionSpec as P

HEAD = 64
EPS = 1e-05
HIGH = lax.Precision.HIGHEST
BF = jnp.bfloat16
F32 = jnp.float32
SWAP = ((0, 1), (1, 0))
TILE = 16


def norm_back(upstream, hval, rstat, gain):
    scaled = upstream * gain
    dgain = jnp.sum(upstream * hval * rstat, axis=(0, 1))
    dhval = rstat * scaled - hval * rstat**3 * jnp.mean(scaled * hval, axis=-1, keepdims=True)
    return (dhval, dgain)


def half(array, axis, which):
    size = array.shape[axis] // 2
    return lax.dynamic_slice_in_dim(array, which * size, size, axis)


def ordered(core, own, other, axis):
    is_first = core == 0
    return jnp.concatenate(
        [jnp.where(is_first, own, other), jnp.where(is_first, other, own)], axis=axis
    )


def make_shards(tensor_size):
    def around(shift):
        return [(i, (i + shift) % tensor_size) for i in range(tensor_size)]

    def trade(core, weight, split_axis, join_axis):
        mine = half(weight, split_axis, core)
        theirs = half(weight, split_axis, 1 - core)
        got = lax.ppermute(theirs, "core", SWAP)
        return ordered(core, mine, got, join_axis)

    def collect(rows):
        parts = [rows] + [
            lax.ppermute(rows, "tensor", around(k)) for k in range(1, tensor_size)
        ]
        near = jnp.stack(parts, axis=1)
        far = lax.ppermute(near, "core", SWAP)
        whole = jnp.concatenate([near, far], axis=1)
        return whole.reshape(rows.shape[0], -1, rows.shape[2])

    def deal(partial):
        steps, frames, width = partial.shape
        split = partial.reshape(steps, 2, tensor_size, frames // (2 * tensor_size), width)
        got = lax.ppermute(split[:, 1].astype(BF), "core", SWAP)
        chip = split[:, 0].astype(F32) + got.astype(F32)
        total = chip[:, 0]
        for k in range(1, tensor_size):
            total = total + lax.ppermute(chip[:, k].astype(BF), "tensor", around(-k)).astype(F32)
        return total

    def shards(
        layer_in, text_mask, w_qkv, w_out, w_gate_up, w_down, norm_gains, pad_row, out_grad
    ):
        core = lax.axis_index("core")
        steps, local_frames, width = layer_in.shape

        w_attn = jnp.concatenate(
            [w_qkv.astype(BF), jnp.swapaxes(w_out, 1, 2)[:, None].astype(BF)], axis=1
        )
        w_attn = lax.all_gather(trade(core, w_attn, 3, 2), "xy", axis=2, tiled=True)
        small = jnp.concatenate([norm_gains, pad_row[None]], axis=0).astype(BF)
        small = lax.all_gather(small, ("xy", "core"), axis=1, tiled=True).astype(F32)
        wgu = lax.all_gather(trade(core, w_gate_up.astype(BF), 3, 2), "xy", axis=2, tiled=True)
        wdown = lax.all_gather(trade(core, w_down.astype(BF), 1, 2), "xy", axis=2, tiled=True)

        gain_one, gain_two, pad_vec = small[0], small[1], small[2]
        maskf = text_mask.astype(F32)
        first = (jnp.arange(steps) == 0).astype(F32)
        h0 = (
            layer_in.astype(F32)
            + first[:, None, None] * (1.0 - maskf)[None, :, None] * pad_vec[None, None, :]
        )
        r1 = lax.rsqrt(jnp.mean(h0 * h0, axis=-1, keepdims=True) + EPS)
        n1 = (h0 * r1 * gain_one).astype(BF)
        n1_all = collect(n1)
        grad_all = collect(out_grad)
        frames = n1_all.shape[1]
        wqkv, wout_t = w_attn[:, :3], w_attn[:, 3]
        qkv = jnp.einsum("sfd,sjde->sjfe", n1_all, wqkv, preferred_element_type=F32).astype(BF)
        col_width = qkv.shape[-1]
        heads = col_width // HEAD
        scale = 1.0 / math.sqrt(HEAD)
        query = qkv[:, 0].reshape(steps, frames, heads, HEAD)
        keyv = qkv[:, 1].reshape(steps, frames, heads, HEAD)
        value = qkv[:, 2].reshape(steps, frames, heads, HEAD)
        causal = jnp.arange(steps)[:, None] >= jnp.arange(steps)[None, :]

        def score_of(qv, kv):
            raw = jnp.einsum("sfhe,tfhe->fhst", qv, kv, preferred_element_type=F32) * scale
            return jnp.where(causal, raw, -1e30)

        scores = score_of(query, keyv)
        top = jnp.max(scores, axis=-1, keepdims=True)
        expo = jnp.exp(scores - top)
        total = jnp.sum(expo, axis=-1, keepdims=True)
        lse = top + jnp.log(total)
        probs_low = (expo / total).astype(BF)
        mixed = jnp.einsum("fhst,tfhe->sfhe", probs_low, value, preferred_element_type=F32)
        mixed = mixed.reshape(steps, frames, col_width).astype(BF)
        attn = deal(jnp.einsum("sfd,sed->sfe", mixed, wout_t, preferred_element_type=F32))
        h1 = h0 + attn
        r2 = lax.rsqrt(jnp.mean(h1 * h1, axis=-1, keepdims=True) + EPS)
        n2 = (h1 * r2 * gain_two).astype(BF)
        n2_all = collect(n2)
        gate_up = jnp.einsum("sfd,sjde->sjfe", n2_all, wgu, preferred_element_type=F32)
        gate = gate_up[:, 0]
        upval = gate_up[:, 1]
        sigma = jax.nn.sigmoid(gate)
        silu_val = gate * sigma
        hidden = (silu_val * upval).astype(BF)
        d_down = jnp.einsum("sfk,sfd->skd", hidden, grad_all, preferred_element_type=F32)
        r_down = lax.psum_scatter(d_down.astype(BF), "xy", scatter_dimension=2, tiled=True)
        d_hidden = jnp.einsum("sfd,skd->sfk", grad_all, wdown, preferred_element_type=F32)
        d_gate = d_hidden * upval * (sigma * (1.0 + gate * (1.0 - sigma)))
        d_up = d_hidden * silu_val
        d_gu = jnp.stack([d_gate, d_up], axis=1).astype(BF)
        d_gate_up = jnp.einsum("sfd,sjfe->sjde", n2_all, d_gu, preferred_element_type=F32)
        r_gate_up = lax.psum_scatter(d_gate_up.astype(BF), "xy", scatter_dimension=2, tiled=True)
        dn2 = deal(jnp.einsum("sjfe,sjde->sfd", d_gu, wgu, preferred_element_type=F32))
        dh_norm2, dgain_two = norm_back(dn2, h1, r2, gain_two)
        dh1 = out_grad.astype(F32) + dh_norm2
        dh1_all = collect(dh1.astype(BF))
        ffout = deal(jnp.einsum("sfk,skd->sfd", hidden, wdown, preferred_element_type=F32))
        layer_out = (h1 + ffout).astype(BF)
        d_out_t = jnp.einsum("sfe,sfd->sed", dh1_all, mixed, preferred_element_type=F32)
        d_mixed = jnp.einsum("sfe,sed->sfd", dh1_all, wout_t, preferred_element_type=F32)
        d_mixed = d_mixed.astype(BF).reshape(steps, frames, heads, HEAD)
        probs = jnp.exp(score_of(query, keyv) - lse)
        d_probs = jnp.einsum("sfhe,tfhe->fhst", d_mixed, value, preferred_element_type=F32)
        d_value = jnp.einsum("fhst,sfhe->tfhe", probs_low, d_mixed, preferred_element_type=F32)
        d_scores = probs * (d_probs - jnp.sum(probs * d_probs, axis=-1, keepdims=True))
        d_query = (
            jnp.einsum("fhst,tfhe->sfhe", d_scores, keyv.astype(F32), precision=HIGH) * scale
        )
        d_key = (
            jnp.einsum("fhst,sfhe->tfhe", d_scores, query.astype(F32), precision=HIGH) * scale
        )
        d_qkv = jnp.stack(
            [
                d_query.reshape(steps, frames, col_width),
                d_key.reshape(steps, frames, col_width),
                d_value.reshape(steps, frames, col_width),
            ],
            axis=1,
        ).astype(BF)
        d_wqkv = jnp.einsum("sfd,sjfe->sjde", n1_all, d_qkv, preferred_element_type=F32)
        d_attn = jnp.concatenate([d_wqkv.astype(BF), d_out_t[:, None].astype(BF)], axis=1)
        r_attn = lax.psum_scatter(d_attn, "xy", scatter_dimension=2, tiled=True)
        dn1 = deal(jnp.einsum("sjfe,sjde->sfd", d_qkv, wqkv, preferred_element_type=F32))
        dh_norm1, dgain_one = norm_back(dn1, h0, r1, gain_one)
        dh0 = dh1 + dh_norm1
        input_grad = dh0.astype(BF)
        d_pad = jnp.sum(dh0[0] * (1.0 - maskf)[:, None], axis=0)
        small_grad = jnp.stack([dgain_one, dgain_two, d_pad], axis=0)
        small_grad = lax.psum(small_grad, ("xy", "core", "tensor"))
        place = lax.axis_index("xy") * 2 + core
        g_small = lax.dynamic_slice_in_dim(
            small_grad, place * pad_row.shape[0], pad_row.shape[0], 1
        )

        def settle(reduced, split_axis, join_axis):
            return trade(core, reduced, split_axis, join_axis).astype(F32)

        g_down = settle(r_down, 2, 1)
        g_gate_up = settle(r_gate_up, 2, 3)
        g_attn = settle(r_attn, 2, 3)
        g_qkv = g_attn[:, :3]
        g_out = jnp.swapaxes(g_attn[:, 3], 1, 2)
        return (layer_out, input_grad, g_qkv, g_out, g_gate_up, g_down, g_small[0:2], g_small[2])

    return shards


def attention_masks(steps):
    size = steps * TILE
    row = lax.broadcasted_iota(jnp.int32, (size, size), 0)
    col = lax.broadcasted_iota(jnp.int32, (size, size), 1)
    keep = (row % TILE == col % TILE) & (row <= col)
    lane = lax.broadcasted_iota(jnp.int32, (size, 2 * HEAD), 1)
    return keep, lane < HEAD


def times(left, right, left_axis, right_axis):
    return lax.dot_general(
        left, right, (((left_axis,), (right_axis,)), ((), ())), preferred_element_type=F32
    )


def attention_probs(query, keyv, keep):
    scores = jnp.where(keep, times(keyv, query, 1, 1) * (1.0 / math.sqrt(HEAD)), -1e30)
    expo = jnp.exp(scores - jnp.max(scores, axis=0, keepdims=True))
    return expo * (1.0 / jnp.sum(expo, axis=0, keepdims=True))


def attention_tile(ref, tile, start):
    part = ref[:, tile * TILE : (tile + 1) * TILE, start : start + 2 * HEAD]
    return part.reshape(-1, 2 * HEAD)


def attention_forward_body(qkv_ref, out_ref):
    steps, frames, cols = out_ref.shape
    keep, is_first = attention_masks(steps)
    for tile in range(frames // TILE):
        for pair in range(0, cols, 2 * HEAD):
            query, keyv, value = [
                attention_tile(qkv_ref, tile, j * cols + pair) for j in range(3)
            ]
            mixed = []
            for mine in (is_first, ~is_first):
                probs = attention_probs(jnp.where(mine, query, 0), keyv, keep)
                mixed.append(times(probs.astype(BF), value, 0, 0))
            mixed = jnp.where(is_first, mixed[0], mixed[1]).astype(BF)
            out_ref[:, tile * TILE : (tile + 1) * TILE, pair : pair + 2 * HEAD] = mixed.reshape(
                steps, TILE, 2 * HEAD
            )


def attention_backward_body(qkv_ref, grad_ref, out_ref):
    steps, frames, cols = grad_ref.shape
    keep, is_first = attention_masks(steps)
    scale = 1.0 / math.sqrt(HEAD)
    for tile in range(frames // TILE):
        for pair in range(0, cols, 2 * HEAD):
            query, keyv, value = [
                attention_tile(qkv_ref, tile, j * cols + pair) for j in range(3)
            ]
            grad = attention_tile(grad_ref, tile, pair)
            found = []
            for mine in (is_first, ~is_first):
                probs = attention_probs(jnp.where(mine, query, 0), keyv, keep)
                d_probs = times(value, jnp.where(mine, grad, 0), 1, 1)
                d_value = times(probs.astype(BF), grad, 1, 0)
                d_scores = probs * (d_probs - jnp.sum(probs * d_probs, axis=0, keepdims=True))
                high = d_scores.astype(BF)
                rest = (d_scores - high.astype(F32)).astype(BF)
                d_query = (times(high, keyv, 0, 0) + times(rest, keyv, 0, 0)) * scale
                d_key = (times(high, query, 1, 0) + times(rest, query, 1, 0)) * scale
                found.append((d_query, d_key, d_value))
            for j in range(3):
                part = jnp.where(is_first, found[0][j], found[1][j]).astype(BF)
                start = j * cols + pair
                out_ref[:, tile * TILE : (tile + 1) * TILE, start : start + 2 * HEAD] = (
                    part.reshape(steps, TILE, 2 * HEAD)
                )


def attention_call(body, arrays, cols, span):
    steps, frames = arrays[0].shape[:2]

    def spec(width):
        return pl.BlockSpec((steps, span, width), lambda i: (0, i, 0))

    return pl.pallas_call(
        body,
        grid=(frames // span,),
        in_specs=[spec(a.shape[2]) for a in arrays],
        out_specs=spec(cols),
        out_shape=jax.ShapeDtypeStruct((steps, frames, cols), BF),
    )(*arrays)


def feed_body(
    n2_ref, grad_ref, wgate_ref, wup_ref, wdown_ref, wrow_ref,
    hid_ref, d_gate_ref, d_up_ref, dn2_ref, kept_ref,
):
    step = pl.program_id(0)
    count = kept_ref.shape[0]

    @pl.when(step < count)
    def _():
        wdown = jnp.concatenate([wdown_ref[r] for r in range(wdown_ref.shape[0])], axis=1)
        gate = times(n2_ref[...], wgate_ref[...], 1, 0)
        upval = times(n2_ref[...], wup_ref[...], 1, 0)
        d_hidden = times(grad_ref[...], wdown, 1, 1)
        sigma = 1.0 / (1.0 + jnp.exp(-gate))
        silu_val = gate * sigma
        hid_ref[...] = (silu_val * upval).astype(BF)
        d_gate = (d_hidden * upval * (sigma * (1.0 + gate * (1.0 - sigma)))).astype(BF)
        d_up = (d_hidden * silu_val).astype(BF)
        d_gate_ref[...] = d_gate
        d_up_ref[...] = d_up
        kept_ref[step, 0] = d_gate
        kept_ref[step, 1] = d_up

    @pl.when(step >= count)
    def _():
        kept = [kept_ref[k, half] for half in range(2) for k in range(count)]
        dn2_ref[...] = times(jnp.concatenate(kept, axis=1), wrow_ref[...], 1, 1).astype(BF)


def feed_call(n2, grad, wgu, wdown):
    frames, width = n2.shape
    parts, hidden, block = wdown.shape
    span, part = min(256, hidden), min(512, width)
    count = hidden // span

    def hid_block(i):
        return jnp.minimum(i, count - 1)

    def out_block(i):
        return jnp.maximum(i - count, 0)

    whole = pl.BlockSpec((frames, width), lambda i: (0, 0))
    piece = pl.BlockSpec((frames, span), lambda i: (0, hid_block(i)))
    return pl.pallas_call(
        feed_body,
        grid=(count + width // part,),
        in_specs=[
            whole,
            whole,
            pl.BlockSpec((width, span), lambda i: (0, hid_block(i))),
            pl.BlockSpec((width, span), lambda i: (0, hid_block(i) + count)),
            pl.BlockSpec((parts, span, block), lambda i: (0, hid_block(i), 0)),
            pl.BlockSpec((part, 2 * hidden), lambda i: (out_block(i), 0)),
        ],
        out_specs=[piece, piece, piece, pl.BlockSpec((frames, part), lambda i: (0, out_block(i)))],
        out_shape=[jax.ShapeDtypeStruct((frames, hidden), BF)] * 3
        + [jax.ShapeDtypeStruct((frames, width), BF)],
        scratch_shapes=[pltpu.VMEM((count, 2, frames, span), BF)],
    )(n2, grad, wgu, wgu, wdown, wgu)


def make_step_shards(count, lanes):

    def exchange(blocks):
        return lax.all_to_all(blocks, "dp", 0, 0, tiled=True)

    def collect(rows):
        return lax.all_gather(rows, "tensor", axis=0).reshape(-1, rows.shape[-1])

    def deal(partial):
        slots = partial.astype(BF).reshape(lanes, count, -1, partial.shape[-1])
        return lax.psum_scatter(slots, "tensor", scatter_dimension=0)

    def frame_split(array):
        slots = array.reshape(lanes, count, -1, array.shape[-1])
        slots = jnp.swapaxes(slots, 0, 1)
        return exchange(slots.reshape(count, -1, array.shape[-1]))

    def frame_join(array):
        slots = exchange(array).reshape(count, lanes, -1, array.shape[-1])
        return jnp.swapaxes(slots, 0, 1).reshape(-1, array.shape[-1])

    def rowwise(array):
        return with_layout_constraint(array, Layout(tuple(range(array.ndim))))

    def after(value, *waiting):
        return lax.optimization_barrier((value,) + waiting)

    def shards(
        layer_in, text_mask, w_qkv, w_out, w_gate_up, w_down, norm_gains, pad_row, out_grad
    ):
        me = lax.axis_index("dp")
        steps, local, width = layer_in.shape
        block = width // count

        def tile(line):
            pads = [(0, 0)] * (line.ndim - 1) + [(0, TILE - 1), (0, width - line.shape[-1])]
            return jnp.pad(line[..., None, :], pads)

        small = jnp.concatenate([norm_gains, pad_row[None]], axis=0).astype(BF).reshape(-1)
        line = jnp.concatenate([small, text_mask.astype(BF)])
        notes = jnp.broadcast_to(tile(line)[None], (count, TILE, width))
        hello = exchange(jnp.concatenate([layer_in, notes], axis=1))
        rows_in = hello[:, :local].astype(F32)
        notes = hello[:, local].astype(F32)
        small = jnp.swapaxes(notes[:, : 3 * block].reshape(count, 3, block), 0, 1)
        gain_one, gain_two, pad_vec = small.reshape(3, width)
        padded = jnp.where(me == 0, 1.0 - notes[:, 3 * block : 3 * block + local], 0.0)[..., None]
        h0 = rows_in + padded * pad_vec
        r1 = lax.rsqrt(jnp.mean(h0 * h0, axis=-1, keepdims=True) + EPS)
        n1 = (h0 * r1 * gain_one).astype(BF)
        n1, w_qkv, w_out = after(n1, w_qkv, w_out)
        n1_all = collect(n1)

        w_attn = jnp.concatenate(
            [w_qkv[:, 0], w_qkv[:, 1], w_qkv[:, 2], jnp.swapaxes(w_out, 1, 2)], axis=2
        )
        w_attn = exchange(w_attn.astype(BF)).reshape(width, -1)
        cols = w_attn.shape[1] // 4
        w_in, wout_t = w_attn[:, : 3 * cols], w_attn[:, 3 * cols :]
        w_attn, out_grad = after(w_attn, out_grad)
        grad = exchange(out_grad)
        n1_all, grad = after(n1_all, grad)
        grad_all = collect(grad)
        qkv = jnp.dot(n1_all, w_in, preferred_element_type=F32).astype(BF)

        qkv = frame_split(qkv)
        mixed_all = frame_join(attention_call(attention_forward_body, (qkv,), cols, 2 * TILE))
        attn = jnp.einsum("fe,de->fd", mixed_all, wout_t, preferred_element_type=F32)

        attn, w_down, w_gate_up, grad_all = after(attn.astype(BF), w_down, w_gate_up, grad_all)
        attn = deal(attn)
        wdown = exchange(w_down.astype(BF))
        wgu = jnp.concatenate([w_gate_up[:, 0], w_gate_up[:, 1]], axis=2).astype(BF)
        wdown, wgu = after(wdown, wgu)
        attn, wdown = after(attn, wdown)
        wgu = exchange(wgu).reshape(width, -1)
        h1 = h0 + attn.astype(F32)
        r2 = lax.rsqrt(jnp.mean(h1 * h1, axis=-1, keepdims=True) + EPS)
        n2 = (h1 * r2 * gain_two).astype(BF)
        n2_all = collect(n2)

        hidden, d_gate, d_up, dn2 = feed_call(n2_all, grad_all, wgu, wdown)
        hid_width = hidden.shape[1]
        dn2, hidden, d_gate, d_up = after(dn2, hidden, d_gate, d_up)
        dn2 = deal(dn2)
        d_down = jnp.einsum(
            "fk,frd->rkd",
            hidden,
            grad_all.reshape(-1, count, block),
            preferred_element_type=F32,
        )
        g_down = exchange(rowwise(d_down.astype(BF)))
        g_gate = jnp.einsum("fd,fk->dk", n2_all, d_gate, preferred_element_type=F32).astype(BF)
        g_up = jnp.einsum("fd,fk->dk", n2_all, d_up, preferred_element_type=F32).astype(BF)
        part = hid_width // 2
        g_gate = jnp.concatenate([g_gate, g_up[:, :part]], axis=1).reshape(count, block, -1)
        g_up = g_up[:, part:].reshape(count, block, -1)
        dn2, g_down, g_gate, g_up = after(dn2, g_down, g_gate, g_up)
        dh_norm2, dgain_two = norm_back(dn2.astype(F32), h1, r2, gain_two)
        dh1 = grad.astype(F32) + dh_norm2
        dh1_low, g_gate, hidden = after(dh1.astype(BF), g_gate, hidden)
        dh1_all = collect(dh1_low)
        g_gate = exchange(g_gate)
        dh1_all, g_gate = after(dh1_all, g_gate)

        wdown = jnp.swapaxes(wdown, 0, 1).reshape(-1, width)
        ffout = deal(jnp.dot(hidden, wdown, preferred_element_type=F32))
        d_mixed = jnp.dot(dh1_all, wout_t, preferred_element_type=F32).astype(BF)
        d_mixed, g_up = after(frame_split(d_mixed), g_up)
        g_up = exchange(g_up)
        d_qkv = attention_call(attention_backward_body, (qkv, d_mixed), 3 * cols, 2 * TILE)
        d_qkv, g_up = after(d_qkv, g_up)
        g_up = jnp.concatenate([g_gate[..., hid_width:], g_up], axis=2)
        g_gate_up = jnp.stack([g_gate[..., :hid_width], g_up], axis=1).astype(F32)
        d_qkv = frame_join(d_qkv)
        dn1 = jnp.einsum("fe,de->fd", d_qkv, w_in, preferred_element_type=F32).astype(BF)

        dn1, d_qkv, ffout = after(dn1, d_qkv, ffout)
        dn1 = deal(dn1)
        d_attn = jnp.concatenate(
            [
                jnp.einsum("fd,fe->de", n1_all, d_qkv, preferred_element_type=F32).astype(BF),
                jnp.einsum("fd,fe->de", dh1_all, mixed_all, preferred_element_type=F32).astype(BF),
            ],
            axis=1,
        )
        g_attn = exchange(rowwise(d_attn.reshape(count, block, -1)))
        layer_out = (h1 + ffout.astype(F32)).astype(BF)
        dn1, g_attn, layer_out = after(dn1, g_attn, layer_out)
        g_down, g_attn = g_down.astype(F32), g_attn.astype(F32)
        g_qkv = jnp.stack([g_attn[..., j * cols : (j + 1) * cols] for j in range(3)], axis=1)
        g_out = jnp.swapaxes(g_attn[..., 3 * cols :], 1, 2)

        dh_norm1, dgain_one = norm_back(dn1.astype(F32), h0, r1, gain_one)
        dh0 = dh1 + dh_norm1
        d_pad = jnp.sum(dh0 * padded, axis=(0, 1))
        sums = jnp.stack([dgain_one, dgain_two, d_pad])
        last = exchange(jnp.concatenate([dh0.astype(BF), layer_out], axis=1))

        total = sums
        for k in range(1, lanes):
            around = [(i, (i + k) % lanes) for i in range(lanes)]
            total = total + lax.ppermute(sums, "tensor", around)
        total = jnp.swapaxes(total.reshape(3, count, block), 0, 1)
        g_small = lax.dynamic_index_in_dim(total, me, 0, keepdims=False)
        for k in range(1, count):
            theirs = lax.dynamic_index_in_dim(total, me ^ k, 0, keepdims=False)
            g_small = g_small + lax.ppermute(theirs, "dp", [(i, i ^ k) for i in range(count)])

        g_qkv, g_out = rowwise(g_qkv), rowwise(g_out)
        last, g_small, g_gate_up, g_qkv, g_out, g_down = after(
            last, g_small, g_gate_up, g_qkv, g_out, g_down
        )
        input_grad, layer_out = last[:, :local], last[:, local:]
        return (layer_out, input_grad, g_qkv, g_out, g_gate_up, g_down, g_small[0:2], g_small[2])

    return shards


def spread(body, mesh, dp):
    rows = dp + ("tensor",)
    weights = (
        P(None, None, dp, "tensor"),
        P(None, "tensor", dp),
        P(None, None, dp, "tensor"),
        P(None, "tensor", dp),
        P(None, dp),
        P(dp),
    )
    return jax.shard_map(
        body,
        mesh=mesh,
        in_specs=(P(None, rows, None), P(rows)) + weights + (P(None, rows, None),),
        out_specs=(P(None, rows, None), P(None, rows, None)) + weights,
        check_vma=False,
    )


def solution(mesh):
    dp_size, tensor_size = mesh.shape["dp"], mesh.shape["tensor"]

    def layer(layer_in, *others):
        steps, frames, width = layer_in.shape
        local = frames // (dp_size * tensor_size)
        block = width // dp_size
        fits = 3 * block + local <= width
        if steps == dp_size and dp_size & (dp_size - 1) == 0 and fits:
            body, over, dp = make_step_shards(dp_size, tensor_size), mesh, ("dp",)
        else:
            over = Mesh(
                np.asarray(mesh.devices).reshape(dp_size // 2, 2, tensor_size),
                ("xy", "core", "tensor"),
            )
            body, dp = make_shards(tensor_size), ("xy", "core")
        return spread(body, over, dp)(layer_in, *others)

    return layer
```

```python
import math

import jax
import jax.numpy as jnp
import numpy as np
from jax import lax
from jax.experimental import pallas as pl
from jax.experimental.layout import Layout, with_layout_constraint
from jax.experimental.pallas import tpu as pltpu
from jax.sharding import Mesh
from jax.sharding import PartitionSpec as P

HEAD = 64
EPS = 1e-05
HIGH = lax.Precision.HIGHEST
BF = jnp.bfloat16
F32 = jnp.float32
SWAP = ((0, 1), (1, 0))
TILE = 16


def norm_back(upstream, hval, rstat, gain):
    scaled = upstream * gain
    dgain = jnp.sum(upstream * hval * rstat, axis=(0, 1))
    dhval = rstat * scaled - hval * rstat**3 * jnp.mean(scaled * hval, axis=-1, keepdims=True)
    return (dhval, dgain)


def half(array, axis, which):
    size = array.shape[axis] // 2
    return lax.dynamic_slice_in_dim(array, which * size, size, axis)


def ordered(core, own, other, axis):
    is_first = core == 0
    return jnp.concatenate(
        [jnp.where(is_first, own, other), jnp.where(is_first, other, own)], axis=axis
    )


def make_shards(tensor_size):
    def around(shift):
        return [(i, (i + shift) % tensor_size) for i in range(tensor_size)]

    def trade(core, weight, split_axis, join_axis):
        mine = half(weight, split_axis, core)
        theirs = half(weight, split_axis, 1 - core)
        got = lax.ppermute(theirs, "core", SWAP)
        return ordered(core, mine, got, join_axis)

    def collect(rows):
        parts = [rows] + [
            lax.ppermute(rows, "tensor", around(k)) for k in range(1, tensor_size)
        ]
        near = jnp.stack(parts, axis=1)
        far = lax.ppermute(near, "core", SWAP)
        whole = jnp.concatenate([near, far], axis=1)
        return whole.reshape(rows.shape[0], -1, rows.shape[2])

    def deal(partial):
        steps, frames, width = partial.shape
        split = partial.reshape(steps, 2, tensor_size, frames // (2 * tensor_size), width)
        got = lax.ppermute(split[:, 1].astype(BF), "core", SWAP)
        chip = split[:, 0].astype(F32) + got.astype(F32)
        total = chip[:, 0]
        for k in range(1, tensor_size):
            total = total + lax.ppermute(chip[:, k].astype(BF), "tensor", around(-k)).astype(F32)
        return total

    def shards(
        layer_in, text_mask, w_qkv, w_out, w_gate_up, w_down, norm_gains, pad_row, out_grad
    ):
        core = lax.axis_index("core")
        steps, local_frames, width = layer_in.shape

        w_attn = jnp.concatenate(
            [w_qkv.astype(BF), jnp.swapaxes(w_out, 1, 2)[:, None].astype(BF)], axis=1
        )
        w_attn = lax.all_gather(trade(core, w_attn, 3, 2), "xy", axis=2, tiled=True)
        small = jnp.concatenate([norm_gains, pad_row[None]], axis=0).astype(BF)
        small = lax.all_gather(small, ("xy", "core"), axis=1, tiled=True).astype(F32)
        wgu = lax.all_gather(trade(core, w_gate_up.astype(BF), 3, 2), "xy", axis=2, tiled=True)
        wdown = lax.all_gather(trade(core, w_down.astype(BF), 1, 2), "xy", axis=2, tiled=True)

        gain_one, gain_two, pad_vec = small[0], small[1], small[2]
        maskf = text_mask.astype(F32)
        first = (jnp.arange(steps) == 0).astype(F32)
        h0 = (
            layer_in.astype(F32)
            + first[:, None, None] * (1.0 - maskf)[None, :, None] * pad_vec[None, None, :]
        )
        r1 = lax.rsqrt(jnp.mean(h0 * h0, axis=-1, keepdims=True) + EPS)
        n1 = (h0 * r1 * gain_one).astype(BF)
        n1_all = collect(n1)
        grad_all = collect(out_grad)
        frames = n1_all.shape[1]
        wqkv, wout_t = w_attn[:, :3], w_attn[:, 3]
        qkv = jnp.einsum("sfd,sjde->sjfe", n1_all, wqkv, preferred_element_type=F32).astype(BF)
        col_width = qkv.shape[-1]
        heads = col_width // HEAD
        scale = 1.0 / math.sqrt(HEAD)
        query = qkv[:, 0].reshape(steps, frames, heads, HEAD)
        keyv = qkv[:, 1].reshape(steps, frames, heads, HEAD)
        value = qkv[:, 2].reshape(steps, frames, heads, HEAD)
        causal = jnp.arange(steps)[:, None] >= jnp.arange(steps)[None, :]

        def score_of(qv, kv):
            raw = jnp.einsum("sfhe,tfhe->fhst", qv, kv, preferred_element_type=F32) * scale
            return jnp.where(causal, raw, -1e30)

        scores = score_of(query, keyv)
        top = jnp.max(scores, axis=-1, keepdims=True)
        expo = jnp.exp(scores - top)
        total = jnp.sum(expo, axis=-1, keepdims=True)
        lse = top + jnp.log(total)
        probs_low = (expo / total).astype(BF)
        mixed = jnp.einsum("fhst,tfhe->sfhe", probs_low, value, preferred_element_type=F32)
        mixed = mixed.reshape(steps, frames, col_width).astype(BF)
        attn = deal(jnp.einsum("sfd,sed->sfe", mixed, wout_t, preferred_element_type=F32))
        h1 = h0 + attn
        r2 = lax.rsqrt(jnp.mean(h1 * h1, axis=-1, keepdims=True) + EPS)
        n2 = (h1 * r2 * gain_two).astype(BF)
        n2_all = collect(n2)
        gate_up = jnp.einsum("sfd,sjde->sjfe", n2_all, wgu, preferred_element_type=F32)
        gate = gate_up[:, 0]
        upval = gate_up[:, 1]
        sigma = jax.nn.sigmoid(gate)
        silu_val = gate * sigma
        hidden = (silu_val * upval).astype(BF)
        d_down = jnp.einsum("sfk,sfd->skd", hidden, grad_all, preferred_element_type=F32)
        r_down = lax.psum_scatter(d_down.astype(BF), "xy", scatter_dimension=2, tiled=True)
        d_hidden = jnp.einsum("sfd,skd->sfk", grad_all, wdown, preferred_element_type=F32)
        d_gate = d_hidden * upval * (sigma * (1.0 + gate * (1.0 - sigma)))
        d_up = d_hidden * silu_val
        d_gu = jnp.stack([d_gate, d_up], axis=1).astype(BF)
        d_gate_up = jnp.einsum("sfd,sjfe->sjde", n2_all, d_gu, preferred_element_type=F32)
        r_gate_up = lax.psum_scatter(d_gate_up.astype(BF), "xy", scatter_dimension=2, tiled=True)
        dn2 = deal(jnp.einsum("sjfe,sjde->sfd", d_gu, wgu, preferred_element_type=F32))
        dh_norm2, dgain_two = norm_back(dn2, h1, r2, gain_two)
        dh1 = out_grad.astype(F32) + dh_norm2
        dh1_all = collect(dh1.astype(BF))
        ffout = deal(jnp.einsum("sfk,skd->sfd", hidden, wdown, preferred_element_type=F32))
        layer_out = (h1 + ffout).astype(BF)
        d_out_t = jnp.einsum("sfe,sfd->sed", dh1_all, mixed, preferred_element_type=F32)
        d_mixed = jnp.einsum("sfe,sed->sfd", dh1_all, wout_t, preferred_element_type=F32)
        d_mixed = d_mixed.astype(BF).reshape(steps, frames, heads, HEAD)
        probs = jnp.exp(score_of(query, keyv) - lse)
        d_probs = jnp.einsum("sfhe,tfhe->fhst", d_mixed, value, preferred_element_type=F32)
        d_value = jnp.einsum("fhst,sfhe->tfhe", probs_low, d_mixed, preferred_element_type=F32)
        d_scores = probs * (d_probs - jnp.sum(probs * d_probs, axis=-1, keepdims=True))
        d_query = (
            jnp.einsum("fhst,tfhe->sfhe", d_scores, keyv.astype(F32), precision=HIGH) * scale
        )
        d_key = (
            jnp.einsum("fhst,sfhe->tfhe", d_scores, query.astype(F32), precision=HIGH) * scale
        )
        d_qkv = jnp.stack(
            [
                d_query.reshape(steps, frames, col_width),
                d_key.reshape(steps, frames, col_width),
                d_value.reshape(steps, frames, col_width),
            ],
            axis=1,
        ).astype(BF)
        d_wqkv = jnp.einsum("sfd,sjfe->sjde", n1_all, d_qkv, preferred_element_type=F32)
        d_attn = jnp.concatenate([d_wqkv.astype(BF), d_out_t[:, None].astype(BF)], axis=1)
        r_attn = lax.psum_scatter(d_attn, "xy", scatter_dimension=2, tiled=True)
        dn1 = deal(jnp.einsum("sjfe,sjde->sfd", d_qkv, wqkv, preferred_element_type=F32))
        dh_norm1, dgain_one = norm_back(dn1, h0, r1, gain_one)
        dh0 = dh1 + dh_norm1
        input_grad = dh0.astype(BF)
        d_pad = jnp.sum(dh0[0] * (1.0 - maskf)[:, None], axis=0)
        small_grad = jnp.stack([dgain_one, dgain_two, d_pad], axis=0)
        small_grad = lax.psum(small_grad, ("xy", "core", "tensor"))
        place = lax.axis_index("xy") * 2 + core
        g_small = lax.dynamic_slice_in_dim(
            small_grad, place * pad_row.shape[0], pad_row.shape[0], 1
        )

        def settle(reduced, split_axis, join_axis):
            return trade(core, reduced, split_axis, join_axis).astype(F32)

        g_down = settle(r_down, 2, 1)
        g_gate_up = settle(r_gate_up, 2, 3)
        g_attn = settle(r_attn, 2, 3)
        g_qkv = g_attn[:, :3]
        g_out = jnp.swapaxes(g_attn[:, 3], 1, 2)
        return (layer_out, input_grad, g_qkv, g_out, g_gate_up, g_down, g_small[0:2], g_small[2])

    return shards


def attention_masks(steps):
    size = steps * TILE
    row = lax.broadcasted_iota(jnp.int32, (size, size), 0)
    col = lax.broadcasted_iota(jnp.int32, (size, size), 1)
    keep = (row % TILE == col % TILE) & (row <= col)
    lane = lax.broadcasted_iota(jnp.int32, (size, 2 * HEAD), 1)
    return keep, lane < HEAD


def times(left, right, left_axis, right_axis):
    return lax.dot_general(
        left, right, (((left_axis,), (right_axis,)), ((), ())), preferred_element_type=F32
    )


def attention_probs(query, keyv, keep):
    scores = jnp.where(keep, times(keyv, query, 1, 1) * (1.0 / math.sqrt(HEAD)), -1e30)
    expo = jnp.exp(scores - jnp.max(scores, axis=0, keepdims=True))
    return expo * (1.0 / jnp.sum(expo, axis=0, keepdims=True))


def attention_tile(ref, tile, start):
    part = ref[:, tile * TILE : (tile + 1) * TILE, start : start + 2 * HEAD]
    return part.reshape(-1, 2 * HEAD)


def attention_forward_body(qkv_ref, out_ref):
    steps, frames, cols = out_ref.shape
    keep, is_first = attention_masks(steps)
    for tile in range(frames // TILE):
        for pair in range(0, cols, 2 * HEAD):
            query, keyv, value = [
                attention_tile(qkv_ref, tile, j * cols + pair) for j in range(3)
            ]
            mixed = []
            for mine in (is_first, ~is_first):
                probs = attention_probs(jnp.where(mine, query, 0), keyv, keep)
                mixed.append(times(probs.astype(BF), value, 0, 0))
            mixed = jnp.where(is_first, mixed[0], mixed[1]).astype(BF)
            out_ref[:, tile * TILE : (tile + 1) * TILE, pair : pair + 2 * HEAD] = mixed.reshape(
                steps, TILE, 2 * HEAD
            )


def attention_backward_body(qkv_ref, grad_ref, out_ref):
    steps, frames, cols = grad_ref.shape
    keep, is_first = attention_masks(steps)
    scale = 1.0 / math.sqrt(HEAD)
    for tile in range(frames // TILE):
        for pair in range(0, cols, 2 * HEAD):
            query, keyv, value = [
                attention_tile(qkv_ref, tile, j * cols + pair) for j in range(3)
            ]
            grad = attention_tile(grad_ref, tile, pair)
            found = []
            for mine in (is_first, ~is_first):
                probs = attention_probs(jnp.where(mine, query, 0), keyv, keep)
                d_probs = times(value, jnp.where(mine, grad, 0), 1, 1)
                d_value = times(probs.astype(BF), grad, 1, 0)
                d_scores = probs * (d_probs - jnp.sum(probs * d_probs, axis=0, keepdims=True))
                high = d_scores.astype(BF)
                rest = (d_scores - high.astype(F32)).astype(BF)
                d_query = (times(high, keyv, 0, 0) + times(rest, keyv, 0, 0)) * scale
                d_key = (times(high, query, 1, 0) + times(rest, query, 1, 0)) * scale
                found.append((d_query, d_key, d_value))
            for j in range(3):
                part = jnp.where(is_first, found[0][j], found[1][j]).astype(BF)
                start = j * cols + pair
                out_ref[:, tile * TILE : (tile + 1) * TILE, start : start + 2 * HEAD] = (
                    part.reshape(steps, TILE, 2 * HEAD)
                )


def attention_call(body, arrays, cols, span):
    steps, frames = arrays[0].shape[:2]

    def spec(width):
        return pl.BlockSpec((steps, span, width), lambda i: (0, i, 0))

    return pl.pallas_call(
        body,
        grid=(frames // span,),
        in_specs=[spec(a.shape[2]) for a in arrays],
        out_specs=spec(cols),
        out_shape=jax.ShapeDtypeStruct((steps, frames, cols), BF),
    )(*arrays)


def feed_body(
    n2_ref, grad_ref, wgate_ref, wup_ref, wdown_ref, wrow_ref,
    hid_ref, d_gate_ref, d_up_ref, dn2_ref, kept_ref,
):
    step = pl.program_id(0)
    count = kept_ref.shape[0]

    @pl.when(step < count)
    def _():
        wdown = jnp.concatenate([wdown_ref[r] for r in range(wdown_ref.shape[0])], axis=1)
        gate = times(n2_ref[...], wgate_ref[...], 1, 0)
        upval = times(n2_ref[...], wup_ref[...], 1, 0)
        d_hidden = times(grad_ref[...], wdown, 1, 1)
        sigma = 1.0 / (1.0 + jnp.exp(-gate))
        silu_val = gate * sigma
        hid_ref[...] = (silu_val * upval).astype(BF)
        d_gate = (d_hidden * upval * (sigma * (1.0 + gate * (1.0 - sigma)))).astype(BF)
        d_up = (d_hidden * silu_val).astype(BF)
        d_gate_ref[...] = d_gate
        d_up_ref[...] = d_up
        kept_ref[step, 0] = d_gate
        kept_ref[step, 1] = d_up

    @pl.when(step >= count)
    def _():
        kept = [kept_ref[k, half] for half in range(2) for k in range(count)]
        dn2_ref[...] = times(jnp.concatenate(kept, axis=1), wrow_ref[...], 1, 1).astype(BF)


def feed_call(n2, grad, wgu, wdown):
    frames, width = n2.shape
    parts, hidden, block = wdown.shape
    span, part = min(256, hidden), min(512, width)
    count = hidden // span

    def hid_block(i):
        return jnp.minimum(i, count - 1)

    def out_block(i):
        return jnp.maximum(i - count, 0)

    whole = pl.BlockSpec((frames, width), lambda i: (0, 0))
    piece = pl.BlockSpec((frames, span), lambda i: (0, hid_block(i)))
    return pl.pallas_call(
        feed_body,
        grid=(count + width // part,),
        in_specs=[
            whole,
            whole,
            pl.BlockSpec((width, span), lambda i: (0, hid_block(i))),
            pl.BlockSpec((width, span), lambda i: (0, hid_block(i) + count)),
            pl.BlockSpec((parts, span, block), lambda i: (0, hid_block(i), 0)),
            pl.BlockSpec((part, 2 * hidden), lambda i: (out_block(i), 0)),
        ],
        out_specs=[piece, piece, piece, pl.BlockSpec((frames, part), lambda i: (0, out_block(i)))],
        out_shape=[jax.ShapeDtypeStruct((frames, hidden), BF)] * 3
        + [jax.ShapeDtypeStruct((frames, width), BF)],
        scratch_shapes=[pltpu.VMEM((count, 2, frames, span), BF)],
    )(n2, grad, wgu, wgu, wdown, wgu)


def make_step_shards(count, lanes):

    def exchange(blocks):
        return lax.all_to_all(blocks, "dp", 0, 0, tiled=True)

    def collect(rows):
        return lax.all_gather(rows, "tensor", axis=0).reshape(-1, rows.shape[-1])

    def deal(partial):
        slots = partial.astype(BF).reshape(lanes, count, -1, partial.shape[-1])
        return lax.psum_scatter(slots, "tensor", scatter_dimension=0)

    def frame_split(array):
        slots = array.reshape(lanes, count, -1, array.shape[-1])
        slots = jnp.swapaxes(slots, 0, 1)
        return exchange(slots.reshape(count, -1, array.shape[-1]))

    def frame_join(array):
        slots = exchange(array).reshape(count, lanes, -1, array.shape[-1])
        return jnp.swapaxes(slots, 0, 1).reshape(-1, array.shape[-1])

    def rowwise(array):
        return with_layout_constraint(array, Layout(tuple(range(array.ndim))))

    def after(value, *waiting):
        return lax.optimization_barrier((value,) + waiting)

    def shards(
        layer_in, text_mask, w_qkv, w_out, w_gate_up, w_down, norm_gains, pad_row, out_grad
    ):
        me = lax.axis_index("dp")
        steps, local, width = layer_in.shape
        block = width // count

        small = jnp.concatenate([norm_gains, pad_row[None]], axis=0).astype(BF)
        mask = jnp.pad(text_mask.astype(BF)[None], ((0, 0), (0, block - local)))
        notes = jnp.concatenate([small, mask])
        notes = jnp.pad(notes, ((0, local - notes.shape[0]), (0, 0)))
        notes = jnp.broadcast_to(notes[None], (count, local, block))
        hello = exchange(jnp.concatenate([layer_in, notes], axis=2))
        rows_in = hello[..., :width].astype(F32)
        notes = hello[:, :4, width:].astype(F32)
        small = jnp.swapaxes(notes[:, :3], 0, 1)
        gain_one, gain_two, pad_vec = small.reshape(3, width)
        padded = jnp.where(me == 0, 1.0 - notes[:, 3, :local], 0.0)[..., None]
        h0 = rows_in + padded * pad_vec
        r1 = lax.rsqrt(jnp.mean(h0 * h0, axis=-1, keepdims=True) + EPS)
        n1 = (h0 * r1 * gain_one).astype(BF)
        n1, w_qkv, w_out = after(n1, w_qkv, w_out)
        n1_all = collect(n1)

        w_attn = jnp.concatenate(
            [w_qkv[:, 0], w_qkv[:, 1], w_qkv[:, 2], jnp.swapaxes(w_out, 1, 2)], axis=2
        )
        w_attn = exchange(w_attn.astype(BF)).reshape(width, -1)
        cols = w_attn.shape[1] // 4
        w_in, wout_t = w_attn[:, : 3 * cols], w_attn[:, 3 * cols :]
        w_attn, out_grad = after(w_attn, out_grad)
        grad = exchange(out_grad)
        n1_all, grad = after(n1_all, grad)
        grad_all = collect(grad)
        qkv = jnp.dot(n1_all, w_in, preferred_element_type=F32).astype(BF)

        qkv = frame_split(qkv)
        mixed_all = frame_join(attention_call(attention_forward_body, (qkv,), cols, 2 * TILE))
        attn = jnp.einsum("fe,de->fd", mixed_all, wout_t, preferred_element_type=F32)

        attn, w_down, w_gate_up, grad_all = after(attn.astype(BF), w_down, w_gate_up, grad_all)
        attn = deal(attn)
        wdown = exchange(w_down.astype(BF))
        wgu = jnp.concatenate([w_gate_up[:, 0], w_gate_up[:, 1]], axis=2).astype(BF)
        wdown, wgu = after(wdown, wgu)
        attn, wdown = after(attn, wdown)
        wgu = exchange(wgu).reshape(width, -1)
        h1 = h0 + attn.astype(F32)
        r2 = lax.rsqrt(jnp.mean(h1 * h1, axis=-1, keepdims=True) + EPS)
        n2 = (h1 * r2 * gain_two).astype(BF)
        n2_all = collect(n2)

        hidden, d_gate, d_up, dn2 = feed_call(n2_all, grad_all, wgu, wdown)
        hid_width = hidden.shape[1]
        dn2, hidden, d_gate, d_up = after(dn2, hidden, d_gate, d_up)
        dn2 = deal(dn2)
        d_down = jnp.einsum(
            "fk,frd->rkd",
            hidden,
            grad_all.reshape(-1, count, block),
            preferred_element_type=F32,
        )
        g_down = exchange(rowwise(d_down.astype(BF)))
        g_gate = jnp.einsum("fd,fk->dk", n2_all, d_gate, preferred_element_type=F32).astype(BF)
        g_up = jnp.einsum("fd,fk->dk", n2_all, d_up, preferred_element_type=F32).astype(BF)
        part = hid_width // 2
        g_gate = jnp.concatenate([g_gate, g_up[:, :part]], axis=1).reshape(count, block, -1)
        g_up = g_up[:, part:].reshape(count, block, -1)
        dn2, g_down, g_gate, g_up = after(dn2, g_down, g_gate, g_up)
        dh_norm2, dgain_two = norm_back(dn2.astype(F32), h1, r2, gain_two)
        dh1 = grad.astype(F32) + dh_norm2
        dh1_low, g_gate, hidden = after(dh1.astype(BF), g_gate, hidden)
        dh1_all = collect(dh1_low)
        g_gate = exchange(g_gate)
        dh1_all, g_gate = after(dh1_all, g_gate)

        wdown = jnp.swapaxes(wdown, 0, 1).reshape(-1, width)
        ffout = deal(jnp.dot(hidden, wdown, preferred_element_type=F32))
        d_mixed = jnp.dot(dh1_all, wout_t, preferred_element_type=F32).astype(BF)
        d_mixed, g_up = after(frame_split(d_mixed), g_up)
        g_up = exchange(g_up)
        d_qkv = attention_call(attention_backward_body, (qkv, d_mixed), 3 * cols, 2 * TILE)
        d_qkv, g_up = after(d_qkv, g_up)
        g_up = jnp.concatenate([g_gate[..., hid_width:], g_up], axis=2)
        g_gate_up = jnp.stack([g_gate[..., :hid_width], g_up], axis=1).astype(F32)
        d_qkv = frame_join(d_qkv)
        dn1 = jnp.einsum("fe,de->fd", d_qkv, w_in, preferred_element_type=F32).astype(BF)

        dn1, d_qkv, ffout = after(dn1, d_qkv, ffout)
        dn1 = deal(dn1)
        d_attn = jnp.concatenate(
            [
                jnp.einsum("fd,fe->de", n1_all, d_qkv, preferred_element_type=F32).astype(BF),
                jnp.einsum("fd,fe->de", dh1_all, mixed_all, preferred_element_type=F32).astype(BF),
            ],
            axis=1,
        )
        g_attn = exchange(d_attn.reshape(count, block, -1))
        layer_out = (h1 + ffout.astype(F32)).astype(BF)
        g_down = g_down.astype(F32)
        dn1, g_attn, layer_out, g_gate_up, g_down = after(
            dn1, g_attn, layer_out, g_gate_up, g_down
        )

        dh_norm1, _ = norm_back(dn1.astype(F32), h0, r1, gain_one)
        dh0 = dh1 + dh_norm1
        last = jnp.concatenate([dh0.astype(BF), layer_out], axis=1)
        last, dn1, dh0, g_attn = after(last, dn1, dh0, g_attn)
        last = exchange(last)
        dgain_one = jnp.sum(dn1.astype(F32) * h0 * r1, axis=(0, 1))
        d_pad = jnp.sum(dh0 * padded, axis=(0, 1))
        sums = jnp.stack([dgain_one, dgain_two, d_pad])
        total = sums
        for k in range(1, lanes):
            around = [(i, (i + k) % lanes) for i in range(lanes)]
            total = total + lax.ppermute(sums, "tensor", around)
        total, g_attn = after(total, g_attn)
        g_attn = g_attn.astype(F32)
        g_qkv = jnp.stack([g_attn[..., j * cols : (j + 1) * cols] for j in range(3)], axis=1)
        g_out = jnp.swapaxes(g_attn[..., 3 * cols :], 1, 2)
        total = jnp.swapaxes(total.reshape(3, count, block), 0, 1)
        g_small = lax.dynamic_index_in_dim(total, me, 0, keepdims=False)
        for k in range(1, count):
            theirs = lax.dynamic_index_in_dim(total, me ^ k, 0, keepdims=False)
            g_small = g_small + lax.ppermute(theirs, "dp", [(i, i ^ k) for i in range(count)])

        g_qkv, g_out = rowwise(g_qkv), rowwise(g_out)
        last, g_small, g_gate_up, g_qkv, g_out, g_down = after(
            last, g_small, g_gate_up, g_qkv, g_out, g_down
        )
        input_grad, layer_out = last[:, :local], last[:, local:]
        return (layer_out, input_grad, g_qkv, g_out, g_gate_up, g_down, g_small[0:2], g_small[2])

    return shards


def spread(body, mesh, dp):
    rows = dp + ("tensor",)
    weights = (
        P(None, None, dp, "tensor"),
        P(None, "tensor", dp),
        P(None, None, dp, "tensor"),
        P(None, "tensor", dp),
        P(None, dp),
        P(dp),
    )
    return jax.shard_map(
        body,
        mesh=mesh,
        in_specs=(P(None, rows, None), P(rows)) + weights + (P(None, rows, None),),
        out_specs=(P(None, rows, None), P(None, rows, None)) + weights,
        check_vma=False,
    )


def solution(mesh):
    dp_size, tensor_size = mesh.shape["dp"], mesh.shape["tensor"]

    def layer(layer_in, *others):
        steps, frames, width = layer_in.shape
        local = frames // (dp_size * tensor_size)
        block = width // dp_size
        fits = 4 <= local <= block
        if steps == dp_size and dp_size & (dp_size - 1) == 0 and fits:
            body, over, dp = make_step_shards(dp_size, tensor_size), mesh, ("dp",)
        else:
            over = Mesh(
                np.asarray(mesh.devices).reshape(dp_size // 2, 2, tensor_size),
                ("xy", "core", "tensor"),
            )
            body, dp = make_shards(tensor_size), ("xy", "core")
        return spread(body, over, dp)(layer_in, *others)

    return layer
```

```python
import math

import jax
import jax.numpy as jnp
import numpy as np
from jax import lax
from jax.experimental import pallas as pl
from jax.experimental.layout import Layout, with_layout_constraint
from jax.experimental.pallas import tpu as pltpu
from jax.sharding import Mesh
from jax.sharding import PartitionSpec as P

HEAD = 64
EPS = 1e-05
HIGH = lax.Precision.HIGHEST
BF = jnp.bfloat16
F32 = jnp.float32
SWAP = ((0, 1), (1, 0))
TILE = 16


def norm_back(upstream, hval, rstat, gain):
    scaled = upstream * gain
    dgain = jnp.sum(upstream * hval * rstat, axis=(0, 1))
    dhval = rstat * scaled - hval * rstat**3 * jnp.mean(scaled * hval, axis=-1, keepdims=True)
    return (dhval, dgain)


def half(array, axis, which):
    size = array.shape[axis] // 2
    return lax.dynamic_slice_in_dim(array, which * size, size, axis)


def ordered(core, own, other, axis):
    is_first = core == 0
    return jnp.concatenate(
        [jnp.where(is_first, own, other), jnp.where(is_first, other, own)], axis=axis
    )


def make_shards(tensor_size):
    def around(shift):
        return [(i, (i + shift) % tensor_size) for i in range(tensor_size)]

    def trade(core, weight, split_axis, join_axis):
        mine = half(weight, split_axis, core)
        theirs = half(weight, split_axis, 1 - core)
        got = lax.ppermute(theirs, "core", SWAP)
        return ordered(core, mine, got, join_axis)

    def collect(rows):
        parts = [rows] + [
            lax.ppermute(rows, "tensor", around(k)) for k in range(1, tensor_size)
        ]
        near = jnp.stack(parts, axis=1)
        far = lax.ppermute(near, "core", SWAP)
        whole = jnp.concatenate([near, far], axis=1)
        return whole.reshape(rows.shape[0], -1, rows.shape[2])

    def deal(partial):
        steps, frames, width = partial.shape
        split = partial.reshape(steps, 2, tensor_size, frames // (2 * tensor_size), width)
        got = lax.ppermute(split[:, 1].astype(BF), "core", SWAP)
        chip = split[:, 0].astype(F32) + got.astype(F32)
        total = chip[:, 0]
        for k in range(1, tensor_size):
            total = total + lax.ppermute(chip[:, k].astype(BF), "tensor", around(-k)).astype(F32)
        return total

    def shards(
        layer_in, text_mask, w_qkv, w_out, w_gate_up, w_down, norm_gains, pad_row, out_grad
    ):
        core = lax.axis_index("core")
        steps, local_frames, width = layer_in.shape

        w_attn = jnp.concatenate(
            [w_qkv.astype(BF), jnp.swapaxes(w_out, 1, 2)[:, None].astype(BF)], axis=1
        )
        w_attn = lax.all_gather(trade(core, w_attn, 3, 2), "xy", axis=2, tiled=True)
        small = jnp.concatenate([norm_gains, pad_row[None]], axis=0).astype(BF)
        small = lax.all_gather(small, ("xy", "core"), axis=1, tiled=True).astype(F32)
        wgu = lax.all_gather(trade(core, w_gate_up.astype(BF), 3, 2), "xy", axis=2, tiled=True)
        wdown = lax.all_gather(trade(core, w_down.astype(BF), 1, 2), "xy", axis=2, tiled=True)

        gain_one, gain_two, pad_vec = small[0], small[1], small[2]
        maskf = text_mask.astype(F32)
        first = (jnp.arange(steps) == 0).astype(F32)
        h0 = (
            layer_in.astype(F32)
            + first[:, None, None] * (1.0 - maskf)[None, :, None] * pad_vec[None, None, :]
        )
        r1 = lax.rsqrt(jnp.mean(h0 * h0, axis=-1, keepdims=True) + EPS)
        n1 = (h0 * r1 * gain_one).astype(BF)
        n1_all = collect(n1)
        grad_all = collect(out_grad)
        frames = n1_all.shape[1]
        wqkv, wout_t = w_attn[:, :3], w_attn[:, 3]
        qkv = jnp.einsum("sfd,sjde->sjfe", n1_all, wqkv, preferred_element_type=F32).astype(BF)
        col_width = qkv.shape[-1]
        heads = col_width // HEAD
        scale = 1.0 / math.sqrt(HEAD)
        query = qkv[:, 0].reshape(steps, frames, heads, HEAD)
        keyv = qkv[:, 1].reshape(steps, frames, heads, HEAD)
        value = qkv[:, 2].reshape(steps, frames, heads, HEAD)
        causal = jnp.arange(steps)[:, None] >= jnp.arange(steps)[None, :]

        def score_of(qv, kv):
            raw = jnp.einsum("sfhe,tfhe->fhst", qv, kv, preferred_element_type=F32) * scale
            return jnp.where(causal, raw, -1e30)

        scores = score_of(query, keyv)
        top = jnp.max(scores, axis=-1, keepdims=True)
        expo = jnp.exp(scores - top)
        total = jnp.sum(expo, axis=-1, keepdims=True)
        lse = top + jnp.log(total)
        probs_low = (expo / total).astype(BF)
        mixed = jnp.einsum("fhst,tfhe->sfhe", probs_low, value, preferred_element_type=F32)
        mixed = mixed.reshape(steps, frames, col_width).astype(BF)
        attn = deal(jnp.einsum("sfd,sed->sfe", mixed, wout_t, preferred_element_type=F32))
        h1 = h0 + attn
        r2 = lax.rsqrt(jnp.mean(h1 * h1, axis=-1, keepdims=True) + EPS)
        n2 = (h1 * r2 * gain_two).astype(BF)
        n2_all = collect(n2)
        gate_up = jnp.einsum("sfd,sjde->sjfe", n2_all, wgu, preferred_element_type=F32)
        gate = gate_up[:, 0]
        upval = gate_up[:, 1]
        sigma = jax.nn.sigmoid(gate)
        silu_val = gate * sigma
        hidden = (silu_val * upval).astype(BF)
        d_down = jnp.einsum("sfk,sfd->skd", hidden, grad_all, preferred_element_type=F32)
        r_down = lax.psum_scatter(d_down.astype(BF), "xy", scatter_dimension=2, tiled=True)
        d_hidden = jnp.einsum("sfd,skd->sfk", grad_all, wdown, preferred_element_type=F32)
        d_gate = d_hidden * upval * (sigma * (1.0 + gate * (1.0 - sigma)))
        d_up = d_hidden * silu_val
        d_gu = jnp.stack([d_gate, d_up], axis=1).astype(BF)
        d_gate_up = jnp.einsum("sfd,sjfe->sjde", n2_all, d_gu, preferred_element_type=F32)
        r_gate_up = lax.psum_scatter(d_gate_up.astype(BF), "xy", scatter_dimension=2, tiled=True)
        dn2 = deal(jnp.einsum("sjfe,sjde->sfd", d_gu, wgu, preferred_element_type=F32))
        dh_norm2, dgain_two = norm_back(dn2, h1, r2, gain_two)
        dh1 = out_grad.astype(F32) + dh_norm2
        dh1_all = collect(dh1.astype(BF))
        ffout = deal(jnp.einsum("sfk,skd->sfd", hidden, wdown, preferred_element_type=F32))
        layer_out = (h1 + ffout).astype(BF)
        d_out_t = jnp.einsum("sfe,sfd->sed", dh1_all, mixed, preferred_element_type=F32)
        d_mixed = jnp.einsum("sfe,sed->sfd", dh1_all, wout_t, preferred_element_type=F32)
        d_mixed = d_mixed.astype(BF).reshape(steps, frames, heads, HEAD)
        probs = jnp.exp(score_of(query, keyv) - lse)
        d_probs = jnp.einsum("sfhe,tfhe->fhst", d_mixed, value, preferred_element_type=F32)
        d_value = jnp.einsum("fhst,sfhe->tfhe", probs_low, d_mixed, preferred_element_type=F32)
        d_scores = probs * (d_probs - jnp.sum(probs * d_probs, axis=-1, keepdims=True))
        d_query = (
            jnp.einsum("fhst,tfhe->sfhe", d_scores, keyv.astype(F32), precision=HIGH) * scale
        )
        d_key = (
            jnp.einsum("fhst,sfhe->tfhe", d_scores, query.astype(F32), precision=HIGH) * scale
        )
        d_qkv = jnp.stack(
            [
                d_query.reshape(steps, frames, col_width),
                d_key.reshape(steps, frames, col_width),
                d_value.reshape(steps, frames, col_width),
            ],
            axis=1,
        ).astype(BF)
        d_wqkv = jnp.einsum("sfd,sjfe->sjde", n1_all, d_qkv, preferred_element_type=F32)
        d_attn = jnp.concatenate([d_wqkv.astype(BF), d_out_t[:, None].astype(BF)], axis=1)
        r_attn = lax.psum_scatter(d_attn, "xy", scatter_dimension=2, tiled=True)
        dn1 = deal(jnp.einsum("sjfe,sjde->sfd", d_qkv, wqkv, preferred_element_type=F32))
        dh_norm1, dgain_one = norm_back(dn1, h0, r1, gain_one)
        dh0 = dh1 + dh_norm1
        input_grad = dh0.astype(BF)
        d_pad = jnp.sum(dh0[0] * (1.0 - maskf)[:, None], axis=0)
        small_grad = jnp.stack([dgain_one, dgain_two, d_pad], axis=0)
        small_grad = lax.psum(small_grad, ("xy", "core", "tensor"))
        place = lax.axis_index("xy") * 2 + core
        g_small = lax.dynamic_slice_in_dim(
            small_grad, place * pad_row.shape[0], pad_row.shape[0], 1
        )

        def settle(reduced, split_axis, join_axis):
            return trade(core, reduced, split_axis, join_axis).astype(F32)

        g_down = settle(r_down, 2, 1)
        g_gate_up = settle(r_gate_up, 2, 3)
        g_attn = settle(r_attn, 2, 3)
        g_qkv = g_attn[:, :3]
        g_out = jnp.swapaxes(g_attn[:, 3], 1, 2)
        return (layer_out, input_grad, g_qkv, g_out, g_gate_up, g_down, g_small[0:2], g_small[2])

    return shards


def attention_masks(steps):
    size = steps * TILE
    row = lax.broadcasted_iota(jnp.int32, (size, size), 0)
    col = lax.broadcasted_iota(jnp.int32, (size, size), 1)
    keep = (row % TILE == col % TILE) & (row <= col)
    lane = lax.broadcasted_iota(jnp.int32, (size, 2 * HEAD), 1)
    return keep, lane < HEAD


def times(left, right, left_axis, right_axis):
    return lax.dot_general(
        left, right, (((left_axis,), (right_axis,)), ((), ())), preferred_element_type=F32
    )


def attention_probs(query, keyv, keep):
    scores = jnp.where(keep, times(keyv, query, 1, 1) * (1.0 / math.sqrt(HEAD)), -1e30)
    expo = jnp.exp(scores - jnp.max(scores, axis=0, keepdims=True))
    return expo * (1.0 / jnp.sum(expo, axis=0, keepdims=True))


def attention_tile(ref, tile, start):
    part = ref[:, tile * TILE : (tile + 1) * TILE, start : start + 2 * HEAD]
    return part.reshape(-1, 2 * HEAD)


def attention_forward_body(qkv_ref, out_ref):
    steps, frames, cols = out_ref.shape
    keep, is_first = attention_masks(steps)
    for tile in range(frames // TILE):
        for pair in range(0, cols, 2 * HEAD):
            query, keyv, value = [
                attention_tile(qkv_ref, tile, j * cols + pair) for j in range(3)
            ]
            mixed = []
            for mine in (is_first, ~is_first):
                probs = attention_probs(jnp.where(mine, query, 0), keyv, keep)
                mixed.append(times(probs.astype(BF), value, 0, 0))
            mixed = jnp.where(is_first, mixed[0], mixed[1]).astype(BF)
            out_ref[:, tile * TILE : (tile + 1) * TILE, pair : pair + 2 * HEAD] = mixed.reshape(
                steps, TILE, 2 * HEAD
            )


def attention_backward_body(qkv_ref, grad_ref, out_ref):
    steps, frames, cols = grad_ref.shape
    keep, is_first = attention_masks(steps)
    scale = 1.0 / math.sqrt(HEAD)
    for tile in range(frames // TILE):
        for pair in range(0, cols, 2 * HEAD):
            query, keyv, value = [
                attention_tile(qkv_ref, tile, j * cols + pair) for j in range(3)
            ]
            grad = attention_tile(grad_ref, tile, pair)
            found = []
            for mine in (is_first, ~is_first):
                probs = attention_probs(jnp.where(mine, query, 0), keyv, keep)
                d_probs = times(value, jnp.where(mine, grad, 0), 1, 1)
                d_value = times(probs.astype(BF), grad, 1, 0)
                d_scores = probs * (d_probs - jnp.sum(probs * d_probs, axis=0, keepdims=True))
                high = d_scores.astype(BF)
                rest = (d_scores - high.astype(F32)).astype(BF)
                d_query = (times(high, keyv, 0, 0) + times(rest, keyv, 0, 0)) * scale
                d_key = (times(high, query, 1, 0) + times(rest, query, 1, 0)) * scale
                found.append((d_query, d_key, d_value))
            for j in range(3):
                part = jnp.where(is_first, found[0][j], found[1][j]).astype(BF)
                start = j * cols + pair
                out_ref[:, tile * TILE : (tile + 1) * TILE, start : start + 2 * HEAD] = (
                    part.reshape(steps, TILE, 2 * HEAD)
                )


def attention_call(body, arrays, cols, span):
    steps, frames = arrays[0].shape[:2]

    def spec(width):
        return pl.BlockSpec((steps, span, width), lambda i: (0, i, 0))

    return pl.pallas_call(
        body,
        grid=(frames // span,),
        in_specs=[spec(a.shape[2]) for a in arrays],
        out_specs=spec(cols),
        out_shape=jax.ShapeDtypeStruct((steps, frames, cols), BF),
    )(*arrays)


def feed_body(
    n2_ref, grad_ref, wgate_ref, wup_ref, wdown_ref, wrow_ref,
    hid_ref, d_gate_ref, d_up_ref, dn2_ref, kept_ref,
):
    step = pl.program_id(0)
    count = kept_ref.shape[0]

    @pl.when(step < count)
    def _():
        wdown = jnp.concatenate([wdown_ref[r] for r in range(wdown_ref.shape[0])], axis=1)
        gate = times(n2_ref[...], wgate_ref[...], 1, 0)
        upval = times(n2_ref[...], wup_ref[...], 1, 0)
        d_hidden = times(grad_ref[...], wdown, 1, 1)
        sigma = 1.0 / (1.0 + jnp.exp(-gate))
        silu_val = gate * sigma
        hid_ref[...] = (silu_val * upval).astype(BF)
        d_gate = (d_hidden * upval * (sigma * (1.0 + gate * (1.0 - sigma)))).astype(BF)
        d_up = (d_hidden * silu_val).astype(BF)
        d_gate_ref[...] = d_gate
        d_up_ref[...] = d_up
        kept_ref[step, 0] = d_gate
        kept_ref[step, 1] = d_up

    @pl.when(step >= count)
    def _():
        kept = [kept_ref[k, half] for half in range(2) for k in range(count)]
        dn2_ref[...] = times(jnp.concatenate(kept, axis=1), wrow_ref[...], 1, 1).astype(BF)


def feed_call(n2, grad, wgu, wdown):
    frames, width = n2.shape
    parts, hidden, block = wdown.shape
    span, part = min(256, hidden), min(512, width)
    count = hidden // span

    def hid_block(i):
        return jnp.minimum(i, count - 1)

    def out_block(i):
        return jnp.maximum(i - count, 0)

    whole = pl.BlockSpec((frames, width), lambda i: (0, 0))
    piece = pl.BlockSpec((frames, span), lambda i: (0, hid_block(i)))
    return pl.pallas_call(
        feed_body,
        grid=(count + width // part,),
        in_specs=[
            whole,
            whole,
            pl.BlockSpec((width, span), lambda i: (0, hid_block(i))),
            pl.BlockSpec((width, span), lambda i: (0, hid_block(i) + count)),
            pl.BlockSpec((parts, span, block), lambda i: (0, hid_block(i), 0)),
            pl.BlockSpec((part, 2 * hidden), lambda i: (out_block(i), 0)),
        ],
        out_specs=[piece, piece, piece, pl.BlockSpec((frames, part), lambda i: (0, out_block(i)))],
        out_shape=[jax.ShapeDtypeStruct((frames, hidden), BF)] * 3
        + [jax.ShapeDtypeStruct((frames, width), BF)],
        scratch_shapes=[pltpu.VMEM((count, 2, frames, span), BF)],
    )(n2, grad, wgu, wgu, wdown, wgu)


def make_step_shards(count, lanes):

    def exchange(blocks):
        return lax.all_to_all(blocks, "dp", 0, 0, tiled=True)

    def collect(rows):
        return lax.all_gather(rows, "tensor", axis=0).reshape(-1, rows.shape[-1])

    def deal(partial):
        slots = partial.astype(BF).reshape(lanes, count, -1, partial.shape[-1])
        return lax.psum_scatter(slots, "tensor", scatter_dimension=0)

    def frame_split(array):
        slots = array.reshape(lanes, count, -1, array.shape[-1])
        slots = jnp.swapaxes(slots, 0, 1)
        return exchange(slots.reshape(count, -1, array.shape[-1]))

    def frame_join(array):
        slots = exchange(array).reshape(count, lanes, -1, array.shape[-1])
        return jnp.swapaxes(slots, 0, 1).reshape(-1, array.shape[-1])

    def rowwise(array):
        return with_layout_constraint(array, Layout(tuple(range(array.ndim))))

    def after(value, *waiting):
        return lax.optimization_barrier((value,) + waiting)

    def shards(
        layer_in, text_mask, w_qkv, w_out, w_gate_up, w_down, norm_gains, pad_row, out_grad
    ):
        me = lax.axis_index("dp")
        steps, local, width = layer_in.shape
        block = width // count

        small = jnp.concatenate([norm_gains, pad_row[None]], axis=0).astype(BF)
        mask = jnp.pad(text_mask.astype(BF)[None], ((0, 0), (0, block - local)))
        notes = jnp.concatenate([small, mask])
        notes = jnp.pad(notes, ((0, local - notes.shape[0]), (0, 0)))
        notes = jnp.broadcast_to(notes[None], (count, local, block))
        hello = exchange(jnp.concatenate([layer_in, notes], axis=2))
        rows_in = hello[..., :width].astype(F32)
        notes = hello[:, :4, width:].astype(F32)
        small = jnp.swapaxes(notes[:, :3], 0, 1)
        gain_one, gain_two, pad_vec = small.reshape(3, width)
        padded = jnp.where(me == 0, 1.0 - notes[:, 3, :local], 0.0)[..., None]
        h0 = rows_in + padded * pad_vec
        r1 = lax.rsqrt(jnp.mean(h0 * h0, axis=-1, keepdims=True) + EPS)
        n1 = (h0 * r1 * gain_one).astype(BF)
        n1, w_qkv, w_out = after(n1, w_qkv, w_out)
        n1_all = collect(n1)

        w_attn = jnp.concatenate(
            [w_qkv[:, 0], w_qkv[:, 1], w_qkv[:, 2], jnp.swapaxes(w_out, 1, 2)], axis=2
        )
        w_attn = exchange(w_attn.astype(BF)).reshape(width, -1)
        cols = w_attn.shape[1] // 4
        w_in, wout_t = w_attn[:, : 3 * cols], w_attn[:, 3 * cols :]
        w_attn, out_grad = after(w_attn, out_grad)
        grad = exchange(out_grad)
        n1_all, grad = after(n1_all, grad)
        grad_all = collect(grad)
        qkv = jnp.dot(n1_all, w_in, preferred_element_type=F32).astype(BF)

        qkv = frame_split(qkv)
        mixed_all = frame_join(attention_call(attention_forward_body, (qkv,), cols, 2 * TILE))
        attn = jnp.einsum("fe,de->fd", mixed_all, wout_t, preferred_element_type=F32)

        attn, w_down, w_gate_up, grad_all = after(attn.astype(BF), w_down, w_gate_up, grad_all)
        attn = deal(attn)
        wdown = exchange(w_down.astype(BF))
        wgu = jnp.concatenate([w_gate_up[:, 0], w_gate_up[:, 1]], axis=2).astype(BF)
        wdown, wgu = after(wdown, wgu)
        attn, wdown = after(attn, wdown)
        wgu = exchange(wgu).reshape(width, -1)
        h1 = h0 + attn.astype(F32)
        r2 = lax.rsqrt(jnp.mean(h1 * h1, axis=-1, keepdims=True) + EPS)
        n2 = (h1 * r2 * gain_two).astype(BF)
        n2_all = collect(n2)

        hidden, d_gate, d_up, dn2 = feed_call(n2_all, grad_all, wgu, wdown)
        hid_width = hidden.shape[1]
        dn2, hidden, d_gate, d_up = after(dn2, hidden, d_gate, d_up)
        dn2 = deal(dn2)
        d_down = jnp.einsum(
            "fk,frd->rkd",
            hidden,
            grad_all.reshape(-1, count, block),
            preferred_element_type=F32,
        )
        g_down = exchange(rowwise(d_down.astype(BF)))
        g_gate = jnp.einsum("fd,fk->dk", n2_all, d_gate, preferred_element_type=F32).astype(BF)
        g_up = jnp.einsum("fd,fk->dk", n2_all, d_up, preferred_element_type=F32).astype(BF)
        g_gate_up = rowwise(jnp.concatenate([g_gate, g_up], axis=1))
        g_down, g_gate_up = after(g_down, g_gate_up)
        wdown = jnp.swapaxes(wdown, 0, 1).reshape(-1, width)
        ffout = jnp.dot(hidden, wdown, preferred_element_type=F32).astype(BF)
        dn2, g_down, ffout = after(dn2, g_down, ffout)
        g_gate_up = exchange(g_gate_up.reshape(count, block, -1))
        dh_norm2, dgain_two = norm_back(dn2.astype(F32), h1, r2, gain_two)
        dh1 = grad.astype(F32) + dh_norm2
        dh1_all = collect(dh1.astype(BF))
        dh1_all, g_gate_up, ffout = after(dh1_all, g_gate_up, ffout)
        ffout = deal(ffout)
        d_mixed = jnp.dot(dh1_all, wout_t, preferred_element_type=F32).astype(BF)
        d_mixed = frame_split(d_mixed)
        d_qkv = attention_call(attention_backward_body, (qkv, d_mixed), 3 * cols, 2 * TILE)
        g_gate_up = jnp.stack([g_gate_up[..., :hid_width], g_gate_up[..., hid_width:]], axis=1)
        g_gate_up = g_gate_up.astype(F32)
        d_qkv = frame_join(d_qkv)
        dn1 = jnp.einsum("fe,de->fd", d_qkv, w_in, preferred_element_type=F32).astype(BF)

        dn1, d_qkv, ffout = after(dn1, d_qkv, ffout)
        dn1 = deal(dn1)
        d_attn = jnp.concatenate(
            [
                jnp.einsum("fd,fe->de", n1_all, d_qkv, preferred_element_type=F32).astype(BF),
                jnp.einsum("fd,fe->de", dh1_all, mixed_all, preferred_element_type=F32).astype(BF),
            ],
            axis=1,
        )
        g_attn = exchange(d_attn.reshape(count, block, -1))
        layer_out = (h1 + ffout.astype(F32)).astype(BF)
        g_down = g_down.astype(F32)
        dn1, g_attn, layer_out, g_gate_up, g_down = after(
            dn1, g_attn, layer_out, g_gate_up, g_down
        )

        dh_norm1, _ = norm_back(dn1.astype(F32), h0, r1, gain_one)
        dh0 = dh1 + dh_norm1
        last = jnp.concatenate([dh0.astype(BF), layer_out], axis=1)
        last, dn1, dh0, g_attn = after(last, dn1, dh0, g_attn)
        last = exchange(last)
        dgain_one = jnp.sum(dn1.astype(F32) * h0 * r1, axis=(0, 1))
        d_pad = jnp.sum(dh0 * padded, axis=(0, 1))
        sums = jnp.stack([dgain_one, dgain_two, d_pad])
        total = sums
        for k in range(1, lanes):
            around = [(i, (i + k) % lanes) for i in range(lanes)]
            total = total + lax.ppermute(sums, "tensor", around)
        total, g_attn = after(total, g_attn)
        g_attn = g_attn.astype(F32)
        g_qkv = jnp.stack([g_attn[..., j * cols : (j + 1) * cols] for j in range(3)], axis=1)
        g_out = jnp.swapaxes(g_attn[..., 3 * cols :], 1, 2)
        total = jnp.swapaxes(total.reshape(3, count, block), 0, 1)
        g_small = lax.dynamic_index_in_dim(total, me, 0, keepdims=False)
        for k in range(1, count):
            theirs = lax.dynamic_index_in_dim(total, me ^ k, 0, keepdims=False)
            g_small = g_small + lax.ppermute(theirs, "dp", [(i, i ^ k) for i in range(count)])

        g_qkv, g_out = rowwise(g_qkv), rowwise(g_out)
        last, g_small, g_gate_up, g_qkv, g_out, g_down = after(
            last, g_small, g_gate_up, g_qkv, g_out, g_down
        )
        input_grad, layer_out = last[:, :local], last[:, local:]
        return (layer_out, input_grad, g_qkv, g_out, g_gate_up, g_down, g_small[0:2], g_small[2])

    return shards


def spread(body, mesh, dp):
    rows = dp + ("tensor",)
    weights = (
        P(None, None, dp, "tensor"),
        P(None, "tensor", dp),
        P(None, None, dp, "tensor"),
        P(None, "tensor", dp),
        P(None, dp),
        P(dp),
    )
    return jax.shard_map(
        body,
        mesh=mesh,
        in_specs=(P(None, rows, None), P(rows)) + weights + (P(None, rows, None),),
        out_specs=(P(None, rows, None), P(None, rows, None)) + weights,
        check_vma=False,
    )


def solution(mesh):
    dp_size, tensor_size = mesh.shape["dp"], mesh.shape["tensor"]

    def layer(layer_in, *others):
        steps, frames, width = layer_in.shape
        local = frames // (dp_size * tensor_size)
        block = width // dp_size
        fits = 4 <= local <= block
        if steps == dp_size and dp_size & (dp_size - 1) == 0 and fits:
            body, over, dp = make_step_shards(dp_size, tensor_size), mesh, ("dp",)
        else:
            over = Mesh(
                np.asarray(mesh.devices).reshape(dp_size // 2, 2, tensor_size),
                ("xy", "core", "tensor"),
            )
            body, dp = make_shards(tensor_size), ("xy", "core")
        return spread(body, over, dp)(layer_in, *others)

    return layer
```

```python
import math

import jax
import jax.numpy as jnp
import numpy as np
from jax import lax
from jax.experimental import pallas as pl
from jax.experimental.layout import Layout, with_layout_constraint
from jax.experimental.pallas import tpu as pltpu
from jax.sharding import Mesh
from jax.sharding import PartitionSpec as P

HEAD = 64
EPS = 1e-05
HIGH = lax.Precision.HIGHEST
BF = jnp.bfloat16
F32 = jnp.float32
SWAP = ((0, 1), (1, 0))
TILE = 16


def norm_back(upstream, hval, rstat, gain):
    scaled = upstream * gain
    dgain = jnp.sum(upstream * hval * rstat, axis=(0, 1))
    dhval = rstat * scaled - hval * rstat**3 * jnp.mean(scaled * hval, axis=-1, keepdims=True)
    return (dhval, dgain)


def half(array, axis, which):
    size = array.shape[axis] // 2
    return lax.dynamic_slice_in_dim(array, which * size, size, axis)


def ordered(core, own, other, axis):
    is_first = core == 0
    return jnp.concatenate(
        [jnp.where(is_first, own, other), jnp.where(is_first, other, own)], axis=axis
    )


def make_shards(tensor_size):
    def around(shift):
        return [(i, (i + shift) % tensor_size) for i in range(tensor_size)]

    def trade(core, weight, split_axis, join_axis):
        mine = half(weight, split_axis, core)
        theirs = half(weight, split_axis, 1 - core)
        got = lax.ppermute(theirs, "core", SWAP)
        return ordered(core, mine, got, join_axis)

    def collect(rows):
        parts = [rows] + [
            lax.ppermute(rows, "tensor", around(k)) for k in range(1, tensor_size)
        ]
        near = jnp.stack(parts, axis=1)
        far = lax.ppermute(near, "core", SWAP)
        whole = jnp.concatenate([near, far], axis=1)
        return whole.reshape(rows.shape[0], -1, rows.shape[2])

    def deal(partial):
        steps, frames, width = partial.shape
        split = partial.reshape(steps, 2, tensor_size, frames // (2 * tensor_size), width)
        got = lax.ppermute(split[:, 1].astype(BF), "core", SWAP)
        chip = split[:, 0].astype(F32) + got.astype(F32)
        total = chip[:, 0]
        for k in range(1, tensor_size):
            total = total + lax.ppermute(chip[:, k].astype(BF), "tensor", around(-k)).astype(F32)
        return total

    def shards(
        layer_in, text_mask, w_qkv, w_out, w_gate_up, w_down, norm_gains, pad_row, out_grad
    ):
        core = lax.axis_index("core")
        steps, local_frames, width = layer_in.shape

        w_attn = jnp.concatenate(
            [w_qkv.astype(BF), jnp.swapaxes(w_out, 1, 2)[:, None].astype(BF)], axis=1
        )
        w_attn = lax.all_gather(trade(core, w_attn, 3, 2), "xy", axis=2, tiled=True)
        small = jnp.concatenate([norm_gains, pad_row[None]], axis=0).astype(BF)
        small = lax.all_gather(small, ("xy", "core"), axis=1, tiled=True).astype(F32)
        wgu = lax.all_gather(trade(core, w_gate_up.astype(BF), 3, 2), "xy", axis=2, tiled=True)
        wdown = lax.all_gather(trade(core, w_down.astype(BF), 1, 2), "xy", axis=2, tiled=True)

        gain_one, gain_two, pad_vec = small[0], small[1], small[2]
        maskf = text_mask.astype(F32)
        first = (jnp.arange(steps) == 0).astype(F32)
        h0 = (
            layer_in.astype(F32)
            + first[:, None, None] * (1.0 - maskf)[None, :, None] * pad_vec[None, None, :]
        )
        r1 = lax.rsqrt(jnp.mean(h0 * h0, axis=-1, keepdims=True) + EPS)
        n1 = (h0 * r1 * gain_one).astype(BF)
        n1_all = collect(n1)
        grad_all = collect(out_grad)
        frames = n1_all.shape[1]
        wqkv, wout_t = w_attn[:, :3], w_attn[:, 3]
        qkv = jnp.einsum("sfd,sjde->sjfe", n1_all, wqkv, preferred_element_type=F32).astype(BF)
        col_width = qkv.shape[-1]
        heads = col_width // HEAD
        scale = 1.0 / math.sqrt(HEAD)
        query = qkv[:, 0].reshape(steps, frames, heads, HEAD)
        keyv = qkv[:, 1].reshape(steps, frames, heads, HEAD)
        value = qkv[:, 2].reshape(steps, frames, heads, HEAD)
        causal = jnp.arange(steps)[:, None] >= jnp.arange(steps)[None, :]

        def score_of(qv, kv):
            raw = jnp.einsum("sfhe,tfhe->fhst", qv, kv, preferred_element_type=F32) * scale
            return jnp.where(causal, raw, -1e30)

        scores = score_of(query, keyv)
        top = jnp.max(scores, axis=-1, keepdims=True)
        expo = jnp.exp(scores - top)
        total = jnp.sum(expo, axis=-1, keepdims=True)
        lse = top + jnp.log(total)
        probs_low = (expo / total).astype(BF)
        mixed = jnp.einsum("fhst,tfhe->sfhe", probs_low, value, preferred_element_type=F32)
        mixed = mixed.reshape(steps, frames, col_width).astype(BF)
        attn = deal(jnp.einsum("sfd,sed->sfe", mixed, wout_t, preferred_element_type=F32))
        h1 = h0 + attn
        r2 = lax.rsqrt(jnp.mean(h1 * h1, axis=-1, keepdims=True) + EPS)
        n2 = (h1 * r2 * gain_two).astype(BF)
        n2_all = collect(n2)
        gate_up = jnp.einsum("sfd,sjde->sjfe", n2_all, wgu, preferred_element_type=F32)
        gate = gate_up[:, 0]
        upval = gate_up[:, 1]
        sigma = jax.nn.sigmoid(gate)
        silu_val = gate * sigma
        hidden = (silu_val * upval).astype(BF)
        d_down = jnp.einsum("sfk,sfd->skd", hidden, grad_all, preferred_element_type=F32)
        r_down = lax.psum_scatter(d_down.astype(BF), "xy", scatter_dimension=2, tiled=True)
        d_hidden = jnp.einsum("sfd,skd->sfk", grad_all, wdown, preferred_element_type=F32)
        d_gate = d_hidden * upval * (sigma * (1.0 + gate * (1.0 - sigma)))
        d_up = d_hidden * silu_val
        d_gu = jnp.stack([d_gate, d_up], axis=1).astype(BF)
        d_gate_up = jnp.einsum("sfd,sjfe->sjde", n2_all, d_gu, preferred_element_type=F32)
        r_gate_up = lax.psum_scatter(d_gate_up.astype(BF), "xy", scatter_dimension=2, tiled=True)
        dn2 = deal(jnp.einsum("sjfe,sjde->sfd", d_gu, wgu, preferred_element_type=F32))
        dh_norm2, dgain_two = norm_back(dn2, h1, r2, gain_two)
        dh1 = out_grad.astype(F32) + dh_norm2
        dh1_all = collect(dh1.astype(BF))
        ffout = deal(jnp.einsum("sfk,skd->sfd", hidden, wdown, preferred_element_type=F32))
        layer_out = (h1 + ffout).astype(BF)
        d_out_t = jnp.einsum("sfe,sfd->sed", dh1_all, mixed, preferred_element_type=F32)
        d_mixed = jnp.einsum("sfe,sed->sfd", dh1_all, wout_t, preferred_element_type=F32)
        d_mixed = d_mixed.astype(BF).reshape(steps, frames, heads, HEAD)
        probs = jnp.exp(score_of(query, keyv) - lse)
        d_probs = jnp.einsum("sfhe,tfhe->fhst", d_mixed, value, preferred_element_type=F32)
        d_value = jnp.einsum("fhst,sfhe->tfhe", probs_low, d_mixed, preferred_element_type=F32)
        d_scores = probs * (d_probs - jnp.sum(probs * d_probs, axis=-1, keepdims=True))
        d_query = (
            jnp.einsum("fhst,tfhe->sfhe", d_scores, keyv.astype(F32), precision=HIGH) * scale
        )
        d_key = (
            jnp.einsum("fhst,sfhe->tfhe", d_scores, query.astype(F32), precision=HIGH) * scale
        )
        d_qkv = jnp.stack(
            [
                d_query.reshape(steps, frames, col_width),
                d_key.reshape(steps, frames, col_width),
                d_value.reshape(steps, frames, col_width),
            ],
            axis=1,
        ).astype(BF)
        d_wqkv = jnp.einsum("sfd,sjfe->sjde", n1_all, d_qkv, preferred_element_type=F32)
        d_attn = jnp.concatenate([d_wqkv.astype(BF), d_out_t[:, None].astype(BF)], axis=1)
        r_attn = lax.psum_scatter(d_attn, "xy", scatter_dimension=2, tiled=True)
        dn1 = deal(jnp.einsum("sjfe,sjde->sfd", d_qkv, wqkv, preferred_element_type=F32))
        dh_norm1, dgain_one = norm_back(dn1, h0, r1, gain_one)
        dh0 = dh1 + dh_norm1
        input_grad = dh0.astype(BF)
        d_pad = jnp.sum(dh0[0] * (1.0 - maskf)[:, None], axis=0)
        small_grad = jnp.stack([dgain_one, dgain_two, d_pad], axis=0)
        small_grad = lax.psum(small_grad, ("xy", "core", "tensor"))
        place = lax.axis_index("xy") * 2 + core
        g_small = lax.dynamic_slice_in_dim(
            small_grad, place * pad_row.shape[0], pad_row.shape[0], 1
        )

        def settle(reduced, split_axis, join_axis):
            return trade(core, reduced, split_axis, join_axis).astype(F32)

        g_down = settle(r_down, 2, 1)
        g_gate_up = settle(r_gate_up, 2, 3)
        g_attn = settle(r_attn, 2, 3)
        g_qkv = g_attn[:, :3]
        g_out = jnp.swapaxes(g_attn[:, 3], 1, 2)
        return (layer_out, input_grad, g_qkv, g_out, g_gate_up, g_down, g_small[0:2], g_small[2])

    return shards


def attention_masks(steps):
    size = steps * TILE
    row = lax.broadcasted_iota(jnp.int32, (size, size), 0)
    col = lax.broadcasted_iota(jnp.int32, (size, size), 1)
    keep = (row % TILE == col % TILE) & (row <= col)
    lane = lax.broadcasted_iota(jnp.int32, (size, 2 * HEAD), 1)
    return keep, lane < HEAD


def times(left, right, left_axis, right_axis):
    return lax.dot_general(
        left, right, (((left_axis,), (right_axis,)), ((), ())), preferred_element_type=F32
    )


def attention_probs(query, keyv, keep):
    scores = jnp.where(keep, times(keyv, query, 1, 1) * (1.0 / math.sqrt(HEAD)), -1e30)
    expo = jnp.exp(scores - jnp.max(scores, axis=0, keepdims=True))
    return expo * (1.0 / jnp.sum(expo, axis=0, keepdims=True))


def attention_tile(ref, tile, start):
    part = ref[:, tile * TILE : (tile + 1) * TILE, start : start + 2 * HEAD]
    return part.reshape(-1, 2 * HEAD)


def attention_forward_body(qkv_ref, out_ref):
    steps, frames, cols = out_ref.shape
    keep, is_first = attention_masks(steps)
    for tile in range(frames // TILE):
        for pair in range(0, cols, 2 * HEAD):
            query, keyv, value = [
                attention_tile(qkv_ref, tile, j * cols + pair) for j in range(3)
            ]
            mixed = []
            for mine in (is_first, ~is_first):
                probs = attention_probs(jnp.where(mine, query, 0), keyv, keep)
                mixed.append(times(probs.astype(BF), value, 0, 0))
            mixed = jnp.where(is_first, mixed[0], mixed[1]).astype(BF)
            out_ref[:, tile * TILE : (tile + 1) * TILE, pair : pair + 2 * HEAD] = mixed.reshape(
                steps, TILE, 2 * HEAD
            )


def attention_backward_body(qkv_ref, grad_ref, out_ref):
    steps, frames, cols = grad_ref.shape
    keep, is_first = attention_masks(steps)
    scale = 1.0 / math.sqrt(HEAD)
    for tile in range(frames // TILE):
        for pair in range(0, cols, 2 * HEAD):
            query, keyv, value = [
                attention_tile(qkv_ref, tile, j * cols + pair) for j in range(3)
            ]
            grad = attention_tile(grad_ref, tile, pair)
            found = []
            for mine in (is_first, ~is_first):
                probs = attention_probs(jnp.where(mine, query, 0), keyv, keep)
                d_probs = times(value, jnp.where(mine, grad, 0), 1, 1)
                d_value = times(probs.astype(BF), grad, 1, 0)
                d_scores = probs * (d_probs - jnp.sum(probs * d_probs, axis=0, keepdims=True))
                high = d_scores.astype(BF)
                rest = (d_scores - high.astype(F32)).astype(BF)
                d_query = (times(high, keyv, 0, 0) + times(rest, keyv, 0, 0)) * scale
                d_key = (times(high, query, 1, 0) + times(rest, query, 1, 0)) * scale
                found.append((d_query, d_key, d_value))
            for j in range(3):
                part = jnp.where(is_first, found[0][j], found[1][j]).astype(BF)
                start = j * cols + pair
                out_ref[:, tile * TILE : (tile + 1) * TILE, start : start + 2 * HEAD] = (
                    part.reshape(steps, TILE, 2 * HEAD)
                )


def attention_call(body, arrays, cols, span):
    steps, frames = arrays[0].shape[:2]

    def spec(width):
        return pl.BlockSpec((steps, span, width), lambda i: (0, i, 0))

    return pl.pallas_call(
        body,
        grid=(frames // span,),
        in_specs=[spec(a.shape[2]) for a in arrays],
        out_specs=spec(cols),
        out_shape=jax.ShapeDtypeStruct((steps, frames, cols), BF),
    )(*arrays)


def feed_body(
    n2_ref, grad_ref, wgate_ref, wup_ref, wdown_ref, wrow_ref,
    hid_ref, d_gate_ref, d_up_ref, dn2_ref, kept_ref,
):
    step = pl.program_id(0)
    count = kept_ref.shape[0]

    @pl.when(step < count)
    def _():
        wdown = jnp.concatenate([wdown_ref[r] for r in range(wdown_ref.shape[0])], axis=1)
        gate = times(n2_ref[...], wgate_ref[...], 1, 0)
        upval = times(n2_ref[...], wup_ref[...], 1, 0)
        d_hidden = times(grad_ref[...], wdown, 1, 1)
        sigma = 1.0 / (1.0 + jnp.exp(-gate))
        silu_val = gate * sigma
        hid_ref[...] = (silu_val * upval).astype(BF)
        d_gate = (d_hidden * upval * (sigma * (1.0 + gate * (1.0 - sigma)))).astype(BF)
        d_up = (d_hidden * silu_val).astype(BF)
        d_gate_ref[...] = d_gate
        d_up_ref[...] = d_up
        kept_ref[step, 0] = d_gate
        kept_ref[step, 1] = d_up

    @pl.when(step >= count)
    def _():
        kept = [kept_ref[k, half] for half in range(2) for k in range(count)]
        dn2_ref[...] = times(jnp.concatenate(kept, axis=1), wrow_ref[...], 1, 1).astype(BF)


def feed_call(n2, grad, wgu, wdown):
    frames, width = n2.shape
    parts, hidden, block = wdown.shape
    span, part = min(256, hidden), min(512, width)
    count = hidden // span

    def hid_block(i):
        return jnp.minimum(i, count - 1)

    def out_block(i):
        return jnp.maximum(i - count, 0)

    whole = pl.BlockSpec((frames, width), lambda i: (0, 0))
    piece = pl.BlockSpec((frames, span), lambda i: (0, hid_block(i)))
    return pl.pallas_call(
        feed_body,
        grid=(count + width // part,),
        in_specs=[
            whole,
            whole,
            pl.BlockSpec((width, span), lambda i: (0, hid_block(i))),
            pl.BlockSpec((width, span), lambda i: (0, hid_block(i) + count)),
            pl.BlockSpec((parts, span, block), lambda i: (0, hid_block(i), 0)),
            pl.BlockSpec((part, 2 * hidden), lambda i: (out_block(i), 0)),
        ],
        out_specs=[piece, piece, piece, pl.BlockSpec((frames, part), lambda i: (0, out_block(i)))],
        out_shape=[jax.ShapeDtypeStruct((frames, hidden), BF)] * 3
        + [jax.ShapeDtypeStruct((frames, width), BF)],
        scratch_shapes=[pltpu.VMEM((count, 2, frames, span), BF)],
    )(n2, grad, wgu, wgu, wdown, wgu)


def make_step_shards(count, lanes):

    def exchange(blocks):
        return lax.all_to_all(blocks, "dp", 0, 0, tiled=True)

    def collect(rows):
        return lax.all_gather(rows, "tensor", axis=0).reshape(-1, rows.shape[-1])

    def deal(partial):
        slots = partial.astype(BF).reshape(lanes, count, -1, partial.shape[-1])
        return lax.psum_scatter(slots, "tensor", scatter_dimension=0)

    def frame_split(array):
        slots = array.reshape(lanes, count, -1, array.shape[-1])
        slots = jnp.swapaxes(slots, 0, 1)
        return exchange(slots.reshape(count, -1, array.shape[-1]))

    def frame_join(array):
        slots = exchange(array).reshape(count, lanes, -1, array.shape[-1])
        return jnp.swapaxes(slots, 0, 1).reshape(-1, array.shape[-1])

    def rowwise(array):
        return with_layout_constraint(array, Layout(tuple(range(array.ndim))))

    def after(value, *waiting):
        return lax.optimization_barrier((value,) + waiting)

    def shards(
        layer_in, text_mask, w_qkv, w_out, w_gate_up, w_down, norm_gains, pad_row, out_grad
    ):
        me = lax.axis_index("dp")
        steps, local, width = layer_in.shape
        block = width // count

        small = jnp.concatenate([norm_gains, pad_row[None]], axis=0).astype(BF)
        mask = jnp.pad(text_mask.astype(BF)[None], ((0, 0), (0, block - local)))
        notes = jnp.concatenate([small, mask])
        notes = jnp.pad(notes, ((0, local - notes.shape[0]), (0, 0)))
        notes = jnp.broadcast_to(notes[None], (count, local, block))
        hello = exchange(jnp.concatenate([layer_in, notes], axis=2))
        rows_in = hello[..., :width].astype(F32)
        notes = hello[:, :4, width:].astype(F32)
        small = jnp.swapaxes(notes[:, :3], 0, 1)
        gain_one, gain_two, pad_vec = small.reshape(3, width)
        padded = jnp.where(me == 0, 1.0 - notes[:, 3, :local], 0.0)[..., None]
        h0 = rows_in + padded * pad_vec
        r1 = lax.rsqrt(jnp.mean(h0 * h0, axis=-1, keepdims=True) + EPS)
        n1 = (h0 * r1 * gain_one).astype(BF)
        n1, w_qkv, w_out = after(n1, w_qkv, w_out)
        n1_all = collect(n1)

        w_attn = jnp.concatenate(
            [w_qkv[:, 0], w_qkv[:, 1], w_qkv[:, 2], jnp.swapaxes(w_out, 1, 2)], axis=2
        )
        w_attn = exchange(w_attn.astype(BF)).reshape(width, -1)
        cols = w_attn.shape[1] // 4
        w_in, wout_t = w_attn[:, : 3 * cols], w_attn[:, 3 * cols :]
        w_attn, out_grad = after(w_attn, out_grad)
        grad = exchange(out_grad)
        n1_all, grad = after(n1_all, grad)
        grad_all = collect(grad)
        qkv = jnp.dot(n1_all, w_in, preferred_element_type=F32).astype(BF)

        qkv = frame_split(qkv)
        mixed_all = frame_join(attention_call(attention_forward_body, (qkv,), cols, 2 * TILE))
        attn = jnp.einsum("fe,de->fd", mixed_all, wout_t, preferred_element_type=F32)

        attn, w_down, w_gate_up, grad_all = after(attn.astype(BF), w_down, w_gate_up, grad_all)
        attn = deal(attn)
        wdown = exchange(w_down.astype(BF))
        wgu = jnp.concatenate([w_gate_up[:, 0], w_gate_up[:, 1]], axis=2).astype(BF)
        wdown, wgu = after(wdown, wgu)
        attn, wdown = after(attn, wdown)
        wgu = exchange(wgu).reshape(width, -1)
        h1 = h0 + attn.astype(F32)
        r2 = lax.rsqrt(jnp.mean(h1 * h1, axis=-1, keepdims=True) + EPS)
        n2 = (h1 * r2 * gain_two).astype(BF)
        n2_all = collect(n2)

        hidden, d_gate, d_up, dn2 = feed_call(n2_all, grad_all, wgu, wdown)
        hid_width = hidden.shape[1]
        dn2, hidden, d_gate, d_up = after(dn2, hidden, d_gate, d_up)
        dn2 = deal(dn2)
        d_down = jnp.einsum(
            "fk,frd->rkd",
            hidden,
            grad_all.reshape(-1, count, block),
            preferred_element_type=F32,
        )
        g_down = exchange(rowwise(d_down.astype(BF)))
        g_gate = jnp.einsum("fd,fk->dk", n2_all, d_gate, preferred_element_type=F32).astype(BF)
        g_gate, wdown = after(g_gate, wdown)
        g_up = jnp.einsum("fd,fk->dk", n2_all, d_up, preferred_element_type=F32).astype(BF)
        g_gate_up = rowwise(jnp.concatenate([g_gate, g_up], axis=1))
        g_down, g_gate_up = after(g_down, g_gate_up)
        wdown = jnp.swapaxes(wdown, 0, 1).reshape(-1, width)
        ffout = jnp.dot(hidden, wdown, preferred_element_type=F32).astype(BF)
        dn2, g_down, ffout = after(dn2, g_down, ffout)
        g_gate_up = exchange(g_gate_up.reshape(count, block, -1))
        dh_norm2, dgain_two = norm_back(dn2.astype(F32), h1, r2, gain_two)
        dh1 = grad.astype(F32) + dh_norm2
        dh1_all = collect(dh1.astype(BF))
        dh1_all, g_gate_up, ffout = after(dh1_all, g_gate_up, ffout)
        ffout = deal(ffout)
        d_mixed = jnp.dot(dh1_all, wout_t, preferred_element_type=F32).astype(BF)
        d_mixed = frame_split(d_mixed)
        d_qkv = attention_call(attention_backward_body, (qkv, d_mixed), 3 * cols, 2 * TILE)
        g_gate_up = jnp.stack([g_gate_up[..., :hid_width], g_gate_up[..., hid_width:]], axis=1)
        g_gate_up = g_gate_up.astype(F32)
        d_qkv = frame_join(d_qkv)
        dn1 = jnp.einsum("fe,de->fd", d_qkv, w_in, preferred_element_type=F32).astype(BF)

        dn1, d_qkv, ffout = after(dn1, d_qkv, ffout)
        dn1 = deal(dn1)
        d_attn = jnp.concatenate(
            [
                jnp.einsum("fd,fe->de", n1_all, d_qkv, preferred_element_type=F32).astype(BF),
                jnp.einsum("fd,fe->de", dh1_all, mixed_all, preferred_element_type=F32).astype(BF),
            ],
            axis=1,
        )
        g_attn = rowwise(exchange(rowwise(d_attn).reshape(count, block, -1)))
        layer_out = (h1 + ffout.astype(F32)).astype(BF)
        g_down = g_down.astype(F32)
        dn1, g_attn, layer_out, g_gate_up, g_down = after(
            dn1, g_attn, layer_out, g_gate_up, g_down
        )

        dh_norm1, _ = norm_back(dn1.astype(F32), h0, r1, gain_one)
        dh0 = dh1 + dh_norm1
        last = jnp.concatenate([dh0.astype(BF), layer_out], axis=1)
        last, dn1, dh0, g_attn = after(last, dn1, dh0, g_attn)
        last = exchange(last)
        dgain_one = jnp.sum(dn1.astype(F32) * h0 * r1, axis=(0, 1))
        d_pad = jnp.sum(dh0 * padded, axis=(0, 1))
        sums = jnp.stack([dgain_one, dgain_two, d_pad])
        total = sums
        for k in range(1, lanes):
            around = [(i, (i + k) % lanes) for i in range(lanes)]
            total = total + lax.ppermute(sums, "tensor", around)
        total, g_attn = after(total, g_attn)
        g_attn = rowwise(g_attn.astype(F32))
        g_qkv = jnp.stack([g_attn[..., j * cols : (j + 1) * cols] for j in range(3)], axis=1)
        g_out = jnp.swapaxes(g_attn[..., 3 * cols :], 1, 2)
        total = jnp.swapaxes(total.reshape(3, count, block), 0, 1)
        g_small = lax.dynamic_index_in_dim(total, me, 0, keepdims=False)
        for k in range(1, count):
            theirs = lax.dynamic_index_in_dim(total, me ^ k, 0, keepdims=False)
            g_small = g_small + lax.ppermute(theirs, "dp", [(i, i ^ k) for i in range(count)])

        g_qkv, g_out = rowwise(g_qkv), rowwise(g_out)
        last, g_small, g_gate_up, g_qkv, g_out, g_down = after(
            last, g_small, g_gate_up, g_qkv, g_out, g_down
        )
        input_grad, layer_out = last[:, :local], last[:, local:]
        return (layer_out, input_grad, g_qkv, g_out, g_gate_up, g_down, g_small[0:2], g_small[2])

    return shards


def spread(body, mesh, dp):
    rows = dp + ("tensor",)
    weights = (
        P(None, None, dp, "tensor"),
        P(None, "tensor", dp),
        P(None, None, dp, "tensor"),
        P(None, "tensor", dp),
        P(None, dp),
        P(dp),
    )
    return jax.shard_map(
        body,
        mesh=mesh,
        in_specs=(P(None, rows, None), P(rows)) + weights + (P(None, rows, None),),
        out_specs=(P(None, rows, None), P(None, rows, None)) + weights,
        check_vma=False,
    )


def solution(mesh):
    dp_size, tensor_size = mesh.shape["dp"], mesh.shape["tensor"]

    def layer(layer_in, *others):
        steps, frames, width = layer_in.shape
        local = frames // (dp_size * tensor_size)
        block = width // dp_size
        fits = 4 <= local <= block
        if steps == dp_size and dp_size & (dp_size - 1) == 0 and fits:
            body, over, dp = make_step_shards(dp_size, tensor_size), mesh, ("dp",)
        else:
            over = Mesh(
                np.asarray(mesh.devices).reshape(dp_size // 2, 2, tensor_size),
                ("xy", "core", "tensor"),
            )
            body, dp = make_shards(tensor_size), ("xy", "core")
        return spread(body, over, dp)(layer_in, *others)

    return layer
```
